32 devices in a mesh: seq: 4 (over y, core), fsdp: 8 (over z, x).
Axes of the slice: x: 2, y: 2, z: 4, core: 2. Of those that a mesh axis runs over, the one named last changes fastest.
Arguments:
- hidden: bfloat16 [16, 384, 1536], P('fsdp', 'seq'), may hold values from -6 to 6
- text: bfloat16 [16, 512, 1536], P('fsdp', 'seq'), may hold values from -6 to 6
- time_emb: bfloat16 [16, 6, 1536], P('fsdp'), may hold values from -3 to 3
- modulation: bfloat16 [6, 1536], P(None, 'fsdp'), may hold values from -3 to 3
- self_in: bfloat16 [3, 1536, 1536], P(None, 'fsdp'), may hold values from -0.15625 to 0.15625
- self_out: bfloat16 [1536, 1536], P('fsdp'), may hold values from -0.625 to 0.625
- cross_in: bfloat16 [3, 1536, 1536], P(None, 'fsdp'), may hold values from -0.15625 to 0.15625
- cross_out: bfloat16 [1536, 1536], P('fsdp'), may hold values from -0.625 to 0.625
- ffn_in: bfloat16 [1536, 8960], P('fsdp'), may hold values from -0.15625 to 0.15625
- ffn_out: bfloat16 [8960, 1536], P('fsdp'), may hold values from -0.0625 to 0.0625
- gains: bfloat16 [5, 1536], P(None, 'fsdp'), may hold values from 0.5 to 1.5
- biases: bfloat16 [10, 1536], P(None, 'fsdp'), may hold values from -2 to 2
- ffn_bias: bfloat16 [8960], P('fsdp'), may hold values from -2 to 2
- positions: int32 [16, 3, 384], P('fsdp', None, 'seq'), may hold values from 0 to 63
- cotangent: bfloat16 [16, 384, 1536], P('fsdp', 'seq'), may hold values from -6 to 6
Outputs:
- mixed: bfloat16 [16, 384, 1536], P('fsdp', 'seq')
- grad_hidden: float32 [16, 384, 1536], P('fsdp', 'seq')
- grad_text: float32 [16, 512, 1536], P('fsdp', 'seq')
- grad_time: float32 [16, 6, 1536], P('fsdp')
- grad_modulation: float32 [6, 1536], P(None, 'fsdp')
- grad_self_in: float32 [3, 1536, 1536], P(None, 'fsdp')
- grad_self_out: float32 [1536, 1536], P('fsdp')
- grad_cross_in: float32 [3, 1536, 1536], P(None, 'fsdp')
- grad_cross_out: float32 [1536, 1536], P('fsdp')
- grad_ffn_in: float32 [1536, 8960], P('fsdp')
- grad_ffn_out: float32 [8960, 1536], P('fsdp')
- grad_gains: float32 [5, 1536], P(None, 'fsdp')
- grad_biases: float32 [10, 1536], P(None, 'fsdp')
- grad_ffn_bias: float32 [8960], P('fsdp')
The draws below stay inside these ranges and needn't reach their ends.
All inputs are finite; a program needn't handle non-finite values.
Results may differ from the reference program's by a relative error of at most 0.022.
Values may be sent and summed in bfloat16 or wider, within the bound.
A program may use at most 304 MiB of HBM per device.

```python
import jax
import jax.numpy as jnp
from jax import lax

D = 1536
HEADS = 12
HEAD = 128
FF = 8960
TEXT = 512
LEN = 384
CLIPS = 16


def with_ends(array, stream_key, smallest, largest):
    shape = array.shape
    spot = [jax.random.randint(jax.random.fold_in(stream_key, axis), (), 0, shape[axis]) for axis in range(len(shape))]
    array = array.at[tuple(spot)].set(smallest)
    longest = shape.index(max(shape))
    spot[longest] = (spot[longest] + 1) % shape[longest]
    return array.at[tuple(spot)].set(largest)


def with_spikes(values, key, source, target, parts, factor):
    owner, partner = [(jnp.arange(values.shape[axis_at]) // (values.shape[axis_at] // parts)).reshape([-1 if axis == axis_at else 1 for axis in range(values.ndim)]) for axis_at in (source, target)]
    chosen = jax.random.permutation(key, parts)[partner]
    strong = (owner == chosen) | (owner == (partner + parts // 2) % parts)
    return jnp.where(strong, factor * values, values)


def block_levels(key, dims, pieces, low, top_value):
    def one(dim, shards_of):
        draws = jax.random.uniform(jax.random.fold_in(jax.random.fold_in(key, 6), dim), (shards_of,), jnp.float32, low / len(pieces), top_value / len(pieces))
        return jnp.repeat(jnp.exp(draws), dims[dim] // shards_of).reshape((-1,) + (1,) * (len(dims) - dim - 1))

    level = one(*pieces[0])
    for cut in pieces[1:]:
        level = level * one(*cut)
    return level


def noise(stream_key, shape, deviation, bound, pieces=(), held_as=jnp.bfloat16):
    level = block_levels(stream_key, shape, pieces, -0.22, 0.18) if pieces else 1.0
    drawn = jax.random.normal(stream_key, shape, jnp.float32) * deviation * level
    return jnp.minimum(jnp.maximum(drawn, -bound), bound).astype(held_as)


def bell_draw_with(own_key, dims, deviation, limit, shards, heavy, kind=jnp.bfloat16):
    values = deviation * jax.random.normal(own_key, dims, jnp.float32)
    if shards:
        values = values * block_levels(own_key, dims, shards, -0.22, 0.18)
    return jnp.clip(with_spikes(values, jax.random.fold_in(own_key, 3), *heavy), -limit, limit).astype(kind)


def setup_inputs(seed: int = 0) -> dict:
    keys = jax.random.split(jax.random.key(seed), 16)
    hidden = bell_draw_with(keys[0], (CLIPS, LEN, D), 1.0, 6.0, ((0, 8), (1, 4)), (0, 2, 8, 2.0))
    text = noise(keys[1], (CLIPS, TEXT, D), 1.0, 6.0, ((0, 8), (1, 4)))
    time_emb = noise(keys[2], (CLIPS, 6, D), 0.5, 3.0, ((0, 8),))
    modulation = noise(keys[3], (6, D), 0.5, 3.0, ((1, 8),))
    self_in = noise(keys[4], (3, D, D), D ** -0.5, 0.15625, ((1, 8),))
    self_out = noise(keys[5], (D, D), (D // 16) ** -0.5, 0.625, ((0, 8),))
    cross_in = noise(keys[6], (3, D, D), D ** -0.5, 0.15625, ((1, 8),))
    cross_out = noise(keys[7], (D, D), (D // 16) ** -0.5, 0.625, ((0, 8),))
    ffn_in = noise(keys[8], (D, FF), D ** -0.5, 0.15625, ((0, 8),))
    ffn_out = noise(keys[9], (FF, D), FF ** -0.5, 0.0625, ((0, 8),))
    gains = jnp.clip(1.0 + 0.1 * jax.random.normal(keys[10], (5, D), jnp.float32), 0.5, 1.5).astype(jnp.bfloat16)
    biases = noise(keys[11], (10, D), 0.3, 2.0, ((1, 8),))
    ffn_bias = noise(keys[12], (FF,), 0.3, 2.0, ((0, 8),))
    positions = with_ends(jax.random.randint(keys[13], (CLIPS, 3, LEN), 0, 64), jax.random.fold_in(keys[13], 1), 0, 63).astype(jnp.int32)
    cotangent = noise(keys[14], (CLIPS, LEN, D), 1.0, 6.0, ((0, 8), (1, 4)))
    return dict(hidden=hidden, text=text, time_emb=time_emb, modulation=modulation, self_in=self_in, self_out=self_out, cross_in=cross_in, cross_out=cross_out, ffn_in=ffn_in, ffn_out=ffn_out, gains=gains, biases=biases, ffn_bias=ffn_bias, positions=positions, cotangent=cotangent)


@jax.custom_vjp
def low(v):
    return lax.optimization_barrier(v.astype(jnp.bfloat16)).astype(jnp.float32)

@jax.custom_vjp
def low_back(v):
    return v

def low_keep(v):
    return (low(v), None)

def low_pass(kept, grad):
    return (grad,)

def back_keep(v):
    return (v, None)

def back_low(kept, grad):
    return (low(grad),)
low.defvjp(low_keep, low_pass)
low_back.defvjp(back_keep, back_low)
EPSILON = 1e-06

def matmul(operand, factor):
    return jnp.matmul(operand, factor, precision=lax.Precision.HIGHEST)

def layer_norm(tensor):
    centered = tensor - lax.optimization_barrier(jnp.mean(tensor, axis=-1, keepdims=True))
    return centered * lax.rsqrt(lax.optimization_barrier(jnp.mean(centered * centered, axis=-1, keepdims=True)) + EPSILON)

def rms_norm(tensor, weight):
    return tensor * lax.rsqrt(lax.optimization_barrier(jnp.mean(tensor * tensor, axis=-1, keepdims=True)) + EPSILON) * weight

def gelu_tanh(tensor):
    return jax.nn.gelu(tensor, approximate=True)

def rotary_tables(places, head_size, head_count):
    one_sixth = head_size // 6
    span_sizes = (head_size - 4 * one_sixth, 2 * one_sixth, 2 * one_sixth)
    angles = []
    for component in range(3):
        exponents = jnp.arange(0, span_sizes[component], 2, dtype=jnp.float32) / span_sizes[component]
        frequency = 1.0 / 10000.0 ** exponents
        angles.append(places[component].astype(jnp.float32)[:, None] * frequency[None, :])
    joined = jnp.concatenate(angles, axis=1)
    tiled_angles = jnp.tile(jnp.repeat(joined, 2, axis=1), (1, head_count))
    parity = jnp.where(jnp.arange(tiled_angles.shape[1]) % 2 == 0, -1.0, 1.0)
    return (jnp.cos(tiled_angles), jnp.sin(tiled_angles) * parity)

def rotate(tensor, cosine, signed_sine):
    even_lane = jnp.arange(tensor.shape[1]) % 2 == 0
    swapped = jnp.where(even_lane, jnp.roll(tensor, -1, axis=1), jnp.roll(tensor, 1, axis=1))
    return tensor * cosine + swapped * signed_sine

def attend(queries, key_rows, value_rows):
    heads_here = queries.shape[1] // HEAD
    query_split = queries.reshape(queries.shape[0], heads_here, HEAD)
    key_split = key_rows.reshape(key_rows.shape[0], heads_here, HEAD)
    value_split = value_rows.reshape(value_rows.shape[0], heads_here, HEAD)
    scores = jnp.einsum('qhd,khd->hqk', query_split, key_split, precision=lax.Precision.HIGHEST) * HEAD ** (-0.5)
    scores = low_back(scores)
    row_max = lax.optimization_barrier(jnp.max(scores, axis=-1, keepdims=True))
    exponentials = jnp.exp(scores - row_max)
    probabilities = low(exponentials / lax.optimization_barrier(jnp.sum(exponentials, axis=-1, keepdims=True)))
    result = jnp.einsum('hqk,khd->qhd', probabilities, value_split, precision=lax.Precision.HIGHEST)
    return result.reshape(queries.shape[0], -1)

def block_forward(residual_in, text_rows, time_rows, params, cosine, signed_sine):
    modulation, self_in, self_out, cross_in, cross_out, ffn_in, ffn_out, gains, biases, ffn_bias = params
    modulated = modulation + time_rows
    normed = low(layer_norm(residual_in) * (1.0 + modulated[1]) + modulated[0])
    query_pre = low_back(matmul(normed, self_in[0]) + biases[0])
    key_pre = low_back(matmul(normed, self_in[1]) + biases[1])
    value_rows = low_back(low(matmul(normed, self_in[2]) + biases[2]))
    query_turned = low_back(low(rotate(rms_norm(query_pre, gains[0]), cosine, signed_sine)))
    key_turned = low_back(low(rotate(rms_norm(key_pre, gains[1]), cosine, signed_sine)))
    attended = low_back(low(attend(query_turned, key_turned, value_rows)))
    branch = low_back(matmul(attended, self_out) + biases[3])
    after_attn = residual_in + branch * modulated[2]
    crossed = low(layer_norm(after_attn) * gains[4] + biases[8])
    cross_query = low(rms_norm(low_back(matmul(crossed, cross_in[0]) + biases[4]), gains[2]))
    text_key = low(rms_norm(low_back(matmul(text_rows, cross_in[1]) + biases[5]), gains[3]))
    text_value = low_back(low(matmul(text_rows, cross_in[2]) + biases[6]))
    cross_rows = low_back(low(attend(cross_query, text_key, text_value)))
    second = after_attn + low_back(matmul(cross_rows, cross_out) + biases[7])
    ffn_normed = low(layer_norm(second) * (1.0 + modulated[4]) + modulated[3])
    pre_act = low_back(matmul(ffn_normed, ffn_in) + ffn_bias)
    activation = low(gelu_tanh(pre_act))
    ffn_branch = low_back(matmul(activation, ffn_out) + biases[9])
    return second + ffn_branch * modulated[5]

def reference(hidden, text, time_emb, modulation, self_in, self_out, cross_in, cross_out, ffn_in, ffn_out, gains, biases, ffn_bias, positions, cotangent):
    weights = tuple((weight.astype(jnp.float32) for weight in (modulation, self_in, self_out, cross_in, cross_out, ffn_in, ffn_out, gains, biases, ffn_bias)))

    def per_clip(totals, inputs):
        clip_hidden, clip_text, clip_time, places, clip_cotangent = inputs
        cosine, signed_sine = rotary_tables(places, HEAD, HEADS)

        def forward(residual_in, text_rows, time_rows, params):
            return block_forward(residual_in, text_rows, time_rows, params, cosine, signed_sine)
        result, pullback = jax.vjp(forward, clip_hidden.astype(jnp.float32), clip_text.astype(jnp.float32), clip_time.astype(jnp.float32), weights)
        grad_start, grad_words, grad_clock, grad_weights = pullback(clip_cotangent.astype(jnp.float32))
        totals = jax.tree.map(jnp.add, totals, grad_weights)
        return (totals, (result.astype(jnp.bfloat16), grad_start, grad_words, grad_clock))
    zeros = jax.tree.map(jnp.zeros_like, weights)
    totals, outputs = lax.scan(per_clip, zeros, (hidden, text, time_emb, positions, cotangent))
    mixed, grad_hidden, grad_text, grad_time = outputs
    return (mixed, grad_hidden, grad_text, grad_time, totals[0], totals[1], totals[2], totals[3], totals[4], totals[5], totals[6], totals[7], totals[8], totals[9])
```

```python
import jax
import jax.numpy as jnp
from jax import lax
from jax.sharding import Mesh, PartitionSpec as P

HEADS = 12
HEAD = 128


EPSILON = 1e-06
SEQ = ("y", "core")
SWAP = [(0, 1), (1, 0)]


def matmul(operand, factor):
    return jnp.dot(operand, factor, preferred_element_type=jnp.float32)


def inner_rows(operand, factor):
    return lax.dot_general(
        operand, factor, (((0,), (0,)), ((), ())), preferred_element_type=jnp.float32
    )


def outer_cols(operand, factor):
    return lax.dot_general(
        operand, factor, (((1,), (1,)), ((), ())), preferred_element_type=jnp.float32
    )


def column_sums(tensor):
    return jnp.sum(tensor.astype(jnp.float32), axis=0)


def layer_norm(tensor):
    centered = tensor - jnp.mean(tensor, axis=-1, keepdims=True)
    return centered * lax.rsqrt(jnp.mean(centered * centered, axis=-1, keepdims=True) + EPSILON)


def rms_norm(tensor, weight):
    return tensor * lax.rsqrt(jnp.mean(tensor * tensor, axis=-1, keepdims=True) + EPSILON) * weight


def modulate_norm(tensor, shift, scale):
    return layer_norm(tensor) * (1.0 + scale) + shift


def affine_norm(tensor, weight, offset):
    return layer_norm(tensor) * weight + offset


def gelu_tanh(tensor):
    return jax.nn.gelu(tensor, approximate=True)


def rotary_tables(places, head_size, head_count):
    one_sixth = head_size // 6
    span_sizes = (head_size - 4 * one_sixth, 2 * one_sixth, 2 * one_sixth)
    angles = []
    for component in range(3):
        exponents = (
            jnp.arange(0, span_sizes[component], 2, dtype=jnp.float32) / span_sizes[component]
        )
        frequency = 1.0 / 10000.0**exponents
        angles.append(places[component].astype(jnp.float32)[:, None] * frequency[None, :])
    joined = jnp.concatenate(angles, axis=1)
    tiled_angles = jnp.tile(jnp.repeat(joined, 2, axis=1), (1, head_count))
    parity = jnp.where(jnp.arange(tiled_angles.shape[1]) % 2 == 0, -1.0, 1.0)
    return (jnp.cos(tiled_angles), jnp.sin(tiled_angles) * parity)


def rotate(tensor, cosine, signed_sine):
    even_lane = jnp.arange(tensor.shape[1]) % 2 == 0
    swapped = jnp.where(even_lane, jnp.roll(tensor, -1, axis=1), jnp.roll(tensor, 1, axis=1))
    return tensor * cosine + swapped * signed_sine


def split_heads(tensor):
    return tensor.reshape(tensor.shape[0], tensor.shape[1] // HEAD, HEAD)


def attend(queries, key_rows, value_rows):
    scores = jnp.einsum(
        "qhd,khd->hqk",
        split_heads(queries),
        split_heads(key_rows),
        preferred_element_type=jnp.float32,
    ) * HEAD ** (-0.5)
    row_max = jnp.max(scores, axis=-1, keepdims=True)
    exponentials = jnp.exp(scores - row_max)
    row_total = jnp.sum(exponentials, axis=-1, keepdims=True)
    probabilities = (exponentials / row_total).astype(jnp.bfloat16)
    result = jnp.einsum(
        "hqk,khd->qhd", probabilities, split_heads(value_rows), preferred_element_type=jnp.float32
    )
    return (result.reshape(queries.shape[0], -1).astype(jnp.bfloat16), row_max + jnp.log(row_total))


def attend_back(queries, key_rows, value_rows, log_total, grad_rows):
    query_split = split_heads(queries)
    key_split = split_heads(key_rows)
    grad_split = split_heads(grad_rows)
    scale_factor = HEAD ** (-0.5)
    scores = (
        jnp.einsum("qhd,khd->hqk", query_split, key_split, preferred_element_type=jnp.float32)
        * scale_factor
    )
    probs_full = jnp.exp(scores - log_total)
    probs_low = probs_full.astype(jnp.bfloat16)
    grad_values = jnp.einsum(
        "hqk,qhd->khd", probs_low, grad_split, preferred_element_type=jnp.float32
    )
    grad_probs = jnp.einsum(
        "qhd,khd->hqk", grad_split, split_heads(value_rows), preferred_element_type=jnp.float32
    )
    grad_scores = (
        probs_full * (grad_probs - jnp.sum(grad_probs * probs_full, axis=-1, keepdims=True))
    ).astype(jnp.bfloat16)
    grad_queries = (
        jnp.einsum("hqk,khd->qhd", grad_scores, key_split, preferred_element_type=jnp.float32)
        * scale_factor
    )
    grad_keys = (
        jnp.einsum("hqk,qhd->khd", grad_scores, query_split, preferred_element_type=jnp.float32)
        * scale_factor
    )
    return (
        grad_queries.reshape(queries.shape[0], -1),
        grad_keys.reshape(key_rows.shape[0], -1),
        grad_values.reshape(value_rows.shape[0], -1),
    )


def swap_core(tensor):
    return lax.ppermute(tensor, "core", SWAP)


def join(mine, other, core):
    width = mine.shape[-1]
    both = jnp.concatenate([other, mine, other], axis=-1)
    return lax.dynamic_slice_in_dim(both, (1 - core) * width, 2 * width, axis=-1)


def halves(tensor, core):
    width = tensor.shape[-1] // 2
    return (
        lax.dynamic_slice_in_dim(tensor, core * width, width, axis=-1),
        lax.dynamic_slice_in_dim(tensor, (1 - core) * width, width, axis=-1),
    )


class Split:
    def __init__(self, mine, other, core):
        self.mine, self.other, self.core = mine, other, core

    def apply(self, rows):
        return join(matmul(rows, self.mine), matmul(rows, self.other), self.core)

    def back(self, grad):
        grad_mine, grad_other = halves(grad, self.core)
        return outer_cols(grad_mine, self.mine) + outer_cols(grad_other, self.other)

    def grad(self, rows, grad):
        grad_mine, grad_other = halves(grad, self.core)
        return (inner_rows(rows, grad_mine), inner_rows(rows, grad_other))


def fetch_split(local, gather_axis, core):
    width = local.shape[-1] // 2
    part = lax.dynamic_slice_in_dim(local, core * width, width, axis=-1)
    mine = lax.all_gather(part, "fsdp", axis=gather_axis, tiled=True)
    return mine, swap_core(mine)


def reduce_split(mine_part, other_part, scatter_axis, core):
    received = swap_core(other_part.astype(jnp.bfloat16)).astype(jnp.float32)
    chip = (mine_part + received).astype(jnp.bfloat16)
    owned = lax.psum_scatter(chip, "fsdp", scatter_dimension=scatter_axis, tiled=True)
    summed = lax.psum(owned, "y").astype(jnp.float32)
    return join(summed, swap_core(summed), core)


def fetch_small(modulation, gains, biases, ffn_bias):
    width = modulation.shape[1]
    length = ffn_bias.shape[0]
    rows = -(-length // width)
    padded = jnp.pad(ffn_bias, (0, rows * width - length)).reshape(rows, width)
    packed = jnp.concatenate([modulation, gains, biases, padded], axis=0)
    full = lax.all_gather(packed, "fsdp", axis=1, tiled=True)
    shards = full.shape[1] // width
    bias_rows = full[21:].reshape(rows, shards, width).transpose(1, 0, 2)
    bias_full = bias_rows.reshape(shards, rows * width)[:, :length].reshape(shards * length)
    return full[:6], full[6:11], full[11:21], bias_full


def reduce_small(grad_mod, grad_gains, grad_biases, grad_ffn_bias, grad_time, width, length):
    rows = -(-length // width)
    shards = grad_mod.shape[1] // width
    bias_rows = jnp.pad(grad_ffn_bias.reshape(shards, length), ((0, 0), (0, rows * width - length)))
    bias_rows = bias_rows.reshape(shards, rows, width).transpose(1, 0, 2).reshape(rows, shards * width)
    packed = jnp.concatenate([grad_mod, grad_gains, grad_biases, bias_rows], axis=0)
    owned = lax.psum_scatter(packed, "fsdp", scatter_dimension=1, tiled=True)
    flat = jnp.concatenate([owned.reshape(-1), grad_time.reshape(-1)])
    summed = lax.psum(flat, SEQ)
    owned = summed[: owned.size].reshape(owned.shape)
    grad_time = summed[owned.size :].reshape(grad_time.shape)
    bias_owned = owned[21:].reshape(-1)[:length]
    return owned[:6], owned[6:11], owned[11:21], bias_owned, grad_time


def micro_step(weights, hidden, text, time_emb, places, cotangent):
    modulation, self_q, self_k, self_v, self_o, cross_q, cross_k, cross_v, cross_o, ffn_in, ffn_out, gains, biases, ffn_bias = (
        weights
    )
    gain_rows = gains.astype(jnp.float32)
    bias_rows = biases.astype(jnp.float32)
    modulated = modulation.astype(jnp.float32) + time_emb.astype(jnp.float32)
    cosine, signed_sine = rotary_tables(places, HEAD, HEADS)
    residual_in = hidden.astype(jnp.float32)
    normed_full, pull_first = jax.vjp(modulate_norm, residual_in, modulated[0], modulated[1])
    normed = normed_full.astype(jnp.bfloat16)
    query_pre = self_q.apply(normed) + bias_rows[0]
    key_pre = self_k.apply(normed) + bias_rows[1]
    value_low = (self_v.apply(normed) + bias_rows[2]).astype(jnp.bfloat16)

    def turn_both(query_input, key_input, gain_query, gain_key):
        return (
            rotate(rms_norm(query_input, gain_query), cosine, signed_sine),
            rotate(rms_norm(key_input, gain_key), cosine, signed_sine),
        )

    turned, pull_turn = jax.vjp(turn_both, query_pre, key_pre, gain_rows[0], gain_rows[1])
    query_heads, key_heads, value_heads = (
        lax.all_to_all(turned[0].astype(jnp.bfloat16), SEQ, split_axis=1, concat_axis=0, tiled=True),
        lax.all_to_all(turned[1].astype(jnp.bfloat16), SEQ, split_axis=1, concat_axis=0, tiled=True),
        lax.all_to_all(value_low, SEQ, split_axis=1, concat_axis=0, tiled=True),
    )
    attn_heads, log_total = attend(query_heads, key_heads, value_heads)
    attended = lax.all_to_all(attn_heads, SEQ, split_axis=0, concat_axis=1, tiled=True)
    branch = self_o.apply(attended) + bias_rows[3]
    after_attn = residual_in + branch * modulated[2]
    crossed_full, pull_cross = jax.vjp(affine_norm, after_attn, gain_rows[4], bias_rows[8])
    crossed = crossed_full.astype(jnp.bfloat16)
    cross_query_pre = cross_q.apply(crossed) + bias_rows[4]
    cross_query_full, pull_cross_query = jax.vjp(rms_norm, cross_query_pre, gain_rows[2])
    cross_query = cross_query_full.astype(jnp.bfloat16)
    text_key_pre = cross_k.apply(text) + bias_rows[5]
    text_key_full, pull_text_key = jax.vjp(rms_norm, text_key_pre, gain_rows[3])
    text_value = (cross_v.apply(text) + bias_rows[6]).astype(jnp.bfloat16)
    key_all, value_all = (
        lax.all_gather(text_key_full.astype(jnp.bfloat16), SEQ, axis=0, tiled=True),
        lax.all_gather(text_value, SEQ, axis=0, tiled=True),
    )
    cross_rows, cross_total = attend(cross_query, key_all, value_all)
    second = after_attn + cross_o.apply(cross_rows) + bias_rows[7]
    ffn_normed_full, pull_second = jax.vjp(modulate_norm, second, modulated[3], modulated[4])
    ffn_normed = ffn_normed_full.astype(jnp.bfloat16)
    pre_act = ffn_in.apply(ffn_normed) + ffn_bias.astype(jnp.float32)
    activation_full, pull_gelu = jax.vjp(gelu_tanh, pre_act)
    activation = activation_full.astype(jnp.bfloat16)
    ffn_branch = ffn_out.apply(activation) + bias_rows[9]
    mixed = (second + ffn_branch * modulated[5]).astype(jnp.bfloat16)
    grad_output = cotangent.astype(jnp.float32)
    gate_ffn = jnp.sum(grad_output * ffn_branch, axis=0)
    grad_ffn_branch = (grad_output * modulated[5]).astype(jnp.bfloat16)
    weight_ffn_out = ffn_out.grad(activation, grad_ffn_branch)
    grad_pre_full = pull_gelu(ffn_out.back(grad_ffn_branch))[0]
    grad_pre = grad_pre_full.astype(jnp.bfloat16)
    weight_ffn_in = ffn_in.grad(ffn_normed, grad_pre)
    grad_second_part, shift_ffn, scale_ffn = pull_second(ffn_in.back(grad_pre))
    grad_second = grad_output + grad_second_part
    grad_cross_branch = grad_second.astype(jnp.bfloat16)
    weight_cross_out = cross_o.grad(cross_rows, grad_cross_branch)
    grad_cross_rows = cross_o.back(grad_cross_branch).astype(jnp.bfloat16)
    grad_cross_query, grad_key_all, grad_value_all = attend_back(
        cross_query, key_all, value_all, cross_total, grad_cross_rows
    )
    grad_text_key, grad_text_value_full = (
        lax.psum_scatter(
            grad_key_all.astype(jnp.bfloat16), SEQ, scatter_dimension=0, tiled=True
        ).astype(jnp.float32),
        lax.psum_scatter(
            grad_value_all.astype(jnp.bfloat16), SEQ, scatter_dimension=0, tiled=True
        ).astype(jnp.float32),
    )
    grad_text_value = grad_text_value_full.astype(jnp.bfloat16)
    grad_text_key_full, gain_cross_key = pull_text_key(grad_text_key)
    grad_text_key_pre = grad_text_key_full.astype(jnp.bfloat16)
    weight_cross_key = cross_k.grad(text, grad_text_key_pre)
    weight_cross_value = cross_v.grad(text, grad_text_value)
    grad_words = cross_k.back(grad_text_key_pre) + cross_v.back(grad_text_value)
    grad_cross_query_full, gain_cross_query = pull_cross_query(grad_cross_query)
    grad_cross_query_pre = grad_cross_query_full.astype(jnp.bfloat16)
    weight_cross_query = cross_q.grad(crossed, grad_cross_query_pre)
    grad_after_part, gain_norm, bias_norm = pull_cross(cross_q.back(grad_cross_query_pre))
    grad_after = grad_second + grad_after_part
    gate_attn = jnp.sum(grad_after * branch, axis=0)
    grad_branch = (grad_after * modulated[2]).astype(jnp.bfloat16)
    weight_self_out = self_o.grad(attended, grad_branch)
    grad_attended = self_o.back(grad_branch).astype(jnp.bfloat16)
    grad_attn_heads = lax.all_to_all(grad_attended, SEQ, split_axis=1, concat_axis=0, tiled=True)
    grad_query_heads, grad_key_heads, grad_value_heads = attend_back(
        query_heads, key_heads, value_heads, log_total, grad_attn_heads
    )
    grad_query_turned, grad_key_turned, grad_value = (
        lax.all_to_all(
            grad_query_heads.astype(jnp.bfloat16), SEQ, split_axis=0, concat_axis=1, tiled=True
        ),
        lax.all_to_all(
            grad_key_heads.astype(jnp.bfloat16), SEQ, split_axis=0, concat_axis=1, tiled=True
        ),
        lax.all_to_all(
            grad_value_heads.astype(jnp.bfloat16), SEQ, split_axis=0, concat_axis=1, tiled=True
        ),
    )
    grad_query_full, grad_key_full, gain_query, gain_key = pull_turn(
        (grad_query_turned.astype(jnp.float32), grad_key_turned.astype(jnp.float32))
    )
    grad_query_pre = grad_query_full.astype(jnp.bfloat16)
    grad_key_pre = grad_key_full.astype(jnp.bfloat16)
    weight_self_query = self_q.grad(normed, grad_query_pre)
    weight_self_key = self_k.grad(normed, grad_key_pre)
    weight_self_value = self_v.grad(normed, grad_value)
    grad_normed = self_q.back(grad_query_pre) + self_k.back(grad_key_pre) + self_v.back(grad_value)
    grad_start, shift_attn, scale_attn = pull_first(grad_normed)
    grad_hidden = grad_after + grad_start
    grad_modulated = jnp.stack((shift_attn, scale_attn, gate_attn, shift_ffn, scale_ffn, gate_ffn))
    grad_gains = jnp.stack((gain_query, gain_key, gain_cross_query, gain_cross_key, gain_norm))
    grad_biases = jnp.stack(
        (
            column_sums(grad_query_pre),
            column_sums(grad_key_pre),
            column_sums(grad_value),
            column_sums(grad_branch),
            column_sums(grad_cross_query_pre),
            column_sums(grad_text_key_pre),
            column_sums(grad_text_value),
            column_sums(grad_cross_branch),
            bias_norm,
            column_sums(grad_ffn_branch),
        )
    )
    small = (grad_modulated, grad_gains, grad_biases, column_sums(grad_pre))
    split = tuple(
        jnp.stack(parts) if len(parts) > 1 else parts[0]
        for parts in (
            tuple(w[0] for w in (weight_self_query, weight_self_key, weight_self_value)),
            tuple(w[1] for w in (weight_self_query, weight_self_key, weight_self_value)),
            (weight_self_out[0],),
            (weight_self_out[1],),
            tuple(w[0] for w in (weight_cross_query, weight_cross_key, weight_cross_value)),
            tuple(w[1] for w in (weight_cross_query, weight_cross_key, weight_cross_value)),
            (weight_cross_out[0],),
            (weight_cross_out[1],),
            (weight_ffn_in[0],),
            (weight_ffn_in[1],),
            (weight_ffn_out[0],),
            (weight_ffn_out[1],),
        )
    )
    return (mixed, grad_hidden, grad_words, grad_modulated, small, split)


def body(
    hidden,
    text,
    time_emb,
    modulation,
    self_in,
    self_out,
    cross_in,
    cross_out,
    ffn_in,
    ffn_out,
    gains,
    biases,
    ffn_bias,
    positions,
    cotangent,
):
    core = lax.axis_index("core")
    width = modulation.shape[1]
    length = ffn_bias.shape[0]
    self_in_mine, self_in_other = fetch_split(self_in, 1, core)
    self_out_mine, self_out_other = fetch_split(self_out, 0, core)
    cross_in_mine, cross_in_other = fetch_split(cross_in, 1, core)
    cross_out_mine, cross_out_other = fetch_split(cross_out, 0, core)
    ffn_in_mine, ffn_in_other = fetch_split(ffn_in, 0, core)
    ffn_out_mine, ffn_out_other = fetch_split(ffn_out, 0, core)
    modulation_full, gains_full, biases_full, ffn_bias_full = fetch_small(modulation, gains, biases, ffn_bias)
    weights = (
        modulation_full,
        Split(self_in_mine[0], self_in_other[0], core),
        Split(self_in_mine[1], self_in_other[1], core),
        Split(self_in_mine[2], self_in_other[2], core),
        Split(self_out_mine, self_out_other, core),
        Split(cross_in_mine[0], cross_in_other[0], core),
        Split(cross_in_mine[1], cross_in_other[1], core),
        Split(cross_in_mine[2], cross_in_other[2], core),
        Split(cross_out_mine, cross_out_other, core),
        Split(ffn_in_mine, ffn_in_other, core),
        Split(ffn_out_mine, ffn_out_other, core),
        gains_full,
        biases_full,
        ffn_bias_full,
    )
    mixed_list = []
    hidden_list = []
    words_list = []
    clock_list = []
    small_totals = None
    split_totals = None
    for batch_index in range(hidden.shape[0]):
        mixed, grad_hidden, grad_words, grad_clock, small, split = micro_step(
            weights,
            hidden[batch_index],
            text[batch_index],
            time_emb[batch_index],
            positions[batch_index],
            cotangent[batch_index],
        )
        mixed_list.append(mixed)
        hidden_list.append(grad_hidden)
        words_list.append(grad_words)
        clock_list.append(grad_clock)
        if small_totals is None:
            small_totals, split_totals = small, split
        else:
            small_totals = tuple(a + b for a, b in zip(small_totals, small))
            split_totals = tuple(a + b for a, b in zip(split_totals, split))
    grad_time = jnp.stack(clock_list)
    finals = [
        reduce_split(split_totals[2 * i], split_totals[2 * i + 1], axis, core)
        for i, axis in enumerate((1, 0, 1, 0, 0, 0))
    ]
    grad_mod, grad_gains, grad_biases, grad_ffn_bias, grad_time = reduce_small(
        *small_totals, grad_time, width, length
    )
    return (
        jnp.stack(mixed_list),
        jnp.stack(hidden_list),
        jnp.stack(words_list),
        grad_time,
        grad_mod,
        finals[0],
        finals[1],
        finals[2],
        finals[3],
        finals[4],
        finals[5],
        grad_gains,
        grad_biases,
        grad_ffn_bias,
    )


def solution(mesh):
    devices = mesh.devices
    split_mesh = Mesh(
        devices.reshape(devices.shape[0] // 2, 2, devices.shape[1]), ("y", "core", "fsdp")
    )
    return jax.shard_map(
        body,
        mesh=split_mesh,
        in_specs=(
            P("fsdp", SEQ, None),
            P("fsdp", SEQ, None),
            P("fsdp", None, None),
            P(None, "fsdp"),
            P(None, "fsdp", None),
            P("fsdp", None),
            P(None, "fsdp", None),
            P("fsdp", None),
            P("fsdp", None),
            P("fsdp", None),
            P(None, "fsdp"),
            P(None, "fsdp"),
            P("fsdp"),
            P("fsdp", None, SEQ),
            P("fsdp", SEQ, None),
        ),
        out_specs=(
            P("fsdp", SEQ, None),
            P("fsdp", SEQ, None),
            P("fsdp", SEQ, None),
            P("fsdp", None, None),
            P(None, "fsdp"),
            P(None, "fsdp", None),
            P("fsdp", None),
            P(None, "fsdp", None),
            P("fsdp", None),
            P("fsdp", None),
            P("fsdp", None),
            P(None, "fsdp"),
            P(None, "fsdp"),
            P("fsdp"),
        ),
        check_vma=False,
    )
```

```python
import jax
import jax.numpy as jnp
from jax import lax
from jax.sharding import Mesh, PartitionSpec as P

HEADS = 12
HEAD = 128


EPSILON = 1e-06
SEQ = ("y", "core")
SWAP = [(0, 1), (1, 0)]


def matmul(operand, factor):
    return jnp.dot(operand, factor, preferred_element_type=jnp.float32)


def inner_rows(operand, factor):
    return lax.dot_general(
        operand, factor, (((0,), (0,)), ((), ())), preferred_element_type=jnp.float32
    )


def outer_cols(operand, factor):
    return lax.dot_general(
        operand, factor, (((1,), (1,)), ((), ())), preferred_element_type=jnp.float32
    )


def column_sums(tensor):
    return jnp.sum(tensor.astype(jnp.float32), axis=0)


def layer_norm(tensor):
    centered = tensor - jnp.mean(tensor, axis=-1, keepdims=True)
    return centered * lax.rsqrt(jnp.mean(centered * centered, axis=-1, keepdims=True) + EPSILON)


def rms_norm(tensor, weight):
    return tensor * lax.rsqrt(jnp.mean(tensor * tensor, axis=-1, keepdims=True) + EPSILON) * weight


def modulate_norm(tensor, shift, scale):
    return layer_norm(tensor) * (1.0 + scale) + shift


def affine_norm(tensor, weight, offset):
    return layer_norm(tensor) * weight + offset


def gelu_tanh(tensor):
    return jax.nn.gelu(tensor, approximate=True)


def rotary_tables(places, head_size, head_count):
    one_sixth = head_size // 6
    span_sizes = (head_size - 4 * one_sixth, 2 * one_sixth, 2 * one_sixth)
    angles = []
    for component in range(3):
        exponents = (
            jnp.arange(0, span_sizes[component], 2, dtype=jnp.float32) / span_sizes[component]
        )
        frequency = 1.0 / 10000.0**exponents
        angles.append(places[component].astype(jnp.float32)[:, None] * frequency[None, :])
    joined = jnp.concatenate(angles, axis=1)
    tiled_angles = jnp.tile(jnp.repeat(joined, 2, axis=1), (1, head_count))
    parity = jnp.where(jnp.arange(tiled_angles.shape[1]) % 2 == 0, -1.0, 1.0)
    return (jnp.cos(tiled_angles), jnp.sin(tiled_angles) * parity)


def rotate(tensor, cosine, signed_sine):
    even_lane = jnp.arange(tensor.shape[1]) % 2 == 0
    swapped = jnp.where(even_lane, jnp.roll(tensor, -1, axis=1), jnp.roll(tensor, 1, axis=1))
    return tensor * cosine + swapped * signed_sine


def split_heads(tensor):
    return tensor.reshape(tensor.shape[0], tensor.shape[1] // HEAD, HEAD)


def attend(queries, key_rows, value_rows):
    scores = jnp.einsum(
        "qhd,khd->hqk",
        split_heads(queries),
        split_heads(key_rows),
        preferred_element_type=jnp.float32,
    ) * HEAD ** (-0.5)
    row_max = jnp.max(scores, axis=-1, keepdims=True)
    exponentials = jnp.exp(scores - row_max)
    row_total = jnp.sum(exponentials, axis=-1, keepdims=True)
    probabilities = (exponentials / row_total).astype(jnp.bfloat16)
    result = jnp.einsum(
        "hqk,khd->qhd", probabilities, split_heads(value_rows), preferred_element_type=jnp.float32
    )
    return (result.reshape(queries.shape[0], -1).astype(jnp.bfloat16), row_max + jnp.log(row_total))


def attend_back(queries, key_rows, value_rows, log_total, grad_rows):
    query_split = split_heads(queries)
    key_split = split_heads(key_rows)
    grad_split = split_heads(grad_rows)
    scale_factor = HEAD ** (-0.5)
    scores = (
        jnp.einsum("qhd,khd->hqk", query_split, key_split, preferred_element_type=jnp.float32)
        * scale_factor
    )
    probs_full = jnp.exp(scores - log_total)
    probs_low = probs_full.astype(jnp.bfloat16)
    grad_values = jnp.einsum(
        "hqk,qhd->khd", probs_low, grad_split, preferred_element_type=jnp.float32
    )
    grad_probs = jnp.einsum(
        "qhd,khd->hqk", grad_split, split_heads(value_rows), preferred_element_type=jnp.float32
    )
    grad_scores = (
        probs_full * (grad_probs - jnp.sum(grad_probs * probs_full, axis=-1, keepdims=True))
    ).astype(jnp.bfloat16)
    grad_queries = (
        jnp.einsum("hqk,khd->qhd", grad_scores, key_split, preferred_element_type=jnp.float32)
        * scale_factor
    )
    grad_keys = (
        jnp.einsum("hqk,qhd->khd", grad_scores, query_split, preferred_element_type=jnp.float32)
        * scale_factor
    )
    return (
        grad_queries.reshape(queries.shape[0], -1),
        grad_keys.reshape(key_rows.shape[0], -1),
        grad_values.reshape(value_rows.shape[0], -1),
    )


def swap_core(tensor):
    return lax.ppermute(tensor, "core", SWAP)


def join(mine, other, core):
    width = mine.shape[-1]
    both = jnp.concatenate([other, mine, other], axis=-1)
    return lax.dynamic_slice_in_dim(both, (1 - core) * width, 2 * width, axis=-1)


def halves(tensor, core):
    width = tensor.shape[-1] // 2
    return (
        lax.dynamic_slice_in_dim(tensor, core * width, width, axis=-1),
        lax.dynamic_slice_in_dim(tensor, (1 - core) * width, width, axis=-1),
    )


def swap_y(tensor):
    return lax.ppermute(tensor, "y", SWAP)


class Split:
    def __init__(self, parts, spot):
        self.parts, self.spot = parts, spot

    def apply(self, rows):
        y, core = self.spot
        own, y_part, core_part, cross_part = (matmul(rows, part) for part in self.parts)
        return join(join(own, y_part, y), join(core_part, cross_part, y), core)

    def quarters(self, grad):
        y, core = self.spot
        grad_mine, grad_other = halves(grad, core)
        return halves(grad_mine, y) + halves(grad_other, y)

    def back(self, grad):
        pieces = [outer_cols(g, part) for g, part in zip(self.quarters(grad), self.parts)]
        return (pieces[0] + pieces[1]) + (pieces[2] + pieces[3])

    def grad(self, rows, grad):
        return tuple(inner_rows(rows, g) for g in self.quarters(grad))


def fetch_split(local, gather_axis, spot):
    y, core = spot
    width = local.shape[-1] // 4
    part = lax.dynamic_slice_in_dim(local, (2 * core + y) * width, width, axis=-1)
    own = lax.all_gather(part, "fsdp", axis=gather_axis, tiled=True)
    y_part = swap_y(own)
    return (own, y_part, swap_core(own), swap_core(y_part))


def reduce_split(parts, scatter_axis, spot):
    y, core = spot
    own, y_part, core_part, cross_part = parts
    from_core = swap_core(core_part.astype(jnp.bfloat16)).astype(jnp.float32)
    from_cross = swap_core(cross_part.astype(jnp.bfloat16)).astype(jnp.float32)
    chip_own = own + from_core
    chip_y = (y_part + from_cross).astype(jnp.bfloat16)
    total = (chip_own + swap_y(chip_y).astype(jnp.float32)).astype(jnp.bfloat16)
    owned = lax.psum_scatter(total, "fsdp", scatter_dimension=scatter_axis, tiled=True)
    owned_y = swap_y(owned)
    mine = join(owned, owned_y, y)
    return join(mine, swap_core(mine), core).astype(jnp.float32)


def fetch_small(modulation, gains, biases, ffn_bias):
    width = modulation.shape[1]
    length = ffn_bias.shape[0]
    rows = -(-length // width)
    padded = jnp.pad(ffn_bias, (0, rows * width - length)).reshape(rows, width)
    packed = jnp.concatenate([modulation, gains, biases, padded], axis=0)
    full = lax.all_gather(packed, "fsdp", axis=1, tiled=True)
    shards = full.shape[1] // width
    bias_rows = full[21:].reshape(rows, shards, width).transpose(1, 0, 2)
    bias_full = bias_rows.reshape(shards, rows * width)[:, :length].reshape(shards * length)
    return full[:6], full[6:11], full[11:21], bias_full


def reduce_small(grad_mod, grad_gains, grad_biases, grad_ffn_bias, grad_time, width, length):
    rows = -(-length // width)
    shards = grad_mod.shape[1] // width
    bias_rows = jnp.pad(grad_ffn_bias.reshape(shards, length), ((0, 0), (0, rows * width - length)))
    bias_rows = bias_rows.reshape(shards, rows, width).transpose(1, 0, 2).reshape(rows, shards * width)
    packed = jnp.concatenate([grad_mod, grad_gains, grad_biases, bias_rows], axis=0)
    owned = lax.psum_scatter(packed, "fsdp", scatter_dimension=1, tiled=True)
    flat = jnp.concatenate([owned.reshape(-1), grad_time.reshape(-1)])
    summed = lax.psum(flat, SEQ)
    owned = summed[: owned.size].reshape(owned.shape)
    grad_time = summed[owned.size :].reshape(grad_time.shape)
    bias_owned = owned[21:].reshape(-1)[:length]
    return owned[:6], owned[6:11], owned[11:21], bias_owned, grad_time


def micro_step(weights, hidden, text, time_emb, places, cotangent):
    modulation, self_q, self_k, self_v, self_o, cross_q, cross_k, cross_v, cross_o, ffn_in, ffn_out, gains, biases, ffn_bias = (
        weights
    )
    gain_rows = gains.astype(jnp.float32)
    bias_rows = biases.astype(jnp.float32)
    modulated = modulation.astype(jnp.float32) + time_emb.astype(jnp.float32)
    cosine, signed_sine = rotary_tables(places, HEAD, HEADS)
    residual_in = hidden.astype(jnp.float32)
    normed_full, pull_first = jax.vjp(modulate_norm, residual_in, modulated[0], modulated[1])
    normed = normed_full.astype(jnp.bfloat16)
    query_pre = self_q.apply(normed) + bias_rows[0]
    key_pre = self_k.apply(normed) + bias_rows[1]
    value_low = (self_v.apply(normed) + bias_rows[2]).astype(jnp.bfloat16)

    def turn_both(query_input, key_input, gain_query, gain_key):
        return (
            rotate(rms_norm(query_input, gain_query), cosine, signed_sine),
            rotate(rms_norm(key_input, gain_key), cosine, signed_sine),
        )

    turned, pull_turn = jax.vjp(turn_both, query_pre, key_pre, gain_rows[0], gain_rows[1])
    query_heads, key_heads, value_heads = (
        lax.all_to_all(turned[0].astype(jnp.bfloat16), SEQ, split_axis=1, concat_axis=0, tiled=True),
        lax.all_to_all(turned[1].astype(jnp.bfloat16), SEQ, split_axis=1, concat_axis=0, tiled=True),
        lax.all_to_all(value_low, SEQ, split_axis=1, concat_axis=0, tiled=True),
    )
    attn_heads, log_total = attend(query_heads, key_heads, value_heads)
    attended = lax.all_to_all(attn_heads, SEQ, split_axis=0, concat_axis=1, tiled=True)
    branch = self_o.apply(attended) + bias_rows[3]
    after_attn = residual_in + branch * modulated[2]
    crossed_full, pull_cross = jax.vjp(affine_norm, after_attn, gain_rows[4], bias_rows[8])
    crossed = crossed_full.astype(jnp.bfloat16)
    cross_query_pre = cross_q.apply(crossed) + bias_rows[4]
    cross_query_full, pull_cross_query = jax.vjp(rms_norm, cross_query_pre, gain_rows[2])
    cross_query = cross_query_full.astype(jnp.bfloat16)
    text_key_pre = cross_k.apply(text) + bias_rows[5]
    text_key_full, pull_text_key = jax.vjp(rms_norm, text_key_pre, gain_rows[3])
    text_value = (cross_v.apply(text) + bias_rows[6]).astype(jnp.bfloat16)
    key_all, value_all = (
        lax.all_gather(text_key_full.astype(jnp.bfloat16), SEQ, axis=0, tiled=True),
        lax.all_gather(text_value, SEQ, axis=0, tiled=True),
    )
    cross_rows, cross_total = attend(cross_query, key_all, value_all)
    second = after_attn + cross_o.apply(cross_rows) + bias_rows[7]
    ffn_normed_full, pull_second = jax.vjp(modulate_norm, second, modulated[3], modulated[4])
    ffn_normed = ffn_normed_full.astype(jnp.bfloat16)
    pre_act = ffn_in.apply(ffn_normed) + ffn_bias.astype(jnp.float32)
    activation_full, pull_gelu = jax.vjp(gelu_tanh, pre_act)
    activation = activation_full.astype(jnp.bfloat16)
    ffn_branch = ffn_out.apply(activation) + bias_rows[9]
    mixed = (second + ffn_branch * modulated[5]).astype(jnp.bfloat16)
    grad_output = cotangent.astype(jnp.float32)
    gate_ffn = jnp.sum(grad_output * ffn_branch, axis=0)
    grad_ffn_branch = (grad_output * modulated[5]).astype(jnp.bfloat16)
    weight_ffn_out = ffn_out.grad(activation, grad_ffn_branch)
    grad_pre_full = pull_gelu(ffn_out.back(grad_ffn_branch))[0]
    grad_pre = grad_pre_full.astype(jnp.bfloat16)
    weight_ffn_in = ffn_in.grad(ffn_normed, grad_pre)
    grad_second_part, shift_ffn, scale_ffn = pull_second(ffn_in.back(grad_pre))
    grad_second = grad_output + grad_second_part
    grad_cross_branch = grad_second.astype(jnp.bfloat16)
    weight_cross_out = cross_o.grad(cross_rows, grad_cross_branch)
    grad_cross_rows = cross_o.back(grad_cross_branch).astype(jnp.bfloat16)
    grad_cross_query, grad_key_all, grad_value_all = attend_back(
        cross_query, key_all, value_all, cross_total, grad_cross_rows
    )
    grad_text_key, grad_text_value_full = (
        lax.psum_scatter(
            grad_key_all.astype(jnp.bfloat16), SEQ, scatter_dimension=0, tiled=True
        ).astype(jnp.float32),
        lax.psum_scatter(
            grad_value_all.astype(jnp.bfloat16), SEQ, scatter_dimension=0, tiled=True
        ).astype(jnp.float32),
    )
    grad_text_value = grad_text_value_full.astype(jnp.bfloat16)
    grad_text_key_full, gain_cross_key = pull_text_key(grad_text_key)
    grad_text_key_pre = grad_text_key_full.astype(jnp.bfloat16)
    weight_cross_key = cross_k.grad(text, grad_text_key_pre)
    weight_cross_value = cross_v.grad(text, grad_text_value)
    grad_words = cross_k.back(grad_text_key_pre) + cross_v.back(grad_text_value)
    grad_cross_query_full, gain_cross_query = pull_cross_query(grad_cross_query)
    grad_cross_query_pre = grad_cross_query_full.astype(jnp.bfloat16)
    weight_cross_query = cross_q.grad(crossed, grad_cross_query_pre)
    grad_after_part, gain_norm, bias_norm = pull_cross(cross_q.back(grad_cross_query_pre))
    grad_after = grad_second + grad_after_part
    gate_attn = jnp.sum(grad_after * branch, axis=0)
    grad_branch = (grad_after * modulated[2]).astype(jnp.bfloat16)
    weight_self_out = self_o.grad(attended, grad_branch)
    grad_attended = self_o.back(grad_branch).astype(jnp.bfloat16)
    grad_attn_heads = lax.all_to_all(grad_attended, SEQ, split_axis=1, concat_axis=0, tiled=True)
    grad_query_heads, grad_key_heads, grad_value_heads = attend_back(
        query_heads, key_heads, value_heads, log_total, grad_attn_heads
    )
    grad_query_turned, grad_key_turned, grad_value = (
        lax.all_to_all(
            grad_query_heads.astype(jnp.bfloat16), SEQ, split_axis=0, concat_axis=1, tiled=True
        ),
        lax.all_to_all(
            grad_key_heads.astype(jnp.bfloat16), SEQ, split_axis=0, concat_axis=1, tiled=True
        ),
        lax.all_to_all(
            grad_value_heads.astype(jnp.bfloat16), SEQ, split_axis=0, concat_axis=1, tiled=True
        ),
    )
    grad_query_full, grad_key_full, gain_query, gain_key = pull_turn(
        (grad_query_turned.astype(jnp.float32), grad_key_turned.astype(jnp.float32))
    )
    grad_query_pre = grad_query_full.astype(jnp.bfloat16)
    grad_key_pre = grad_key_full.astype(jnp.bfloat16)
    weight_self_query = self_q.grad(normed, grad_query_pre)
    weight_self_key = self_k.grad(normed, grad_key_pre)
    weight_self_value = self_v.grad(normed, grad_value)
    grad_normed = self_q.back(grad_query_pre) + self_k.back(grad_key_pre) + self_v.back(grad_value)
    grad_start, shift_attn, scale_attn = pull_first(grad_normed)
    grad_hidden = grad_after + grad_start
    grad_modulated = jnp.stack((shift_attn, scale_attn, gate_attn, shift_ffn, scale_ffn, gate_ffn))
    grad_gains = jnp.stack((gain_query, gain_key, gain_cross_query, gain_cross_key, gain_norm))
    grad_biases = jnp.stack(
        (
            column_sums(grad_query_pre),
            column_sums(grad_key_pre),
            column_sums(grad_value),
            column_sums(grad_branch),
            column_sums(grad_cross_query_pre),
            column_sums(grad_text_key_pre),
            column_sums(grad_text_value),
            column_sums(grad_cross_branch),
            bias_norm,
            column_sums(grad_ffn_branch),
        )
    )
    small = (grad_modulated, grad_gains, grad_biases, column_sums(grad_pre))
    stacked = []
    for group in (
        (weight_self_query, weight_self_key, weight_self_value),
        (weight_self_out,),
        (weight_cross_query, weight_cross_key, weight_cross_value),
        (weight_cross_out,),
        (weight_ffn_in,),
        (weight_ffn_out,),
    ):
        for quarter in range(4):
            parts = tuple(w[quarter] for w in group)
            stacked.append(jnp.stack(parts) if len(parts) > 1 else parts[0])
    split = tuple(stacked)
    return (mixed, grad_hidden, grad_words, grad_modulated, small, split)


def body(
    hidden,
    text,
    time_emb,
    modulation,
    self_in,
    self_out,
    cross_in,
    cross_out,
    ffn_in,
    ffn_out,
    gains,
    biases,
    ffn_bias,
    positions,
    cotangent,
):
    spot = (lax.axis_index("y"), lax.axis_index("core"))
    width = modulation.shape[1]
    length = ffn_bias.shape[0]
    self_in_parts = fetch_split(self_in, 1, spot)
    self_out_parts = fetch_split(self_out, 0, spot)
    cross_in_parts = fetch_split(cross_in, 1, spot)
    cross_out_parts = fetch_split(cross_out, 0, spot)
    ffn_in_parts = fetch_split(ffn_in, 0, spot)
    ffn_out_parts = fetch_split(ffn_out, 0, spot)
    modulation_full, gains_full, biases_full, ffn_bias_full = fetch_small(modulation, gains, biases, ffn_bias)
    weights = (
        modulation_full,
        Split(tuple(part[0] for part in self_in_parts), spot),
        Split(tuple(part[1] for part in self_in_parts), spot),
        Split(tuple(part[2] for part in self_in_parts), spot),
        Split(self_out_parts, spot),
        Split(tuple(part[0] for part in cross_in_parts), spot),
        Split(tuple(part[1] for part in cross_in_parts), spot),
        Split(tuple(part[2] for part in cross_in_parts), spot),
        Split(cross_out_parts, spot),
        Split(ffn_in_parts, spot),
        Split(ffn_out_parts, spot),
        gains_full,
        biases_full,
        ffn_bias_full,
    )
    mixed_list = []
    hidden_list = []
    words_list = []
    clock_list = []
    small_totals = None
    split_totals = None
    for batch_index in range(hidden.shape[0]):
        mixed, grad_hidden, grad_words, grad_clock, small, split = micro_step(
            weights,
            hidden[batch_index],
            text[batch_index],
            time_emb[batch_index],
            positions[batch_index],
            cotangent[batch_index],
        )
        mixed_list.append(mixed)
        hidden_list.append(grad_hidden)
        words_list.append(grad_words)
        clock_list.append(grad_clock)
        if small_totals is None:
            small_totals, split_totals = small, split
        else:
            small_totals = tuple(a + b for a, b in zip(small_totals, small))
            split_totals = tuple(a + b for a, b in zip(split_totals, split))
    grad_time = jnp.stack(clock_list)
    finals = [
        reduce_split(split_totals[4 * i : 4 * i + 4], axis, spot)
        for i, axis in enumerate((1, 0, 1, 0, 0, 0))
    ]
    grad_mod, grad_gains, grad_biases, grad_ffn_bias, grad_time = reduce_small(
        *small_totals, grad_time, width, length
    )
    return (
        jnp.stack(mixed_list),
        jnp.stack(hidden_list),
        jnp.stack(words_list),
        grad_time,
        grad_mod,
        finals[0],
        finals[1],
        finals[2],
        finals[3],
        finals[4],
        finals[5],
        grad_gains,
        grad_biases,
        grad_ffn_bias,
    )


def solution(mesh):
    devices = mesh.devices
    split_mesh = Mesh(
        devices.reshape(devices.shape[0] // 2, 2, devices.shape[1]), ("y", "core", "fsdp")
    )
    return jax.shard_map(
        body,
        mesh=split_mesh,
        in_specs=(
            P("fsdp", SEQ, None),
            P("fsdp", SEQ, None),
            P("fsdp", None, None),
            P(None, "fsdp"),
            P(None, "fsdp", None),
            P("fsdp", None),
            P(None, "fsdp", None),
            P("fsdp", None),
            P("fsdp", None),
            P("fsdp", None),
            P(None, "fsdp"),
            P(None, "fsdp"),
            P("fsdp"),
            P("fsdp", None, SEQ),
            P("fsdp", SEQ, None),
        ),
        out_specs=(
            P("fsdp", SEQ, None),
            P("fsdp", SEQ, None),
            P("fsdp", SEQ, None),
            P("fsdp", None, None),
            P(None, "fsdp"),
            P(None, "fsdp", None),
            P("fsdp", None),
            P(None, "fsdp", None),
            P("fsdp", None),
            P("fsdp", None),
            P("fsdp", None),
            P(None, "fsdp"),
            P(None, "fsdp"),
            P("fsdp"),
        ),
        check_vma=False,
    )
```

```python
import jax
import jax.numpy as jnp
from jax import lax
from jax.sharding import Mesh, PartitionSpec as P

HEADS = 12
HEAD = 128


EPSILON = 1e-06
SEQ = ("y", "core")
SWAP = [(0, 1), (1, 0)]


def matmul(operand, factor):
    return jnp.dot(operand, factor, preferred_element_type=jnp.float32)


def inner_rows(operand, factor):
    return lax.dot_general(
        operand, factor, (((0,), (0,)), ((), ())), preferred_element_type=jnp.float32
    )


def outer_cols(operand, factor):
    return lax.dot_general(
        operand, factor, (((1,), (1,)), ((), ())), preferred_element_type=jnp.float32
    )


def column_sums(tensor):
    return jnp.sum(tensor.astype(jnp.float32), axis=0)


def layer_norm(tensor):
    centered = tensor - jnp.mean(tensor, axis=-1, keepdims=True)
    return centered * lax.rsqrt(jnp.mean(centered * centered, axis=-1, keepdims=True) + EPSILON)


def rms_norm(tensor, weight):
    return tensor * lax.rsqrt(jnp.mean(tensor * tensor, axis=-1, keepdims=True) + EPSILON) * weight


def modulate_norm(tensor, shift, scale):
    return layer_norm(tensor) * (1.0 + scale) + shift


def affine_norm(tensor, weight, offset):
    return layer_norm(tensor) * weight + offset


def gelu_tanh(tensor):
    return jax.nn.gelu(tensor, approximate=True)


def rotary_tables(places, head_size, head_count):
    one_sixth = head_size // 6
    span_sizes = (head_size - 4 * one_sixth, 2 * one_sixth, 2 * one_sixth)
    angles = []
    for component in range(3):
        exponents = (
            jnp.arange(0, span_sizes[component], 2, dtype=jnp.float32) / span_sizes[component]
        )
        frequency = 1.0 / 10000.0**exponents
        angles.append(places[component].astype(jnp.float32)[:, None] * frequency[None, :])
    joined = jnp.concatenate(angles, axis=1)
    tiled_angles = jnp.tile(jnp.repeat(joined, 2, axis=1), (1, head_count))
    parity = jnp.where(jnp.arange(tiled_angles.shape[1]) % 2 == 0, -1.0, 1.0)
    return (jnp.cos(tiled_angles), jnp.sin(tiled_angles) * parity)


def rotate(tensor, cosine, signed_sine):
    even_lane = jnp.arange(tensor.shape[1]) % 2 == 0
    swapped = jnp.where(even_lane, jnp.roll(tensor, -1, axis=1), jnp.roll(tensor, 1, axis=1))
    return tensor * cosine + swapped * signed_sine


def split_heads(tensor):
    return tensor.reshape(tensor.shape[0], tensor.shape[1] // HEAD, HEAD)


def attend(queries, key_rows, value_rows):
    scores = jnp.einsum(
        "qhd,khd->hqk",
        split_heads(queries),
        split_heads(key_rows),
        preferred_element_type=jnp.float32,
    ) * HEAD ** (-0.5)
    row_max = jnp.max(scores, axis=-1, keepdims=True)
    exponentials = jnp.exp(scores - row_max)
    row_total = jnp.sum(exponentials, axis=-1, keepdims=True)
    probabilities = (exponentials / row_total).astype(jnp.bfloat16)
    result = jnp.einsum(
        "hqk,khd->qhd", probabilities, split_heads(value_rows), preferred_element_type=jnp.float32
    )
    return (result.reshape(queries.shape[0], -1).astype(jnp.bfloat16), row_max + jnp.log(row_total))


def attend_back(queries, key_rows, value_rows, log_total, grad_rows):
    query_split = split_heads(queries)
    key_split = split_heads(key_rows)
    grad_split = split_heads(grad_rows)
    scale_factor = HEAD ** (-0.5)
    scores = (
        jnp.einsum("qhd,khd->hqk", query_split, key_split, preferred_element_type=jnp.float32)
        * scale_factor
    )
    probs_full = jnp.exp(scores - log_total)
    probs_low = probs_full.astype(jnp.bfloat16)
    grad_values = jnp.einsum(
        "hqk,qhd->khd", probs_low, grad_split, preferred_element_type=jnp.float32
    )
    grad_probs = jnp.einsum(
        "qhd,khd->hqk", grad_split, split_heads(value_rows), preferred_element_type=jnp.float32
    )
    grad_scores = (
        probs_full * (grad_probs - jnp.sum(grad_probs * probs_full, axis=-1, keepdims=True))
    ).astype(jnp.bfloat16)
    grad_queries = (
        jnp.einsum("hqk,khd->qhd", grad_scores, key_split, preferred_element_type=jnp.float32)
        * scale_factor
    )
    grad_keys = (
        jnp.einsum("hqk,qhd->khd", grad_scores, query_split, preferred_element_type=jnp.float32)
        * scale_factor
    )
    return (
        grad_queries.reshape(queries.shape[0], -1),
        grad_keys.reshape(key_rows.shape[0], -1),
        grad_values.reshape(value_rows.shape[0], -1),
    )


def swap_core(tensor):
    return lax.ppermute(tensor, "core", SWAP)


def join(mine, other, core):
    width = mine.shape[-1]
    both = jnp.concatenate([other, mine, other], axis=-1)
    return lax.dynamic_slice_in_dim(both, (1 - core) * width, 2 * width, axis=-1)


def halves(tensor, core):
    width = tensor.shape[-1] // 2
    return (
        lax.dynamic_slice_in_dim(tensor, core * width, width, axis=-1),
        lax.dynamic_slice_in_dim(tensor, (1 - core) * width, width, axis=-1),
    )


def swap_y(tensor):
    return lax.ppermute(tensor, "y", SWAP)


class Split:
    def __init__(self, parts, spot):
        self.parts, self.spot = parts, spot

    def apply(self, rows):
        y, core = self.spot
        outs = [matmul(rows, part) for part in self.parts]
        if len(outs) == 2:
            return join(outs[0], outs[1], core)
        return join(join(outs[0], outs[1], y), join(outs[2], outs[3], y), core)

    def quarters(self, grad):
        y, core = self.spot
        grad_mine, grad_other = halves(grad, core)
        return halves(grad_mine, y) + halves(grad_other, y)

    def back(self, grad):
        if len(self.parts) == 2:
            grad_mine, grad_other = halves(grad, self.spot[1])
            return outer_cols(grad_mine, self.parts[0]) + outer_cols(grad_other, self.parts[1])
        pieces = [outer_cols(g, part) for g, part in zip(self.quarters(grad), self.parts)]
        return (pieces[0] + pieces[1]) + (pieces[2] + pieces[3])

    def grad(self, rows, grad):
        return tuple(inner_rows(rows, g) for g in self.quarters(grad))


def fetch_split(local, gather_axis, spot, quarters=True):
    y, core = spot
    if not quarters:
        width = local.shape[-1] // 2
        part = lax.dynamic_slice_in_dim(local, core * width, width, axis=-1)
        mine = lax.all_gather(part, "fsdp", axis=gather_axis, tiled=True)
        return (mine, swap_core(mine))
    width = local.shape[-1] // 4
    part = lax.dynamic_slice_in_dim(local, (2 * core + y) * width, width, axis=-1)
    own = lax.all_gather(part, "fsdp", axis=gather_axis, tiled=True)
    y_part = swap_y(own)
    return (own, y_part, swap_core(own), swap_core(y_part))


def reduce_split(parts, scatter_axis, spot):
    y, core = spot
    own, y_part, core_part, cross_part = parts
    from_core = swap_core(core_part.astype(jnp.bfloat16)).astype(jnp.float32)
    from_cross = swap_core(cross_part.astype(jnp.bfloat16)).astype(jnp.float32)
    chip_own = own + from_core
    chip_y = (y_part + from_cross).astype(jnp.bfloat16)
    total = (chip_own + swap_y(chip_y).astype(jnp.float32)).astype(jnp.bfloat16)
    owned = lax.psum_scatter(total, "fsdp", scatter_dimension=scatter_axis, tiled=True)
    owned_y = swap_y(owned)
    mine = join(owned, owned_y, y)
    return join(mine, swap_core(mine), core).astype(jnp.float32)


def fetch_small(modulation, gains, biases, ffn_bias):
    width = modulation.shape[1]
    length = ffn_bias.shape[0]
    rows = -(-length // width)
    padded = jnp.pad(ffn_bias, (0, rows * width - length)).reshape(rows, width)
    packed = jnp.concatenate([modulation, gains, biases, padded], axis=0)
    full = lax.all_gather(packed, "fsdp", axis=1, tiled=True)
    shards = full.shape[1] // width
    bias_rows = full[21:].reshape(rows, shards, width).transpose(1, 0, 2)
    bias_full = bias_rows.reshape(shards, rows * width)[:, :length].reshape(shards * length)
    return full[:6], full[6:11], full[11:21], bias_full


def reduce_small(grad_mod, grad_gains, grad_biases, grad_ffn_bias, grad_time, width, length):
    rows = -(-length // width)
    shards = grad_mod.shape[1] // width
    bias_rows = jnp.pad(grad_ffn_bias.reshape(shards, length), ((0, 0), (0, rows * width - length)))
    bias_rows = bias_rows.reshape(shards, rows, width).transpose(1, 0, 2).reshape(rows, shards * width)
    packed = jnp.concatenate([grad_mod, grad_gains, grad_biases, bias_rows], axis=0)
    owned = lax.psum_scatter(packed, "fsdp", scatter_dimension=1, tiled=True)
    flat = jnp.concatenate([owned.reshape(-1), grad_time.reshape(-1)])
    summed = lax.psum(flat, SEQ)
    owned = summed[: owned.size].reshape(owned.shape)
    grad_time = summed[owned.size :].reshape(grad_time.shape)
    bias_owned = owned[21:].reshape(-1)[:length]
    return owned[:6], owned[6:11], owned[11:21], bias_owned, grad_time


def micro_step(weights, hidden, text, time_emb, places, cotangent):
    modulation, self_q, self_k, self_v, self_o, cross_q, cross_k, cross_v, cross_o, ffn_in, ffn_out, gains, biases, ffn_bias = (
        weights
    )
    gain_rows = gains.astype(jnp.float32)
    bias_rows = biases.astype(jnp.float32)
    modulated = modulation.astype(jnp.float32) + time_emb.astype(jnp.float32)
    cosine, signed_sine = rotary_tables(places, HEAD, HEADS)
    residual_in = hidden.astype(jnp.float32)
    normed_full, pull_first = jax.vjp(modulate_norm, residual_in, modulated[0], modulated[1])
    normed = normed_full.astype(jnp.bfloat16)
    query_pre = self_q.apply(normed) + bias_rows[0]
    key_pre = self_k.apply(normed) + bias_rows[1]
    value_low = (self_v.apply(normed) + bias_rows[2]).astype(jnp.bfloat16)

    def turn_both(query_input, key_input, gain_query, gain_key):
        return (
            rotate(rms_norm(query_input, gain_query), cosine, signed_sine),
            rotate(rms_norm(key_input, gain_key), cosine, signed_sine),
        )

    turned, pull_turn = jax.vjp(turn_both, query_pre, key_pre, gain_rows[0], gain_rows[1])
    query_heads, key_heads, value_heads = (
        lax.all_to_all(turned[0].astype(jnp.bfloat16), SEQ, split_axis=1, concat_axis=0, tiled=True),
        lax.all_to_all(turned[1].astype(jnp.bfloat16), SEQ, split_axis=1, concat_axis=0, tiled=True),
        lax.all_to_all(value_low, SEQ, split_axis=1, concat_axis=0, tiled=True),
    )
    attn_heads, log_total = attend(query_heads, key_heads, value_heads)
    attended = lax.all_to_all(attn_heads, SEQ, split_axis=0, concat_axis=1, tiled=True)
    branch = self_o.apply(attended) + bias_rows[3]
    after_attn = residual_in + branch * modulated[2]
    crossed_full, pull_cross = jax.vjp(affine_norm, after_attn, gain_rows[4], bias_rows[8])
    crossed = crossed_full.astype(jnp.bfloat16)
    cross_query_pre = cross_q.apply(crossed) + bias_rows[4]
    cross_query_full, pull_cross_query = jax.vjp(rms_norm, cross_query_pre, gain_rows[2])
    cross_query = cross_query_full.astype(jnp.bfloat16)
    text_key_pre = cross_k.apply(text) + bias_rows[5]
    text_key_full, pull_text_key = jax.vjp(rms_norm, text_key_pre, gain_rows[3])
    text_value = (cross_v.apply(text) + bias_rows[6]).astype(jnp.bfloat16)
    key_all, value_all = (
        lax.all_gather(text_key_full.astype(jnp.bfloat16), SEQ, axis=0, tiled=True),
        lax.all_gather(text_value, SEQ, axis=0, tiled=True),
    )
    cross_rows, cross_total = attend(cross_query, key_all, value_all)
    second = after_attn + cross_o.apply(cross_rows) + bias_rows[7]
    ffn_normed_full, pull_second = jax.vjp(modulate_norm, second, modulated[3], modulated[4])
    ffn_normed = ffn_normed_full.astype(jnp.bfloat16)
    pre_act = ffn_in.apply(ffn_normed) + ffn_bias.astype(jnp.float32)
    activation_full, pull_gelu = jax.vjp(gelu_tanh, pre_act)
    activation = activation_full.astype(jnp.bfloat16)
    ffn_branch = ffn_out.apply(activation) + bias_rows[9]
    mixed = (second + ffn_branch * modulated[5]).astype(jnp.bfloat16)
    grad_output = cotangent.astype(jnp.float32)
    gate_ffn = jnp.sum(grad_output * ffn_branch, axis=0)
    grad_ffn_branch = (grad_output * modulated[5]).astype(jnp.bfloat16)
    weight_ffn_out = ffn_out.grad(activation, grad_ffn_branch)
    grad_pre_full = pull_gelu(ffn_out.back(grad_ffn_branch))[0]
    grad_pre = grad_pre_full.astype(jnp.bfloat16)
    weight_ffn_in = ffn_in.grad(ffn_normed, grad_pre)
    grad_second_part, shift_ffn, scale_ffn = pull_second(ffn_in.back(grad_pre))
    grad_second = grad_output + grad_second_part
    grad_cross_branch = grad_second.astype(jnp.bfloat16)
    weight_cross_out = cross_o.grad(cross_rows, grad_cross_branch)
    grad_cross_rows = cross_o.back(grad_cross_branch).astype(jnp.bfloat16)
    grad_cross_query, grad_key_all, grad_value_all = attend_back(
        cross_query, key_all, value_all, cross_total, grad_cross_rows
    )
    grad_text_key, grad_text_value_full = (
        lax.psum_scatter(
            grad_key_all.astype(jnp.bfloat16), SEQ, scatter_dimension=0, tiled=True
        ).astype(jnp.float32),
        lax.psum_scatter(
            grad_value_all.astype(jnp.bfloat16), SEQ, scatter_dimension=0, tiled=True
        ).astype(jnp.float32),
    )
    grad_text_value = grad_text_value_full.astype(jnp.bfloat16)
    grad_text_key_full, gain_cross_key = pull_text_key(grad_text_key)
    grad_text_key_pre = grad_text_key_full.astype(jnp.bfloat16)
    weight_cross_key = cross_k.grad(text, grad_text_key_pre)
    weight_cross_value = cross_v.grad(text, grad_text_value)
    grad_words = cross_k.back(grad_text_key_pre) + cross_v.back(grad_text_value)
    grad_cross_query_full, gain_cross_query = pull_cross_query(grad_cross_query)
    grad_cross_query_pre = grad_cross_query_full.astype(jnp.bfloat16)
    weight_cross_query = cross_q.grad(crossed, grad_cross_query_pre)
    grad_after_part, gain_norm, bias_norm = pull_cross(cross_q.back(grad_cross_query_pre))
    grad_after = grad_second + grad_after_part
    gate_attn = jnp.sum(grad_after * branch, axis=0)
    grad_branch = (grad_after * modulated[2]).astype(jnp.bfloat16)
    weight_self_out = self_o.grad(attended, grad_branch)
    grad_attended = self_o.back(grad_branch).astype(jnp.bfloat16)
    grad_attn_heads = lax.all_to_all(grad_attended, SEQ, split_axis=1, concat_axis=0, tiled=True)
    grad_query_heads, grad_key_heads, grad_value_heads = attend_back(
        query_heads, key_heads, value_heads, log_total, grad_attn_heads
    )
    grad_query_turned, grad_key_turned, grad_value = (
        lax.all_to_all(
            grad_query_heads.astype(jnp.bfloat16), SEQ, split_axis=0, concat_axis=1, tiled=True
        ),
        lax.all_to_all(
            grad_key_heads.astype(jnp.bfloat16), SEQ, split_axis=0, concat_axis=1, tiled=True
        ),
        lax.all_to_all(
            grad_value_heads.astype(jnp.bfloat16), SEQ, split_axis=0, concat_axis=1, tiled=True
        ),
    )
    grad_query_full, grad_key_full, gain_query, gain_key = pull_turn(
        (grad_query_turned.astype(jnp.float32), grad_key_turned.astype(jnp.float32))
    )
    grad_query_pre = grad_query_full.astype(jnp.bfloat16)
    grad_key_pre = grad_key_full.astype(jnp.bfloat16)
    weight_self_query = self_q.grad(normed, grad_query_pre)
    weight_self_key = self_k.grad(normed, grad_key_pre)
    weight_self_value = self_v.grad(normed, grad_value)
    grad_normed = self_q.back(grad_query_pre) + self_k.back(grad_key_pre) + self_v.back(grad_value)
    grad_start, shift_attn, scale_attn = pull_first(grad_normed)
    grad_hidden = grad_after + grad_start
    grad_modulated = jnp.stack((shift_attn, scale_attn, gate_attn, shift_ffn, scale_ffn, gate_ffn))
    grad_gains = jnp.stack((gain_query, gain_key, gain_cross_query, gain_cross_key, gain_norm))
    grad_biases = jnp.stack(
        (
            column_sums(grad_query_pre),
            column_sums(grad_key_pre),
            column_sums(grad_value),
            column_sums(grad_branch),
            column_sums(grad_cross_query_pre),
            column_sums(grad_text_key_pre),
            column_sums(grad_text_value),
            column_sums(grad_cross_branch),
            bias_norm,
            column_sums(grad_ffn_branch),
        )
    )
    small = (grad_modulated, grad_gains, grad_biases, column_sums(grad_pre))
    stacked = []
    for group in (
        (weight_self_query, weight_self_key, weight_self_value),
        (weight_self_out,),
        (weight_cross_query, weight_cross_key, weight_cross_value),
        (weight_cross_out,),
        (weight_ffn_in,),
        (weight_ffn_out,),
    ):
        for quarter in range(4):
            parts = tuple(w[quarter] for w in group)
            stacked.append(jnp.stack(parts) if len(parts) > 1 else parts[0])
    split = tuple(stacked)
    return (mixed, grad_hidden, grad_words, grad_modulated, small, split)


def body(
    hidden,
    text,
    time_emb,
    modulation,
    self_in,
    self_out,
    cross_in,
    cross_out,
    ffn_in,
    ffn_out,
    gains,
    biases,
    ffn_bias,
    positions,
    cotangent,
):
    spot = (lax.axis_index("y"), lax.axis_index("core"))
    width = modulation.shape[1]
    length = ffn_bias.shape[0]
    self_in_parts = fetch_split(self_in, 1, spot)
    self_out_parts = fetch_split(self_out, 0, spot)
    cross_in_parts = fetch_split(cross_in, 1, spot)
    cross_out_parts = fetch_split(cross_out, 0, spot)
    ffn_in_parts = fetch_split(ffn_in, 0, spot, quarters=False)
    ffn_out_parts = fetch_split(ffn_out, 0, spot, quarters=False)
    modulation_full, gains_full, biases_full, ffn_bias_full = fetch_small(modulation, gains, biases, ffn_bias)
    weights = (
        modulation_full,
        Split(tuple(part[0] for part in self_in_parts), spot),
        Split(tuple(part[1] for part in self_in_parts), spot),
        Split(tuple(part[2] for part in self_in_parts), spot),
        Split(self_out_parts, spot),
        Split(tuple(part[0] for part in cross_in_parts), spot),
        Split(tuple(part[1] for part in cross_in_parts), spot),
        Split(tuple(part[2] for part in cross_in_parts), spot),
        Split(cross_out_parts, spot),
        Split(ffn_in_parts, spot),
        Split(ffn_out_parts, spot),
        gains_full,
        biases_full,
        ffn_bias_full,
    )
    mixed_list = []
    hidden_list = []
    words_list = []
    clock_list = []
    small_totals = None
    split_totals = None
    for batch_index in range(hidden.shape[0]):
        mixed, grad_hidden, grad_words, grad_clock, small, split = micro_step(
            weights,
            hidden[batch_index],
            text[batch_index],
            time_emb[batch_index],
            positions[batch_index],
            cotangent[batch_index],
        )
        mixed_list.append(mixed)
        hidden_list.append(grad_hidden)
        words_list.append(grad_words)
        clock_list.append(grad_clock)
        if small_totals is None:
            small_totals, split_totals = small, split
        else:
            small_totals = tuple(a + b for a, b in zip(small_totals, small))
            split_totals = tuple(a + b for a, b in zip(split_totals, split))
    grad_time = jnp.stack(clock_list)
    finals = [
        reduce_split(split_totals[4 * i : 4 * i + 4], axis, spot)
        for i, axis in enumerate((1, 0, 1, 0, 0, 0))
    ]
    grad_mod, grad_gains, grad_biases, grad_ffn_bias, grad_time = reduce_small(
        *small_totals, grad_time, width, length
    )
    return (
        jnp.stack(mixed_list),
        jnp.stack(hidden_list),
        jnp.stack(words_list),
        grad_time,
        grad_mod,
        finals[0],
        finals[1],
        finals[2],
        finals[3],
        finals[4],
        finals[5],
        grad_gains,
        grad_biases,
        grad_ffn_bias,
    )


def solution(mesh):
    devices = mesh.devices
    split_mesh = Mesh(
        devices.reshape(devices.shape[0] // 2, 2, devices.shape[1]), ("y", "core", "fsdp")
    )
    return jax.shard_map(
        body,
        mesh=split_mesh,
        in_specs=(
            P("fsdp", SEQ, None),
            P("fsdp", SEQ, None),
            P("fsdp", None, None),
            P(None, "fsdp"),
            P(None, "fsdp", None),
            P("fsdp", None),
            P(None, "fsdp", None),
            P("fsdp", None),
            P("fsdp", None),
            P("fsdp", None),
            P(None, "fsdp"),
            P(None, "fsdp"),
            P("fsdp"),
            P("fsdp", None, SEQ),
            P("fsdp", SEQ, None),
        ),
        out_specs=(
            P("fsdp", SEQ, None),
            P("fsdp", SEQ, None),
            P("fsdp", SEQ, None),
            P("fsdp", None, None),
            P(None, "fsdp"),
            P(None, "fsdp", None),
            P("fsdp", None),
            P(None, "fsdp", None),
            P("fsdp", None),
            P("fsdp", None),
            P("fsdp", None),
            P(None, "fsdp"),
            P(None, "fsdp"),
            P("fsdp"),
        ),
        check_vma=False,
    )
```

```python
import jax
import jax.numpy as jnp
from jax import lax
from jax.sharding import Mesh, PartitionSpec as P

HEADS = 12
HEAD = 128


EPSILON = 1e-06
SEQ = ("y", "core")
SWAP = [(0, 1), (1, 0)]


def matmul(operand, factor):
    return jnp.dot(operand, factor, preferred_element_type=jnp.float32)


def inner_rows(operand, factor):
    return lax.dot_general(
        operand, factor, (((0,), (0,)), ((), ())), preferred_element_type=jnp.float32
    )


def outer_cols(operand, factor):
    return lax.dot_general(
        operand, factor, (((1,), (1,)), ((), ())), preferred_element_type=jnp.float32
    )


def column_sums(tensor):
    return jnp.sum(tensor.astype(jnp.float32), axis=0)


def layer_norm(tensor):
    centered = tensor - jnp.mean(tensor, axis=-1, keepdims=True)
    return centered * lax.rsqrt(jnp.mean(centered * centered, axis=-1, keepdims=True) + EPSILON)


def rms_norm(tensor, weight):
    return tensor * lax.rsqrt(jnp.mean(tensor * tensor, axis=-1, keepdims=True) + EPSILON) * weight


def modulate_norm(tensor, shift, scale):
    return layer_norm(tensor) * (1.0 + scale) + shift


def affine_norm(tensor, weight, offset):
    return layer_norm(tensor) * weight + offset


def gelu_tanh(tensor):
    return jax.nn.gelu(tensor, approximate=True)


def rotary_tables(places, head_size, head_count):
    one_sixth = head_size // 6
    span_sizes = (head_size - 4 * one_sixth, 2 * one_sixth, 2 * one_sixth)
    angles = []
    for component in range(3):
        exponents = (
            jnp.arange(0, span_sizes[component], 2, dtype=jnp.float32) / span_sizes[component]
        )
        frequency = 1.0 / 10000.0**exponents
        angles.append(places[component].astype(jnp.float32)[:, None] * frequency[None, :])
    joined = jnp.concatenate(angles, axis=1)
    tiled_angles = jnp.tile(jnp.repeat(joined, 2, axis=1), (1, head_count))
    parity = jnp.where(jnp.arange(tiled_angles.shape[1]) % 2 == 0, -1.0, 1.0)
    return (jnp.cos(tiled_angles), jnp.sin(tiled_angles) * parity)


def rotate(tensor, cosine, signed_sine):
    even_lane = jnp.arange(tensor.shape[1]) % 2 == 0
    swapped = jnp.where(even_lane, jnp.roll(tensor, -1, axis=1), jnp.roll(tensor, 1, axis=1))
    return tensor * cosine + swapped * signed_sine


def split_heads(tensor):
    return tensor.reshape(tensor.shape[0], tensor.shape[1] // HEAD, HEAD)


def attend(queries, key_rows, value_rows):
    scores = jnp.einsum(
        "qhd,khd->hqk",
        split_heads(queries),
        split_heads(key_rows),
        preferred_element_type=jnp.float32,
    ) * HEAD ** (-0.5)
    row_max = jnp.max(scores, axis=-1, keepdims=True)
    exponentials = jnp.exp(scores - row_max)
    row_total = jnp.sum(exponentials, axis=-1, keepdims=True)
    probabilities = (exponentials / row_total).astype(jnp.bfloat16)
    result = jnp.einsum(
        "hqk,khd->qhd", probabilities, split_heads(value_rows), preferred_element_type=jnp.float32
    )
    return (result.reshape(queries.shape[0], -1).astype(jnp.bfloat16), row_max + jnp.log(row_total))


def attend_back(queries, key_rows, value_rows, log_total, grad_rows):
    query_split = split_heads(queries)
    key_split = split_heads(key_rows)
    grad_split = split_heads(grad_rows)
    scale_factor = HEAD ** (-0.5)
    scores = (
        jnp.einsum("qhd,khd->hqk", query_split, key_split, preferred_element_type=jnp.float32)
        * scale_factor
    )
    probs_full = jnp.exp(scores - log_total)
    probs_low = probs_full.astype(jnp.bfloat16)
    grad_values = jnp.einsum(
        "hqk,qhd->khd", probs_low, grad_split, preferred_element_type=jnp.float32
    )
    grad_probs = jnp.einsum(
        "qhd,khd->hqk", grad_split, split_heads(value_rows), preferred_element_type=jnp.float32
    )
    grad_scores = (
        probs_full * (grad_probs - jnp.sum(grad_probs * probs_full, axis=-1, keepdims=True))
    ).astype(jnp.bfloat16)
    grad_queries = (
        jnp.einsum("hqk,khd->qhd", grad_scores, key_split, preferred_element_type=jnp.float32)
        * scale_factor
    )
    grad_keys = (
        jnp.einsum("hqk,qhd->khd", grad_scores, query_split, preferred_element_type=jnp.float32)
        * scale_factor
    )
    return (
        grad_queries.reshape(queries.shape[0], -1),
        grad_keys.reshape(key_rows.shape[0], -1),
        grad_values.reshape(value_rows.shape[0], -1),
    )


def swap_core(tensor):
    return lax.ppermute(tensor, "core", SWAP)


def join(mine, other, core):
    width = mine.shape[-1]
    both = jnp.concatenate([other, mine, other], axis=-1)
    return lax.dynamic_slice_in_dim(both, (1 - core) * width, 2 * width, axis=-1)


def halves(tensor, core):
    width = tensor.shape[-1] // 2
    return (
        lax.dynamic_slice_in_dim(tensor, core * width, width, axis=-1),
        lax.dynamic_slice_in_dim(tensor, (1 - core) * width, width, axis=-1),
    )


def swap_y(tensor):
    return lax.ppermute(tensor, "y", SWAP)


class Split:
    def __init__(self, parts, spot):
        self.parts, self.spot = parts, spot

    def apply(self, rows):
        y, core = self.spot
        outs = [matmul(rows, part) for part in self.parts]
        if len(outs) == 2:
            return join(outs[0], outs[1], core)
        return join(join(outs[0], outs[1], y), join(outs[2], outs[3], y), core)

    def quarters(self, grad):
        y, core = self.spot
        grad_mine, grad_other = halves(grad, core)
        return halves(grad_mine, y) + halves(grad_other, y)

    def back(self, grad):
        if len(self.parts) == 2:
            grad_mine, grad_other = halves(grad, self.spot[1])
            return outer_cols(grad_mine, self.parts[0]) + outer_cols(grad_other, self.parts[1])
        pieces = [outer_cols(g, part) for g, part in zip(self.quarters(grad), self.parts)]
        return (pieces[0] + pieces[1]) + (pieces[2] + pieces[3])

    def grad(self, rows, grad):
        return tuple(inner_rows(rows, g) for g in self.quarters(grad))


def fetch_split(local, gather_axis, spot, quarters=True):
    y, core = spot
    if not quarters:
        width = local.shape[-1] // 2
        part = lax.dynamic_slice_in_dim(local, core * width, width, axis=-1)
        mine = lax.all_gather(part, "fsdp", axis=gather_axis, tiled=True)
        return (mine, swap_core(mine))
    width = local.shape[-1] // 4
    part = lax.dynamic_slice_in_dim(local, (2 * core + y) * width, width, axis=-1)
    own = lax.all_gather(part, "fsdp", axis=gather_axis, tiled=True)
    y_part = swap_y(own)
    return (own, y_part, swap_core(own), swap_core(y_part))


def reduce_split(parts, scatter_axis, spot):
    y, core = spot
    own, y_part, core_part, cross_part = parts
    from_core = swap_core(core_part.astype(jnp.bfloat16)).astype(jnp.float32)
    from_cross = swap_core(cross_part.astype(jnp.bfloat16)).astype(jnp.float32)
    chip_own = own + from_core
    chip_y = (y_part + from_cross).astype(jnp.bfloat16)
    total = (chip_own + swap_y(chip_y).astype(jnp.float32)).astype(jnp.bfloat16)
    owned = lax.psum_scatter(total, "fsdp", scatter_dimension=scatter_axis, tiled=True)
    owned_y = swap_y(owned)
    mine = join(owned, owned_y, y)
    return join(mine, swap_core(mine), core).astype(jnp.float32)


def fetch_small(modulation, gains, biases, ffn_bias):
    width = modulation.shape[1]
    length = ffn_bias.shape[0]
    rows = -(-length // width)
    padded = jnp.pad(ffn_bias, (0, rows * width - length)).reshape(rows, width)
    packed = jnp.concatenate([modulation, gains, biases, padded], axis=0)
    full = lax.all_gather(packed, "fsdp", axis=1, tiled=True)
    shards = full.shape[1] // width
    bias_rows = full[21:].reshape(rows, shards, width).transpose(1, 0, 2)
    bias_full = bias_rows.reshape(shards, rows * width)[:, :length].reshape(shards * length)
    return full[:6], full[6:11], full[11:21], bias_full


def reduce_small(grad_mod, grad_gains, grad_biases, grad_ffn_bias, grad_time, width, length):
    rows = -(-length // width)
    shards = grad_mod.shape[1] // width
    bias_rows = jnp.pad(grad_ffn_bias.reshape(shards, length), ((0, 0), (0, rows * width - length)))
    bias_rows = bias_rows.reshape(shards, rows, width).transpose(1, 0, 2).reshape(rows, shards * width)
    packed = jnp.concatenate([grad_mod, grad_gains, grad_biases, bias_rows], axis=0)
    owned = lax.psum_scatter(packed, "fsdp", scatter_dimension=1, tiled=True)
    flat = jnp.concatenate([owned.reshape(-1), grad_time.reshape(-1)])
    summed = lax.psum(flat, SEQ)
    owned = summed[: owned.size].reshape(owned.shape)
    grad_time = summed[owned.size :].reshape(grad_time.shape)
    bias_owned = owned[21:].reshape(-1)[:length]
    return owned[:6], owned[6:11], owned[11:21], bias_owned, grad_time


def micro_step(weights, hidden, key_all, value_all, time_emb, places, cotangent):
    modulation, self_q, self_k, self_v, self_o, cross_q, cross_k, cross_v, cross_o, ffn_in, ffn_out, gains, biases, ffn_bias = (
        weights
    )
    gain_rows = gains.astype(jnp.float32)
    bias_rows = biases.astype(jnp.float32)
    modulated = modulation.astype(jnp.float32) + time_emb.astype(jnp.float32)
    cosine, signed_sine = rotary_tables(places, HEAD, HEADS)
    residual_in = hidden.astype(jnp.float32)
    normed_full, pull_first = jax.vjp(modulate_norm, residual_in, modulated[0], modulated[1])
    normed = normed_full.astype(jnp.bfloat16)
    query_pre = self_q.apply(normed) + bias_rows[0]
    key_pre = self_k.apply(normed) + bias_rows[1]
    value_low = (self_v.apply(normed) + bias_rows[2]).astype(jnp.bfloat16)

    def turn_both(query_input, key_input, gain_query, gain_key):
        return (
            rotate(rms_norm(query_input, gain_query), cosine, signed_sine),
            rotate(rms_norm(key_input, gain_key), cosine, signed_sine),
        )

    turned, pull_turn = jax.vjp(turn_both, query_pre, key_pre, gain_rows[0], gain_rows[1])
    query_heads, key_heads, value_heads = (
        lax.all_to_all(turned[0].astype(jnp.bfloat16), SEQ, split_axis=1, concat_axis=0, tiled=True),
        lax.all_to_all(turned[1].astype(jnp.bfloat16), SEQ, split_axis=1, concat_axis=0, tiled=True),
        lax.all_to_all(value_low, SEQ, split_axis=1, concat_axis=0, tiled=True),
    )
    attn_heads, log_total = attend(query_heads, key_heads, value_heads)
    attended = lax.all_to_all(attn_heads, SEQ, split_axis=0, concat_axis=1, tiled=True)
    branch = self_o.apply(attended) + bias_rows[3]
    after_attn = residual_in + branch * modulated[2]
    crossed_full, pull_cross = jax.vjp(affine_norm, after_attn, gain_rows[4], bias_rows[8])
    crossed = crossed_full.astype(jnp.bfloat16)
    cross_query_pre = cross_q.apply(crossed) + bias_rows[4]
    cross_query_full, pull_cross_query = jax.vjp(rms_norm, cross_query_pre, gain_rows[2])
    cross_query = cross_query_full.astype(jnp.bfloat16)
    cross_rows, cross_total = attend(cross_query, key_all, value_all)
    second = after_attn + cross_o.apply(cross_rows) + bias_rows[7]
    ffn_normed_full, pull_second = jax.vjp(modulate_norm, second, modulated[3], modulated[4])
    ffn_normed = ffn_normed_full.astype(jnp.bfloat16)
    pre_act = ffn_in.apply(ffn_normed) + ffn_bias.astype(jnp.float32)
    activation_full, pull_gelu = jax.vjp(gelu_tanh, pre_act)
    activation = activation_full.astype(jnp.bfloat16)
    ffn_branch = ffn_out.apply(activation) + bias_rows[9]
    mixed = (second + ffn_branch * modulated[5]).astype(jnp.bfloat16)
    grad_output = cotangent.astype(jnp.float32)
    gate_ffn = jnp.sum(grad_output * ffn_branch, axis=0)
    grad_ffn_branch = (grad_output * modulated[5]).astype(jnp.bfloat16)
    grad_pre_full = pull_gelu(ffn_out.back(grad_ffn_branch))[0]
    grad_pre = grad_pre_full.astype(jnp.bfloat16)
    grad_second_part, shift_ffn, scale_ffn = pull_second(ffn_in.back(grad_pre))
    grad_second = grad_output + grad_second_part
    grad_cross_branch = grad_second.astype(jnp.bfloat16)
    grad_cross_rows = cross_o.back(grad_cross_branch).astype(jnp.bfloat16)
    grad_cross_query, grad_key_all, grad_value_all = attend_back(
        cross_query, key_all, value_all, cross_total, grad_cross_rows
    )
    grad_cross_query_full, gain_cross_query = pull_cross_query(grad_cross_query)
    grad_cross_query_pre = grad_cross_query_full.astype(jnp.bfloat16)
    grad_after_part, gain_norm, bias_norm = pull_cross(cross_q.back(grad_cross_query_pre))
    grad_after = grad_second + grad_after_part
    gate_attn = jnp.sum(grad_after * branch, axis=0)
    grad_branch = (grad_after * modulated[2]).astype(jnp.bfloat16)
    grad_attended = self_o.back(grad_branch).astype(jnp.bfloat16)
    grad_attn_heads = lax.all_to_all(grad_attended, SEQ, split_axis=1, concat_axis=0, tiled=True)
    grad_query_heads, grad_key_heads, grad_value_heads = attend_back(
        query_heads, key_heads, value_heads, log_total, grad_attn_heads
    )
    grad_query_turned, grad_key_turned, grad_value = (
        lax.all_to_all(
            grad_query_heads.astype(jnp.bfloat16), SEQ, split_axis=0, concat_axis=1, tiled=True
        ),
        lax.all_to_all(
            grad_key_heads.astype(jnp.bfloat16), SEQ, split_axis=0, concat_axis=1, tiled=True
        ),
        lax.all_to_all(
            grad_value_heads.astype(jnp.bfloat16), SEQ, split_axis=0, concat_axis=1, tiled=True
        ),
    )
    grad_query_full, grad_key_full, gain_query, gain_key = pull_turn(
        (grad_query_turned.astype(jnp.float32), grad_key_turned.astype(jnp.float32))
    )
    grad_query_pre = grad_query_full.astype(jnp.bfloat16)
    grad_key_pre = grad_key_full.astype(jnp.bfloat16)
    grad_normed = self_q.back(grad_query_pre) + self_k.back(grad_key_pre) + self_v.back(grad_value)
    grad_start, shift_attn, scale_attn = pull_first(grad_normed)
    grad_hidden = grad_after + grad_start
    grad_modulated = jnp.stack((shift_attn, scale_attn, gate_attn, shift_ffn, scale_ffn, gate_ffn))
    grad_gains = jnp.stack((gain_query, gain_key, gain_cross_query, jnp.zeros_like(gain_query), gain_norm))
    grad_biases = jnp.stack(
        (
            column_sums(grad_query_pre),
            column_sums(grad_key_pre),
            column_sums(grad_value),
            column_sums(grad_branch),
            column_sums(grad_cross_query_pre),
            jnp.zeros_like(bias_norm),
            jnp.zeros_like(bias_norm),
            column_sums(grad_cross_branch),
            bias_norm,
            column_sums(grad_ffn_branch),
        )
    )
    small = (grad_modulated, grad_gains, grad_biases, column_sums(grad_pre))
    split = (
        (normed, grad_query_pre),
        (normed, grad_key_pre),
        (normed, grad_value),
        (attended, grad_branch),
        (crossed, grad_cross_query_pre),
        (cross_rows, grad_cross_branch),
        (ffn_normed, grad_pre),
        (activation, grad_ffn_branch),
    )
    return (mixed, grad_hidden, (grad_key_all, grad_value_all), grad_modulated, small, split)


def body(
    hidden,
    text,
    time_emb,
    modulation,
    self_in,
    self_out,
    cross_in,
    cross_out,
    ffn_in,
    ffn_out,
    gains,
    biases,
    ffn_bias,
    positions,
    cotangent,
):
    spot = (lax.axis_index("y"), lax.axis_index("core"))
    width = modulation.shape[1]
    length = ffn_bias.shape[0]
    heads_in = self_in.shape[0]
    attn_in_parts = fetch_split(jnp.concatenate([self_in, cross_in], axis=0), 1, spot)
    attn_out_parts = fetch_split(jnp.stack([self_out, cross_out]), 1, spot)
    ffn_in_parts = fetch_split(ffn_in, 0, spot, quarters=False)
    ffn_out_parts = fetch_split(ffn_out, 0, spot, quarters=False)
    modulation_full, gains_full, biases_full, ffn_bias_full = fetch_small(modulation, gains, biases, ffn_bias)
    in_split = [Split(tuple(part[i] for part in attn_in_parts), spot) for i in range(2 * heads_in)]
    out_split = [Split(tuple(part[i] for part in attn_out_parts), spot) for i in range(2)]
    weights = (
        modulation_full,
        in_split[0],
        in_split[1],
        in_split[2],
        out_split[0],
        in_split[3],
        in_split[4],
        in_split[5],
        out_split[1],
        Split(ffn_in_parts, spot),
        Split(ffn_out_parts, spot),
        gains_full,
        biases_full,
        ffn_bias_full,
    )
    cross_k, cross_v = in_split[4], in_split[5]
    gain_rows = gains_full.astype(jnp.float32)
    bias_rows = biases_full.astype(jnp.float32)
    clips, words, model = text.shape
    text_flat = text.reshape(clips * words, model)
    text_key_pre = cross_k.apply(text_flat) + bias_rows[5]
    text_key_full, pull_text_key = jax.vjp(rms_norm, text_key_pre, gain_rows[3])
    text_value = (cross_v.apply(text_flat) + bias_rows[6]).astype(jnp.bfloat16)
    text_key_low = text_key_full.astype(jnp.bfloat16)
    local_kv = jnp.concatenate(
        [part[i * words : (i + 1) * words] for part in (text_key_low, text_value) for i in range(clips)], axis=1
    )
    all_kv = lax.all_gather(local_kv, SEQ, axis=0, tiled=True)
    mixed_list = []
    hidden_list = []
    key_grads = []
    value_grads = []
    clock_list = []
    small_totals = None
    pair_lists = None
    for batch_index in range(clips):
        mixed, grad_hidden, text_grads, grad_clock, small, split = micro_step(
            weights,
            hidden[batch_index],
            all_kv[:, batch_index * model : (batch_index + 1) * model],
            all_kv[:, (clips + batch_index) * model : (clips + batch_index + 1) * model],
            time_emb[batch_index],
            positions[batch_index],
            cotangent[batch_index],
        )
        mixed_list.append(mixed)
        hidden_list.append(grad_hidden)
        key_grads.append(text_grads[0])
        value_grads.append(text_grads[1])
        clock_list.append(grad_clock)
        if small_totals is None:
            small_totals, pair_lists = small, [[pair] for pair in split]
        else:
            small_totals = tuple(a + b for a, b in zip(small_totals, small))
            for found, pair in zip(pair_lists, split):
                found.append(pair)
    pairs = [
        (jnp.concatenate([p[0] for p in found]), jnp.concatenate([p[1] for p in found]))
        for found in pair_lists
    ]
    split_grads = [
        split_weight.grad(rows, grad)
        for split_weight, (rows, grad) in zip(
            (in_split[0], in_split[1], in_split[2], out_split[0], in_split[3], out_split[1], weights[9], weights[10]),
            pairs,
        )
    ]
    grad_kv = jnp.concatenate(key_grads + value_grads, axis=1).astype(jnp.bfloat16)
    owned_kv = lax.psum_scatter(grad_kv, SEQ, scatter_dimension=0, tiled=True).astype(jnp.float32)
    owned_parts = [owned_kv[:, i * model : (i + 1) * model] for i in range(2 * clips)]
    grad_text_key = jnp.concatenate(owned_parts[:clips], axis=0)
    grad_text_value = jnp.concatenate(owned_parts[clips:], axis=0).astype(jnp.bfloat16)
    grad_text_key_full, gain_cross_key = pull_text_key(grad_text_key)
    grad_text_key_pre = grad_text_key_full.astype(jnp.bfloat16)
    weight_cross_key = cross_k.grad(text_flat, grad_text_key_pre)
    weight_cross_value = cross_v.grad(text_flat, grad_text_value)
    grad_words = cross_k.back(grad_text_key_pre) + cross_v.back(grad_text_value)
    grad_mod, grad_gains, grad_biases, grad_ffn_bias_local = small_totals
    grad_gains = grad_gains.at[3].add(gain_cross_key)
    grad_biases = grad_biases.at[5].add(column_sums(grad_text_key_pre))
    grad_biases = grad_biases.at[6].add(column_sums(grad_text_value))
    attn_in_grads = tuple(
        jnp.stack(
            [split_grads[0][q], split_grads[1][q], split_grads[2][q], split_grads[4][q], weight_cross_key[q], weight_cross_value[q]]
        )
        for q in range(4)
    )
    attn_out_grads = tuple(jnp.stack([split_grads[3][q], split_grads[5][q]]) for q in range(4))
    attn_in_final = reduce_split(attn_in_grads, 1, spot)
    attn_out_final = reduce_split(attn_out_grads, 1, spot)
    ffn_in_final = reduce_split(split_grads[6], 0, spot)
    ffn_out_final = reduce_split(split_grads[7], 0, spot)
    grad_time = jnp.stack(clock_list)
    grad_mod, grad_gains, grad_biases, grad_ffn_bias, grad_time = reduce_small(
        grad_mod, grad_gains, grad_biases, grad_ffn_bias_local, grad_time, width, length
    )
    return (
        jnp.stack(mixed_list),
        jnp.stack(hidden_list),
        grad_words.reshape(clips, words, model),
        grad_time,
        grad_mod,
        attn_in_final[:heads_in],
        attn_out_final[0],
        attn_in_final[heads_in:],
        attn_out_final[1],
        ffn_in_final,
        ffn_out_final,
        grad_gains,
        grad_biases,
        grad_ffn_bias,
    )


def solution(mesh):
    devices = mesh.devices
    split_mesh = Mesh(
        devices.reshape(devices.shape[0] // 2, 2, devices.shape[1]), ("y", "core", "fsdp")
    )
    return jax.shard_map(
        body,
        mesh=split_mesh,
        in_specs=(
            P("fsdp", SEQ, None),
            P("fsdp", SEQ, None),
            P("fsdp", None, None),
            P(None, "fsdp"),
            P(None, "fsdp", None),
            P("fsdp", None),
            P(None, "fsdp", None),
            P("fsdp", None),
            P("fsdp", None),
            P("fsdp", None),
            P(None, "fsdp"),
            P(None, "fsdp"),
            P("fsdp"),
            P("fsdp", None, SEQ),
            P("fsdp", SEQ, None),
        ),
        out_specs=(
            P("fsdp", SEQ, None),
            P("fsdp", SEQ, None),
            P("fsdp", SEQ, None),
            P("fsdp", None, None),
            P(None, "fsdp"),
            P(None, "fsdp", None),
            P("fsdp", None),
            P(None, "fsdp", None),
            P("fsdp", None),
            P("fsdp", None),
            P("fsdp", None),
            P(None, "fsdp"),
            P(None, "fsdp"),
            P("fsdp"),
        ),
        check_vma=False,
    )
```

```python
import jax
import jax.numpy as jnp
from jax import lax
from jax.sharding import Mesh, PartitionSpec as P

HEADS = 12
HEAD = 128


EPSILON = 1e-06
SEQ = ("y", "core")
SWAP = [(0, 1), (1, 0)]


def matmul(operand, factor):
    return jnp.dot(operand, factor, preferred_element_type=jnp.float32)


def inner_rows(operand, factor):
    return lax.dot_general(
        operand, factor, (((0,), (0,)), ((), ())), preferred_element_type=jnp.float32
    )


def outer_cols(operand, factor):
    return lax.dot_general(
        operand, factor, (((1,), (1,)), ((), ())), preferred_element_type=jnp.float32
    )


def column_sums(tensor):
    return jnp.sum(tensor.astype(jnp.float32), axis=0)


def layer_norm(tensor):
    centered = tensor - jnp.mean(tensor, axis=-1, keepdims=True)
    return centered * lax.rsqrt(jnp.mean(centered * centered, axis=-1, keepdims=True) + EPSILON)


def rms_norm(tensor, weight):
    return tensor * lax.rsqrt(jnp.mean(tensor * tensor, axis=-1, keepdims=True) + EPSILON) * weight


def modulate_norm(tensor, shift, scale):
    return layer_norm(tensor) * (1.0 + scale) + shift


def affine_norm(tensor, weight, offset):
    return layer_norm(tensor) * weight + offset


def gelu_tanh(tensor):
    return jax.nn.gelu(tensor, approximate=True)


def rotary_tables(places, head_size, head_count):
    one_sixth = head_size // 6
    span_sizes = (head_size - 4 * one_sixth, 2 * one_sixth, 2 * one_sixth)
    angles = []
    for component in range(3):
        exponents = (
            jnp.arange(0, span_sizes[component], 2, dtype=jnp.float32) / span_sizes[component]
        )
        frequency = 1.0 / 10000.0**exponents
        angles.append(places[component].astype(jnp.float32)[:, None] * frequency[None, :])
    joined = jnp.concatenate(angles, axis=1)
    tiled_angles = jnp.tile(jnp.repeat(joined, 2, axis=1), (1, head_count))
    parity = jnp.where(jnp.arange(tiled_angles.shape[1]) % 2 == 0, -1.0, 1.0)
    return (jnp.cos(tiled_angles), jnp.sin(tiled_angles) * parity)


def rotate(tensor, cosine, signed_sine):
    even_lane = jnp.arange(tensor.shape[1]) % 2 == 0
    swapped = jnp.where(even_lane, jnp.roll(tensor, -1, axis=1), jnp.roll(tensor, 1, axis=1))
    return tensor * cosine + swapped * signed_sine


def split_heads(tensor):
    return tensor.reshape(tensor.shape[0], tensor.shape[1] // HEAD, HEAD)


def attend(queries, key_rows, value_rows):
    scores = jnp.einsum(
        "qhd,khd->hqk",
        split_heads(queries),
        split_heads(key_rows),
        preferred_element_type=jnp.float32,
    ) * HEAD ** (-0.5)
    row_max = jnp.max(scores, axis=-1, keepdims=True)
    exponentials = jnp.exp(scores - row_max)
    row_total = jnp.sum(exponentials, axis=-1, keepdims=True)
    probabilities = (exponentials / row_total).astype(jnp.bfloat16)
    result = jnp.einsum(
        "hqk,khd->qhd", probabilities, split_heads(value_rows), preferred_element_type=jnp.float32
    )
    return (result.reshape(queries.shape[0], -1).astype(jnp.bfloat16), row_max + jnp.log(row_total))


def attend_back(queries, key_rows, value_rows, log_total, grad_rows):
    query_split = split_heads(queries)
    key_split = split_heads(key_rows)
    grad_split = split_heads(grad_rows)
    scale_factor = HEAD ** (-0.5)
    scores = (
        jnp.einsum("qhd,khd->hqk", query_split, key_split, preferred_element_type=jnp.float32)
        * scale_factor
    )
    probs_full = jnp.exp(scores - log_total)
    probs_low = probs_full.astype(jnp.bfloat16)
    grad_values = jnp.einsum(
        "hqk,qhd->khd", probs_low, grad_split, preferred_element_type=jnp.float32
    )
    grad_probs = jnp.einsum(
        "qhd,khd->hqk", grad_split, split_heads(value_rows), preferred_element_type=jnp.float32
    )
    grad_scores = (
        probs_full * (grad_probs - jnp.sum(grad_probs * probs_full, axis=-1, keepdims=True))
    ).astype(jnp.bfloat16)
    grad_queries = (
        jnp.einsum("hqk,khd->qhd", grad_scores, key_split, preferred_element_type=jnp.float32)
        * scale_factor
    )
    grad_keys = (
        jnp.einsum("hqk,qhd->khd", grad_scores, query_split, preferred_element_type=jnp.float32)
        * scale_factor
    )
    return (
        grad_queries.reshape(queries.shape[0], -1),
        grad_keys.reshape(key_rows.shape[0], -1),
        grad_values.reshape(value_rows.shape[0], -1),
    )


def swap_core(tensor):
    return lax.ppermute(tensor, "core", SWAP)


def join(mine, other, core):
    width = mine.shape[-1]
    both = jnp.concatenate([other, mine, other], axis=-1)
    return lax.dynamic_slice_in_dim(both, (1 - core) * width, 2 * width, axis=-1)


def halves(tensor, core):
    width = tensor.shape[-1] // 2
    return (
        lax.dynamic_slice_in_dim(tensor, core * width, width, axis=-1),
        lax.dynamic_slice_in_dim(tensor, (1 - core) * width, width, axis=-1),
    )


def swap_y(tensor):
    return lax.ppermute(tensor, "y", SWAP)


class Split:
    def __init__(self, parts, spot):
        self.parts, self.spot = parts, spot

    def apply(self, rows):
        y, core = self.spot
        outs = [matmul(rows, part) for part in self.parts]
        if len(outs) == 2:
            return join(outs[0], outs[1], core)
        return join(join(outs[0], outs[1], y), join(outs[2], outs[3], y), core)

    def quarters(self, grad):
        y, core = self.spot
        grad_mine, grad_other = halves(grad, core)
        return halves(grad_mine, y) + halves(grad_other, y)

    def back(self, grad):
        if len(self.parts) == 2:
            grad_mine, grad_other = halves(grad, self.spot[1])
            return outer_cols(grad_mine, self.parts[0]) + outer_cols(grad_other, self.parts[1])
        pieces = [outer_cols(g, part) for g, part in zip(self.quarters(grad), self.parts)]
        return (pieces[0] + pieces[1]) + (pieces[2] + pieces[3])

    def grad(self, rows, grad, quarters=True):
        pieces = self.quarters(grad) if quarters else halves(grad, self.spot[1])
        return tuple(inner_rows(rows, g) for g in pieces)


def fetch_split(local, gather_axis, spot, quarters=True):
    y, core = spot
    if not quarters:
        width = local.shape[-1] // 2
        part = lax.dynamic_slice_in_dim(local, core * width, width, axis=-1)
        mine = lax.all_gather(part, "fsdp", axis=gather_axis, tiled=True)
        return (mine, swap_core(mine))
    width = local.shape[-1] // 4
    part = lax.dynamic_slice_in_dim(local, (2 * core + y) * width, width, axis=-1)
    own = lax.all_gather(part, "fsdp", axis=gather_axis, tiled=True)
    y_part = swap_y(own)
    return (own, y_part, swap_core(own), swap_core(y_part))


def reduce_split(parts, scatter_axis, spot):
    y, core = spot
    own, y_part, core_part, cross_part = parts
    from_core = swap_core(core_part.astype(jnp.bfloat16)).astype(jnp.float32)
    from_cross = swap_core(cross_part.astype(jnp.bfloat16)).astype(jnp.float32)
    chip_own = own + from_core
    chip_y = (y_part + from_cross).astype(jnp.bfloat16)
    total = (chip_own + swap_y(chip_y).astype(jnp.float32)).astype(jnp.bfloat16)
    owned = lax.psum_scatter(total, "fsdp", scatter_dimension=scatter_axis, tiled=True)
    owned_y = swap_y(owned)
    mine = join(owned, owned_y, y)
    return join(mine, swap_core(mine), core).astype(jnp.float32)


def reduce_half(parts, scatter_axis, spot):
    y, core = spot
    mine, other = parts
    received = swap_core(other.astype(jnp.bfloat16)).astype(jnp.float32)
    chip = (mine + received).astype(jnp.bfloat16)
    owned = lax.psum_scatter(chip, "fsdp", scatter_dimension=scatter_axis, tiled=True)
    summed = owned.astype(jnp.float32) + swap_y(owned).astype(jnp.float32)
    return join(summed, swap_core(summed), core)


def fetch_small(modulation, gains, biases, ffn_bias):
    width = modulation.shape[1]
    length = ffn_bias.shape[0]
    rows = -(-length // width)
    padded = jnp.pad(ffn_bias, (0, rows * width - length)).reshape(rows, width)
    packed = jnp.concatenate([modulation, gains, biases, padded], axis=0)
    full = lax.all_gather(packed, "fsdp", axis=1, tiled=True)
    shards = full.shape[1] // width
    bias_rows = full[21:].reshape(rows, shards, width).transpose(1, 0, 2)
    bias_full = bias_rows.reshape(shards, rows * width)[:, :length].reshape(shards * length)
    return full[:6], full[6:11], full[11:21], bias_full


def reduce_small(grad_mod, grad_gains, grad_biases, grad_ffn_bias, grad_time, width, length):
    rows = -(-length // width)
    shards = grad_mod.shape[1] // width
    bias_rows = jnp.pad(grad_ffn_bias.reshape(shards, length), ((0, 0), (0, rows * width - length)))
    bias_rows = bias_rows.reshape(shards, rows, width).transpose(1, 0, 2).reshape(rows, shards * width)
    packed = jnp.concatenate([grad_mod, grad_gains, grad_biases, bias_rows], axis=0)
    owned = lax.psum_scatter(packed, "fsdp", scatter_dimension=1, tiled=True)
    flat = jnp.concatenate([owned.reshape(-1), grad_time.reshape(-1)])
    summed = lax.psum(flat, SEQ)
    owned = summed[: owned.size].reshape(owned.shape)
    grad_time = summed[owned.size :].reshape(grad_time.shape)
    bias_owned = owned[21:].reshape(-1)[:length]
    return owned[:6], owned[6:11], owned[11:21], bias_owned, grad_time


def micro_step(weights, hidden, key_all, value_all, time_emb, places, cotangent):
    modulation, self_q, self_k, self_v, self_o, cross_q, cross_k, cross_v, cross_o, ffn_in, ffn_out, gains, biases, ffn_bias = (
        weights
    )
    gain_rows = gains.astype(jnp.float32)
    bias_rows = biases.astype(jnp.float32)
    modulated = modulation.astype(jnp.float32) + time_emb.astype(jnp.float32)
    cosine, signed_sine = rotary_tables(places, HEAD, HEADS)
    residual_in = hidden.astype(jnp.float32)
    normed_full, pull_first = jax.vjp(modulate_norm, residual_in, modulated[0], modulated[1])
    normed = normed_full.astype(jnp.bfloat16)
    query_pre = self_q.apply(normed) + bias_rows[0]
    key_pre = self_k.apply(normed) + bias_rows[1]
    value_low = (self_v.apply(normed) + bias_rows[2]).astype(jnp.bfloat16)

    def turn_both(query_input, key_input, gain_query, gain_key):
        return (
            rotate(rms_norm(query_input, gain_query), cosine, signed_sine),
            rotate(rms_norm(key_input, gain_key), cosine, signed_sine),
        )

    turned, pull_turn = jax.vjp(turn_both, query_pre, key_pre, gain_rows[0], gain_rows[1])
    query_heads, key_heads, value_heads = (
        lax.all_to_all(turned[0].astype(jnp.bfloat16), SEQ, split_axis=1, concat_axis=0, tiled=True),
        lax.all_to_all(turned[1].astype(jnp.bfloat16), SEQ, split_axis=1, concat_axis=0, tiled=True),
        lax.all_to_all(value_low, SEQ, split_axis=1, concat_axis=0, tiled=True),
    )
    attn_heads, log_total = attend(query_heads, key_heads, value_heads)
    attended = lax.all_to_all(attn_heads, SEQ, split_axis=0, concat_axis=1, tiled=True)
    branch = self_o.apply(attended) + bias_rows[3]
    after_attn = residual_in + branch * modulated[2]
    crossed_full, pull_cross = jax.vjp(affine_norm, after_attn, gain_rows[4], bias_rows[8])
    crossed = crossed_full.astype(jnp.bfloat16)
    cross_query_pre = cross_q.apply(crossed) + bias_rows[4]
    cross_query_full, pull_cross_query = jax.vjp(rms_norm, cross_query_pre, gain_rows[2])
    cross_query = cross_query_full.astype(jnp.bfloat16)
    cross_rows, cross_total = attend(cross_query, key_all, value_all)
    second = after_attn + cross_o.apply(cross_rows) + bias_rows[7]
    ffn_normed_full, pull_second = jax.vjp(modulate_norm, second, modulated[3], modulated[4])
    ffn_normed = ffn_normed_full.astype(jnp.bfloat16)
    pre_act = ffn_in.apply(ffn_normed) + ffn_bias.astype(jnp.float32)
    activation_full, pull_gelu = jax.vjp(gelu_tanh, pre_act)
    activation = activation_full.astype(jnp.bfloat16)
    ffn_branch = ffn_out.apply(activation) + bias_rows[9]
    mixed = (second + ffn_branch * modulated[5]).astype(jnp.bfloat16)
    grad_output = cotangent.astype(jnp.float32)
    gate_ffn = jnp.sum(grad_output * ffn_branch, axis=0)
    grad_ffn_branch = (grad_output * modulated[5]).astype(jnp.bfloat16)
    grad_pre_full = pull_gelu(ffn_out.back(grad_ffn_branch))[0]
    grad_pre = grad_pre_full.astype(jnp.bfloat16)
    grad_second_part, shift_ffn, scale_ffn = pull_second(ffn_in.back(grad_pre))
    grad_second = grad_output + grad_second_part
    grad_cross_branch = grad_second.astype(jnp.bfloat16)
    grad_cross_rows = cross_o.back(grad_cross_branch).astype(jnp.bfloat16)
    grad_cross_query, grad_key_all, grad_value_all = attend_back(
        cross_query, key_all, value_all, cross_total, grad_cross_rows
    )
    grad_cross_query_full, gain_cross_query = pull_cross_query(grad_cross_query)
    grad_cross_query_pre = grad_cross_query_full.astype(jnp.bfloat16)
    grad_after_part, gain_norm, bias_norm = pull_cross(cross_q.back(grad_cross_query_pre))
    grad_after = grad_second + grad_after_part
    gate_attn = jnp.sum(grad_after * branch, axis=0)
    grad_branch = (grad_after * modulated[2]).astype(jnp.bfloat16)
    grad_attended = self_o.back(grad_branch).astype(jnp.bfloat16)
    grad_attn_heads = lax.all_to_all(grad_attended, SEQ, split_axis=1, concat_axis=0, tiled=True)
    grad_query_heads, grad_key_heads, grad_value_heads = attend_back(
        query_heads, key_heads, value_heads, log_total, grad_attn_heads
    )
    grad_query_turned, grad_key_turned, grad_value = (
        lax.all_to_all(
            grad_query_heads.astype(jnp.bfloat16), SEQ, split_axis=0, concat_axis=1, tiled=True
        ),
        lax.all_to_all(
            grad_key_heads.astype(jnp.bfloat16), SEQ, split_axis=0, concat_axis=1, tiled=True
        ),
        lax.all_to_all(
            grad_value_heads.astype(jnp.bfloat16), SEQ, split_axis=0, concat_axis=1, tiled=True
        ),
    )
    grad_query_full, grad_key_full, gain_query, gain_key = pull_turn(
        (grad_query_turned.astype(jnp.float32), grad_key_turned.astype(jnp.float32))
    )
    grad_query_pre = grad_query_full.astype(jnp.bfloat16)
    grad_key_pre = grad_key_full.astype(jnp.bfloat16)
    grad_normed = self_q.back(grad_query_pre) + self_k.back(grad_key_pre) + self_v.back(grad_value)
    grad_start, shift_attn, scale_attn = pull_first(grad_normed)
    grad_hidden = grad_after + grad_start
    grad_modulated = jnp.stack((shift_attn, scale_attn, gate_attn, shift_ffn, scale_ffn, gate_ffn))
    grad_gains = jnp.stack((gain_query, gain_key, gain_cross_query, jnp.zeros_like(gain_query), gain_norm))
    grad_biases = jnp.stack(
        (
            column_sums(grad_query_pre),
            column_sums(grad_key_pre),
            column_sums(grad_value),
            column_sums(grad_branch),
            column_sums(grad_cross_query_pre),
            jnp.zeros_like(bias_norm),
            jnp.zeros_like(bias_norm),
            column_sums(grad_cross_branch),
            bias_norm,
            column_sums(grad_ffn_branch),
        )
    )
    small = (grad_modulated, grad_gains, grad_biases, column_sums(grad_pre))
    split = (
        (normed, grad_query_pre),
        (normed, grad_key_pre),
        (normed, grad_value),
        (attended, grad_branch),
        (crossed, grad_cross_query_pre),
        (cross_rows, grad_cross_branch),
        (ffn_normed, grad_pre),
        (activation, grad_ffn_branch),
    )
    return (mixed, grad_hidden, (grad_key_all, grad_value_all), grad_modulated, small, split)


def body(
    hidden,
    text,
    time_emb,
    modulation,
    self_in,
    self_out,
    cross_in,
    cross_out,
    ffn_in,
    ffn_out,
    gains,
    biases,
    ffn_bias,
    positions,
    cotangent,
):
    spot = (lax.axis_index("y"), lax.axis_index("core"))
    width = modulation.shape[1]
    length = ffn_bias.shape[0]
    heads_in = self_in.shape[0]
    attn_in_parts = fetch_split(jnp.concatenate([self_in, cross_in], axis=0), 1, spot)
    attn_out_parts = fetch_split(jnp.stack([self_out, cross_out]), 1, spot)
    ffn_in_parts = fetch_split(ffn_in, 0, spot, quarters=False)
    ffn_out_parts = fetch_split(ffn_out, 0, spot, quarters=False)
    modulation_full, gains_full, biases_full, ffn_bias_full = fetch_small(modulation, gains, biases, ffn_bias)
    in_split = [Split(tuple(part[i] for part in attn_in_parts), spot) for i in range(2 * heads_in)]
    out_split = [Split(tuple(part[i] for part in attn_out_parts), spot) for i in range(2)]
    weights = (
        modulation_full,
        in_split[0],
        in_split[1],
        in_split[2],
        out_split[0],
        in_split[3],
        in_split[4],
        in_split[5],
        out_split[1],
        Split(ffn_in_parts, spot),
        Split(ffn_out_parts, spot),
        gains_full,
        biases_full,
        ffn_bias_full,
    )
    cross_k, cross_v = in_split[4], in_split[5]
    gain_rows = gains_full.astype(jnp.float32)
    bias_rows = biases_full.astype(jnp.float32)
    clips, words, model = text.shape
    text_flat = text.reshape(clips * words, model)
    text_key_pre = cross_k.apply(text_flat) + bias_rows[5]
    text_key_full, pull_text_key = jax.vjp(rms_norm, text_key_pre, gain_rows[3])
    text_value = (cross_v.apply(text_flat) + bias_rows[6]).astype(jnp.bfloat16)
    text_key_low = text_key_full.astype(jnp.bfloat16)
    local_kv = jnp.concatenate(
        [part[i * words : (i + 1) * words] for part in (text_key_low, text_value) for i in range(clips)], axis=1
    )
    all_kv = lax.all_gather(local_kv, SEQ, axis=0, tiled=True)
    mixed_list = []
    hidden_list = []
    key_grads = []
    value_grads = []
    clock_list = []
    small_totals = None
    pair_lists = None
    for batch_index in range(clips):
        mixed, grad_hidden, text_grads, grad_clock, small, split = micro_step(
            weights,
            hidden[batch_index],
            all_kv[:, batch_index * model : (batch_index + 1) * model],
            all_kv[:, (clips + batch_index) * model : (clips + batch_index + 1) * model],
            time_emb[batch_index],
            positions[batch_index],
            cotangent[batch_index],
        )
        mixed_list.append(mixed)
        hidden_list.append(grad_hidden)
        key_grads.append(text_grads[0])
        value_grads.append(text_grads[1])
        clock_list.append(grad_clock)
        if small_totals is None:
            small_totals, pair_lists = small, [[pair] for pair in split]
        else:
            small_totals = tuple(a + b for a, b in zip(small_totals, small))
            for found, pair in zip(pair_lists, split):
                found.append(pair)
    pairs = [
        (jnp.concatenate([p[0] for p in found]), jnp.concatenate([p[1] for p in found]))
        for found in pair_lists
    ]
    split_grads = [
        split_weight.grad(rows, grad, quarters=index < 6)
        for index, (split_weight, (rows, grad)) in enumerate(
            zip(
                (in_split[0], in_split[1], in_split[2], out_split[0], in_split[3], out_split[1], weights[9], weights[10]),
                pairs,
            )
        )
    ]
    grad_kv = jnp.concatenate(key_grads + value_grads, axis=1).astype(jnp.bfloat16)
    owned_kv = lax.psum_scatter(grad_kv, SEQ, scatter_dimension=0, tiled=True).astype(jnp.float32)
    owned_parts = [owned_kv[:, i * model : (i + 1) * model] for i in range(2 * clips)]
    grad_text_key = jnp.concatenate(owned_parts[:clips], axis=0)
    grad_text_value = jnp.concatenate(owned_parts[clips:], axis=0).astype(jnp.bfloat16)
    grad_text_key_full, gain_cross_key = pull_text_key(grad_text_key)
    grad_text_key_pre = grad_text_key_full.astype(jnp.bfloat16)
    weight_cross_key = cross_k.grad(text_flat, grad_text_key_pre)
    weight_cross_value = cross_v.grad(text_flat, grad_text_value)
    grad_words = cross_k.back(grad_text_key_pre) + cross_v.back(grad_text_value)
    grad_mod, grad_gains, grad_biases, grad_ffn_bias_local = small_totals
    grad_gains = grad_gains.at[3].add(gain_cross_key)
    grad_biases = grad_biases.at[5].add(column_sums(grad_text_key_pre))
    grad_biases = grad_biases.at[6].add(column_sums(grad_text_value))
    attn_in_grads = tuple(
        jnp.stack(
            [split_grads[0][q], split_grads[1][q], split_grads[2][q], split_grads[4][q], weight_cross_key[q], weight_cross_value[q]]
        )
        for q in range(4)
    )
    attn_out_grads = tuple(jnp.stack([split_grads[3][q], split_grads[5][q]]) for q in range(4))
    attn_in_final = reduce_split(attn_in_grads, 1, spot)
    attn_out_final = reduce_split(attn_out_grads, 1, spot)
    ffn_in_final = reduce_half(split_grads[6], 0, spot)
    ffn_out_final = reduce_half(split_grads[7], 0, spot)
    grad_time = jnp.stack(clock_list)
    grad_mod, grad_gains, grad_biases, grad_ffn_bias, grad_time = reduce_small(
        grad_mod, grad_gains, grad_biases, grad_ffn_bias_local, grad_time, width, length
    )
    return (
        jnp.stack(mixed_list),
        jnp.stack(hidden_list),
        grad_words.reshape(clips, words, model),
        grad_time,
        grad_mod,
        attn_in_final[:heads_in],
        attn_out_final[0],
        attn_in_final[heads_in:],
        attn_out_final[1],
        ffn_in_final,
        ffn_out_final,
        grad_gains,
        grad_biases,
        grad_ffn_bias,
    )


def solution(mesh):
    devices = mesh.devices
    split_mesh = Mesh(
        devices.reshape(devices.shape[0] // 2, 2, devices.shape[1]), ("y", "core", "fsdp")
    )
    return jax.shard_map(
        body,
        mesh=split_mesh,
        in_specs=(
            P("fsdp", SEQ, None),
            P("fsdp", SEQ, None),
            P("fsdp", None, None),
            P(None, "fsdp"),
            P(None, "fsdp", None),
            P("fsdp", None),
            P(None, "fsdp", None),
            P("fsdp", None),
            P("fsdp", None),
            P("fsdp", None),
            P(None, "fsdp"),
            P(None, "fsdp"),
            P("fsdp"),
            P("fsdp", None, SEQ),
            P("fsdp", SEQ, None),
        ),
        out_specs=(
            P("fsdp", SEQ, None),
            P("fsdp", SEQ, None),
            P("fsdp", SEQ, None),
            P("fsdp", None, None),
            P(None, "fsdp"),
            P(None, "fsdp", None),
            P("fsdp", None),
            P(None, "fsdp", None),
            P("fsdp", None),
            P("fsdp", None),
            P("fsdp", None),
            P(None, "fsdp"),
            P(None, "fsdp"),
            P("fsdp"),
        ),
        check_vma=False,
    )
```

```python
import jax
import jax.numpy as jnp
from jax import lax
from jax.sharding import Mesh, PartitionSpec as P

HEADS = 12
HEAD = 128


EPSILON = 1e-06
SEQ = ("y", "core")
SWAP = [(0, 1), (1, 0)]


def matmul(operand, factor):
    return jnp.dot(operand, factor, preferred_element_type=jnp.float32)


def inner_rows(operand, factor):
    return lax.dot_general(
        operand, factor, (((0,), (0,)), ((), ())), preferred_element_type=jnp.float32
    )


def outer_cols(operand, factor):
    return lax.dot_general(
        operand, factor, (((operand.ndim - 1,), (1,)), ((), ())), preferred_element_type=jnp.float32
    )


def column_sums(tensor):
    return jnp.sum(tensor.astype(jnp.float32), axis=tuple(range(tensor.ndim - 1)))


def layer_norm(tensor):
    centered = tensor - jnp.mean(tensor, axis=-1, keepdims=True)
    return centered * lax.rsqrt(jnp.mean(centered * centered, axis=-1, keepdims=True) + EPSILON)


def rms_norm(tensor, weight):
    return tensor * lax.rsqrt(jnp.mean(tensor * tensor, axis=-1, keepdims=True) + EPSILON) * weight


def modulate_norm(tensor, shift, scale):
    return layer_norm(tensor) * (1.0 + scale) + shift


def affine_norm(tensor, weight, offset):
    return layer_norm(tensor) * weight + offset


def gelu_tanh(tensor):
    return jax.nn.gelu(tensor, approximate=True)


def rotary_tables(places, head_size, head_count):
    one_sixth = head_size // 6
    span_sizes = (head_size - 4 * one_sixth, 2 * one_sixth, 2 * one_sixth)
    angles = []
    for component in range(3):
        exponents = (
            jnp.arange(0, span_sizes[component], 2, dtype=jnp.float32) / span_sizes[component]
        )
        frequency = 1.0 / 10000.0**exponents
        angles.append(places[component].astype(jnp.float32)[:, None] * frequency[None, :])
    joined = jnp.concatenate(angles, axis=1)
    tiled_angles = jnp.tile(jnp.repeat(joined, 2, axis=1), (1, head_count))
    parity = jnp.where(jnp.arange(tiled_angles.shape[1]) % 2 == 0, -1.0, 1.0)
    return (jnp.cos(tiled_angles), jnp.sin(tiled_angles) * parity)


def rotate(tensor, cosine, signed_sine):
    even_lane = jnp.arange(tensor.shape[-1]) % 2 == 0
    swapped = jnp.where(even_lane, jnp.roll(tensor, -1, axis=-1), jnp.roll(tensor, 1, axis=-1))
    return tensor * cosine + swapped * signed_sine


def split_heads(tensor):
    return tensor.reshape(tensor.shape[0], tensor.shape[1], tensor.shape[2] // HEAD, HEAD)


def attend(queries, key_rows, value_rows):
    scores = jnp.einsum(
        "bqhd,bkhd->bhqk",
        split_heads(queries),
        split_heads(key_rows),
        preferred_element_type=jnp.float32,
    ) * HEAD ** (-0.5)
    row_max = jnp.max(scores, axis=-1, keepdims=True)
    exponentials = jnp.exp(scores - row_max)
    row_total = jnp.sum(exponentials, axis=-1, keepdims=True)
    probabilities = (exponentials / row_total).astype(jnp.bfloat16)
    result = jnp.einsum(
        "bhqk,bkhd->bqhd", probabilities, split_heads(value_rows), preferred_element_type=jnp.float32
    )
    return (result.reshape(queries.shape).astype(jnp.bfloat16), row_max + jnp.log(row_total))


def attend_back(queries, key_rows, value_rows, log_total, grad_rows):
    query_split = split_heads(queries)
    key_split = split_heads(key_rows)
    grad_split = split_heads(grad_rows)
    scale_factor = HEAD ** (-0.5)
    scores = (
        jnp.einsum("bqhd,bkhd->bhqk", query_split, key_split, preferred_element_type=jnp.float32)
        * scale_factor
    )
    probs_full = jnp.exp(scores - log_total)
    probs_low = probs_full.astype(jnp.bfloat16)
    grad_values = jnp.einsum(
        "bhqk,bqhd->bkhd", probs_low, grad_split, preferred_element_type=jnp.float32
    )
    grad_probs = jnp.einsum(
        "bqhd,bkhd->bhqk", grad_split, split_heads(value_rows), preferred_element_type=jnp.float32
    )
    grad_scores = (
        probs_full * (grad_probs - jnp.sum(grad_probs * probs_full, axis=-1, keepdims=True))
    ).astype(jnp.bfloat16)
    grad_queries = (
        jnp.einsum("bhqk,bkhd->bqhd", grad_scores, key_split, preferred_element_type=jnp.float32)
        * scale_factor
    )
    grad_keys = (
        jnp.einsum("bhqk,bqhd->bkhd", grad_scores, query_split, preferred_element_type=jnp.float32)
        * scale_factor
    )
    return (
        grad_queries.reshape(queries.shape),
        grad_keys.reshape(key_rows.shape),
        grad_values.reshape(value_rows.shape),
    )


def swap_core(tensor):
    return lax.ppermute(tensor, "core", SWAP)


def join(mine, other, core):
    width = mine.shape[-1]
    both = jnp.concatenate([other, mine, other], axis=-1)
    return lax.dynamic_slice_in_dim(both, (1 - core) * width, 2 * width, axis=-1)


def halves(tensor, core):
    width = tensor.shape[-1] // 2
    return (
        lax.dynamic_slice_in_dim(tensor, core * width, width, axis=-1),
        lax.dynamic_slice_in_dim(tensor, (1 - core) * width, width, axis=-1),
    )


def swap_y(tensor):
    return lax.ppermute(tensor, "y", SWAP)


class Split:
    def __init__(self, parts, spot):
        self.parts, self.spot = parts, spot

    def apply(self, rows):
        y, core = self.spot
        outs = [matmul(rows, part) for part in self.parts]
        if len(outs) == 2:
            return join(outs[0], outs[1], core)
        return join(join(outs[0], outs[1], y), join(outs[2], outs[3], y), core)

    def quarters(self, grad):
        y, core = self.spot
        grad_mine, grad_other = halves(grad, core)
        return halves(grad_mine, y) + halves(grad_other, y)

    def back(self, grad):
        if len(self.parts) == 2:
            grad_mine, grad_other = halves(grad, self.spot[1])
            return outer_cols(grad_mine, self.parts[0]) + outer_cols(grad_other, self.parts[1])
        pieces = [outer_cols(g, part) for g, part in zip(self.quarters(grad), self.parts)]
        return (pieces[0] + pieces[1]) + (pieces[2] + pieces[3])

    def grad(self, rows, grad, quarters=True):
        pieces = self.quarters(grad) if quarters else halves(grad, self.spot[1])
        return tuple(inner_rows(rows, g) for g in pieces)


def fetch_split(local, gather_axis, spot, quarters=True):
    y, core = spot
    if not quarters:
        width = local.shape[-1] // 2
        part = lax.dynamic_slice_in_dim(local, core * width, width, axis=-1)
        mine = lax.all_gather(part, "fsdp", axis=gather_axis, tiled=True)
        return (mine, swap_core(mine))
    width = local.shape[-1] // 4
    part = lax.dynamic_slice_in_dim(local, (2 * core + y) * width, width, axis=-1)
    own = lax.all_gather(part, "fsdp", axis=gather_axis, tiled=True)
    y_part = swap_y(own)
    return (own, y_part, swap_core(own), swap_core(y_part))


def reduce_split(parts, scatter_axis, spot):
    y, core = spot
    own, y_part, core_part, cross_part = parts
    from_core = swap_core(core_part.astype(jnp.bfloat16)).astype(jnp.float32)
    from_cross = swap_core(cross_part.astype(jnp.bfloat16)).astype(jnp.float32)
    chip_own = own + from_core
    chip_y = (y_part + from_cross).astype(jnp.bfloat16)
    total = (chip_own + swap_y(chip_y).astype(jnp.float32)).astype(jnp.bfloat16)
    owned = lax.psum_scatter(total, "fsdp", scatter_dimension=scatter_axis, tiled=True)
    owned_y = swap_y(owned)
    mine = join(owned, owned_y, y)
    return join(mine, swap_core(mine), core).astype(jnp.float32)


def reduce_half(parts, scatter_axis, spot):
    y, core = spot
    mine, other = parts
    received = swap_core(other.astype(jnp.bfloat16)).astype(jnp.float32)
    chip = (mine + received).astype(jnp.bfloat16)
    owned = lax.psum_scatter(chip, "fsdp", scatter_dimension=scatter_axis, tiled=True)
    summed = owned.astype(jnp.float32) + swap_y(owned).astype(jnp.float32)
    return join(summed, swap_core(summed), core)


def fetch_small(modulation, gains, biases, ffn_bias):
    width = modulation.shape[1]
    length = ffn_bias.shape[0]
    rows = -(-length // width)
    padded = jnp.pad(ffn_bias, (0, rows * width - length)).reshape(rows, width)
    packed = jnp.concatenate([modulation, gains, biases, padded], axis=0)
    full = lax.all_gather(packed, "fsdp", axis=1, tiled=True)
    shards = full.shape[1] // width
    bias_rows = full[21:].reshape(rows, shards, width).transpose(1, 0, 2)
    bias_full = bias_rows.reshape(shards, rows * width)[:, :length].reshape(shards * length)
    return full[:6], full[6:11], full[11:21], bias_full


def reduce_small(grad_mod, grad_gains, grad_biases, grad_ffn_bias, grad_time, width, length):
    rows = -(-length // width)
    shards = grad_mod.shape[1] // width
    bias_rows = jnp.pad(grad_ffn_bias.reshape(shards, length), ((0, 0), (0, rows * width - length)))
    bias_rows = bias_rows.reshape(shards, rows, width).transpose(1, 0, 2).reshape(rows, shards * width)
    packed = jnp.concatenate([grad_mod, grad_gains, grad_biases, bias_rows], axis=0)
    owned = lax.psum_scatter(packed, "fsdp", scatter_dimension=1, tiled=True)
    flat = jnp.concatenate([owned.reshape(-1), grad_time.reshape(-1)])
    summed = lax.psum(flat, SEQ)
    owned = summed[: owned.size].reshape(owned.shape)
    grad_time = summed[owned.size :].reshape(grad_time.shape)
    bias_owned = owned[21:].reshape(-1)[:length]
    return owned[:6], owned[6:11], owned[11:21], bias_owned, grad_time


def micro_step(weights, hidden, key_all, value_all, time_emb, places, cotangent):
    modulation, self_q, self_k, self_v, self_o, cross_q, cross_k, cross_v, cross_o, ffn_in, ffn_out, gains, biases, ffn_bias = (
        weights
    )
    gain_rows = gains.astype(jnp.float32)
    bias_rows = biases.astype(jnp.float32)
    modulated = modulation.astype(jnp.float32)[None] + time_emb.astype(jnp.float32)
    mod = [modulated[:, row, None, :] for row in range(6)]
    cosine, signed_sine = jax.vmap(lambda clip_places: rotary_tables(clip_places, HEAD, HEADS))(places)
    residual_in = hidden.astype(jnp.float32)
    normed_full, pull_first = jax.vjp(modulate_norm, residual_in, mod[0], mod[1])
    normed = normed_full.astype(jnp.bfloat16)
    query_pre = self_q.apply(normed) + bias_rows[0]
    key_pre = self_k.apply(normed) + bias_rows[1]
    value_low = (self_v.apply(normed) + bias_rows[2]).astype(jnp.bfloat16)

    def turn_both(query_input, key_input, gain_query, gain_key):
        return (
            rotate(rms_norm(query_input, gain_query), cosine, signed_sine),
            rotate(rms_norm(key_input, gain_key), cosine, signed_sine),
        )

    turned, pull_turn = jax.vjp(turn_both, query_pre, key_pre, gain_rows[0], gain_rows[1])
    query_heads, key_heads, value_heads = (
        lax.all_to_all(turned[0].astype(jnp.bfloat16), SEQ, split_axis=2, concat_axis=1, tiled=True),
        lax.all_to_all(turned[1].astype(jnp.bfloat16), SEQ, split_axis=2, concat_axis=1, tiled=True),
        lax.all_to_all(value_low, SEQ, split_axis=2, concat_axis=1, tiled=True),
    )
    attn_heads, log_total = attend(query_heads, key_heads, value_heads)
    attended = lax.all_to_all(attn_heads, SEQ, split_axis=1, concat_axis=2, tiled=True)
    branch = self_o.apply(attended) + bias_rows[3]
    after_attn = residual_in + branch * mod[2]
    crossed_full, pull_cross = jax.vjp(affine_norm, after_attn, gain_rows[4], bias_rows[8])
    crossed = crossed_full.astype(jnp.bfloat16)
    cross_query_pre = cross_q.apply(crossed) + bias_rows[4]
    cross_query_full, pull_cross_query = jax.vjp(rms_norm, cross_query_pre, gain_rows[2])
    cross_query = cross_query_full.astype(jnp.bfloat16)
    cross_rows, cross_total = attend(cross_query, key_all, value_all)
    second = after_attn + cross_o.apply(cross_rows) + bias_rows[7]
    ffn_normed_full, pull_second = jax.vjp(modulate_norm, second, mod[3], mod[4])
    ffn_normed = ffn_normed_full.astype(jnp.bfloat16)
    pre_act = ffn_in.apply(ffn_normed) + ffn_bias.astype(jnp.float32)
    activation_full, pull_gelu = jax.vjp(gelu_tanh, pre_act)
    activation = activation_full.astype(jnp.bfloat16)
    ffn_branch = ffn_out.apply(activation) + bias_rows[9]
    mixed = (second + ffn_branch * mod[5]).astype(jnp.bfloat16)
    grad_output = cotangent.astype(jnp.float32)
    gate_ffn = jnp.sum(grad_output * ffn_branch, axis=1)
    grad_ffn_branch = (grad_output * mod[5]).astype(jnp.bfloat16)
    grad_pre_full = pull_gelu(ffn_out.back(grad_ffn_branch))[0]
    grad_pre = grad_pre_full.astype(jnp.bfloat16)
    grad_second_part, shift_ffn, scale_ffn = pull_second(ffn_in.back(grad_pre))
    grad_second = grad_output + grad_second_part
    grad_cross_branch = grad_second.astype(jnp.bfloat16)
    grad_cross_rows = cross_o.back(grad_cross_branch).astype(jnp.bfloat16)
    grad_cross_query, grad_key_all, grad_value_all = attend_back(
        cross_query, key_all, value_all, cross_total, grad_cross_rows
    )
    grad_cross_query_full, gain_cross_query = pull_cross_query(grad_cross_query)
    grad_cross_query_pre = grad_cross_query_full.astype(jnp.bfloat16)
    grad_after_part, gain_norm, bias_norm = pull_cross(cross_q.back(grad_cross_query_pre))
    grad_after = grad_second + grad_after_part
    gate_attn = jnp.sum(grad_after * branch, axis=1)
    grad_branch = (grad_after * mod[2]).astype(jnp.bfloat16)
    grad_attended = self_o.back(grad_branch).astype(jnp.bfloat16)
    grad_attn_heads = lax.all_to_all(grad_attended, SEQ, split_axis=2, concat_axis=1, tiled=True)
    grad_query_heads, grad_key_heads, grad_value_heads = attend_back(
        query_heads, key_heads, value_heads, log_total, grad_attn_heads
    )
    grad_query_turned, grad_key_turned, grad_value = (
        lax.all_to_all(
            grad_query_heads.astype(jnp.bfloat16), SEQ, split_axis=1, concat_axis=2, tiled=True
        ),
        lax.all_to_all(
            grad_key_heads.astype(jnp.bfloat16), SEQ, split_axis=1, concat_axis=2, tiled=True
        ),
        lax.all_to_all(
            grad_value_heads.astype(jnp.bfloat16), SEQ, split_axis=1, concat_axis=2, tiled=True
        ),
    )
    grad_query_full, grad_key_full, gain_query, gain_key = pull_turn(
        (grad_query_turned.astype(jnp.float32), grad_key_turned.astype(jnp.float32))
    )
    grad_query_pre = grad_query_full.astype(jnp.bfloat16)
    grad_key_pre = grad_key_full.astype(jnp.bfloat16)
    grad_normed = self_q.back(grad_query_pre) + self_k.back(grad_key_pre) + self_v.back(grad_value)
    grad_start, shift_attn, scale_attn = pull_first(grad_normed)
    grad_hidden = grad_after + grad_start
    grad_modulated = jnp.stack(
        (shift_attn[:, 0], scale_attn[:, 0], gate_attn, shift_ffn[:, 0], scale_ffn[:, 0], gate_ffn), axis=1
    )
    grad_gains = jnp.stack((gain_query, gain_key, gain_cross_query, jnp.zeros_like(gain_query), gain_norm))
    grad_biases = jnp.stack(
        (
            column_sums(grad_query_pre),
            column_sums(grad_key_pre),
            column_sums(grad_value),
            column_sums(grad_branch),
            column_sums(grad_cross_query_pre),
            jnp.zeros_like(bias_norm),
            jnp.zeros_like(bias_norm),
            column_sums(grad_cross_branch),
            bias_norm,
            column_sums(grad_ffn_branch),
        )
    )
    small = (jnp.sum(grad_modulated, axis=0), grad_gains, grad_biases, column_sums(grad_pre))
    split = (
        (normed, grad_query_pre),
        (normed, grad_key_pre),
        (normed, grad_value),
        (attended, grad_branch),
        (crossed, grad_cross_query_pre),
        (cross_rows, grad_cross_branch),
        (ffn_normed, grad_pre),
        (activation, grad_ffn_branch),
    )
    return (mixed, grad_hidden, (grad_key_all, grad_value_all), grad_modulated, small, split)


def body(
    hidden,
    text,
    time_emb,
    modulation,
    self_in,
    self_out,
    cross_in,
    cross_out,
    ffn_in,
    ffn_out,
    gains,
    biases,
    ffn_bias,
    positions,
    cotangent,
):
    spot = (lax.axis_index("y"), lax.axis_index("core"))
    width = modulation.shape[1]
    length = ffn_bias.shape[0]
    heads_in = self_in.shape[0]
    attn_in_parts = fetch_split(jnp.concatenate([self_in, cross_in], axis=0), 1, spot)
    attn_out_parts = fetch_split(jnp.stack([self_out, cross_out]), 1, spot)
    ffn_in_parts = fetch_split(ffn_in, 0, spot, quarters=False)
    ffn_out_parts = fetch_split(ffn_out, 0, spot, quarters=False)
    modulation_full, gains_full, biases_full, ffn_bias_full = fetch_small(modulation, gains, biases, ffn_bias)
    in_split = [Split(tuple(part[i] for part in attn_in_parts), spot) for i in range(2 * heads_in)]
    out_split = [Split(tuple(part[i] for part in attn_out_parts), spot) for i in range(2)]
    weights = (
        modulation_full,
        in_split[0],
        in_split[1],
        in_split[2],
        out_split[0],
        in_split[3],
        in_split[4],
        in_split[5],
        out_split[1],
        Split(ffn_in_parts, spot),
        Split(ffn_out_parts, spot),
        gains_full,
        biases_full,
        ffn_bias_full,
    )
    cross_k, cross_v = in_split[4], in_split[5]
    gain_rows = gains_full.astype(jnp.float32)
    bias_rows = biases_full.astype(jnp.float32)
    clips, words, model = text.shape
    text_flat = text.reshape(clips * words, model)
    text_key_pre = cross_k.apply(text_flat) + bias_rows[5]
    text_key_full, pull_text_key = jax.vjp(rms_norm, text_key_pre, gain_rows[3])
    text_value = (cross_v.apply(text_flat) + bias_rows[6]).astype(jnp.bfloat16)
    text_key_low = text_key_full.astype(jnp.bfloat16)
    local_kv = jnp.concatenate(
        [part[i * words : (i + 1) * words] for part in (text_key_low, text_value) for i in range(clips)], axis=1
    )
    all_kv = lax.all_gather(local_kv, SEQ, axis=0, tiled=True)
    key_all = jnp.stack([all_kv[:, i * model : (i + 1) * model] for i in range(clips)])
    value_all = jnp.stack([all_kv[:, (clips + i) * model : (clips + i + 1) * model] for i in range(clips)])
    mixed, grad_hidden, text_grads, grad_time, small_totals, split = micro_step(
        weights, hidden, key_all, value_all, time_emb, positions, cotangent
    )
    key_grads = [text_grads[0][i] for i in range(clips)]
    value_grads = [text_grads[1][i] for i in range(clips)]
    pairs = [(rows.reshape(-1, rows.shape[-1]), grad.reshape(-1, grad.shape[-1])) for rows, grad in split]
    split_grads = [
        split_weight.grad(rows, grad, quarters=index < 6)
        for index, (split_weight, (rows, grad)) in enumerate(
            zip(
                (in_split[0], in_split[1], in_split[2], out_split[0], in_split[3], out_split[1], weights[9], weights[10]),
                pairs,
            )
        )
    ]
    grad_kv = jnp.concatenate(key_grads + value_grads, axis=1).astype(jnp.bfloat16)
    owned_kv = lax.psum_scatter(grad_kv, SEQ, scatter_dimension=0, tiled=True).astype(jnp.float32)
    owned_parts = [owned_kv[:, i * model : (i + 1) * model] for i in range(2 * clips)]
    grad_text_key = jnp.concatenate(owned_parts[:clips], axis=0)
    grad_text_value = jnp.concatenate(owned_parts[clips:], axis=0).astype(jnp.bfloat16)
    grad_text_key_full, gain_cross_key = pull_text_key(grad_text_key)
    grad_text_key_pre = grad_text_key_full.astype(jnp.bfloat16)
    weight_cross_key = cross_k.grad(text_flat, grad_text_key_pre)
    weight_cross_value = cross_v.grad(text_flat, grad_text_value)
    grad_words = cross_k.back(grad_text_key_pre) + cross_v.back(grad_text_value)
    grad_mod, grad_gains, grad_biases, grad_ffn_bias_local = small_totals
    grad_gains = grad_gains.at[3].add(gain_cross_key)
    grad_biases = grad_biases.at[5].add(column_sums(grad_text_key_pre))
    grad_biases = grad_biases.at[6].add(column_sums(grad_text_value))
    attn_in_grads = tuple(
        jnp.stack(
            [split_grads[0][q], split_grads[1][q], split_grads[2][q], split_grads[4][q], weight_cross_key[q], weight_cross_value[q]]
        )
        for q in range(4)
    )
    attn_out_grads = tuple(jnp.stack([split_grads[3][q], split_grads[5][q]]) for q in range(4))
    attn_in_final = reduce_split(attn_in_grads, 1, spot)
    attn_out_final = reduce_split(attn_out_grads, 1, spot)
    ffn_in_final = reduce_half(split_grads[6], 0, spot)
    ffn_out_final = reduce_half(split_grads[7], 0, spot)
    grad_mod, grad_gains, grad_biases, grad_ffn_bias, grad_time = reduce_small(
        grad_mod, grad_gains, grad_biases, grad_ffn_bias_local, grad_time, width, length
    )
    return (
        mixed,
        grad_hidden,
        grad_words.reshape(clips, words, model),
        grad_time,
        grad_mod,
        attn_in_final[:heads_in],
        attn_out_final[0],
        attn_in_final[heads_in:],
        attn_out_final[1],
        ffn_in_final,
        ffn_out_final,
        grad_gains,
        grad_biases,
        grad_ffn_bias,
    )


def solution(mesh):
    devices = mesh.devices
    split_mesh = Mesh(
        devices.reshape(devices.shape[0] // 2, 2, devices.shape[1]), ("y", "core", "fsdp")
    )
    return jax.shard_map(
        body,
        mesh=split_mesh,
        in_specs=(
            P("fsdp", SEQ, None),
            P("fsdp", SEQ, None),
            P("fsdp", None, None),
            P(None, "fsdp"),
            P(None, "fsdp", None),
            P("fsdp", None),
            P(None, "fsdp", None),
            P("fsdp", None),
            P("fsdp", None),
            P("fsdp", None),
            P(None, "fsdp"),
            P(None, "fsdp"),
            P("fsdp"),
            P("fsdp", None, SEQ),
            P("fsdp", SEQ, None),
        ),
        out_specs=(
            P("fsdp", SEQ, None),
            P("fsdp", SEQ, None),
            P("fsdp", SEQ, None),
            P("fsdp", None, None),
            P(None, "fsdp"),
            P(None, "fsdp", None),
            P("fsdp", None),
            P(None, "fsdp", None),
            P("fsdp", None),
            P("fsdp", None),
            P("fsdp", None),
            P(None, "fsdp"),
            P(None, "fsdp"),
            P("fsdp"),
        ),
        check_vma=False,
    )
```

```python
import jax
import jax.numpy as jnp
from jax import lax
from jax.sharding import Mesh, PartitionSpec as P

HEADS = 12
HEAD = 128


EPSILON = 1e-06
SEQ = ("y", "core")
SWAP = [(0, 1), (1, 0)]


def matmul(operand, factor):
    return jnp.dot(operand, factor, preferred_element_type=jnp.float32)


def inner_rows(operand, factor):
    return lax.dot_general(
        operand, factor, (((0,), (0,)), ((), ())), preferred_element_type=jnp.float32
    )


def outer_cols(operand, factor):
    return lax.dot_general(
        operand, factor, (((operand.ndim - 1,), (1,)), ((), ())), preferred_element_type=jnp.float32
    )


def column_sums(tensor):
    return jnp.sum(tensor.astype(jnp.float32), axis=tuple(range(tensor.ndim - 1)))


def layer_norm(tensor):
    centered = tensor - jnp.mean(tensor, axis=-1, keepdims=True)
    return centered * lax.rsqrt(jnp.mean(centered * centered, axis=-1, keepdims=True) + EPSILON)


def rms_norm(tensor, weight):
    return tensor * lax.rsqrt(jnp.mean(tensor * tensor, axis=-1, keepdims=True) + EPSILON) * weight


def modulate_norm(tensor, shift, scale):
    return layer_norm(tensor) * (1.0 + scale) + shift


def affine_norm(tensor, weight, offset):
    return layer_norm(tensor) * weight + offset


def gelu_tanh(tensor):
    return jax.nn.gelu(tensor, approximate=True)


def rotary_tables(places, head_size, head_count):
    one_sixth = head_size // 6
    span_sizes = (head_size - 4 * one_sixth, 2 * one_sixth, 2 * one_sixth)
    angles = []
    for component in range(3):
        exponents = (
            jnp.arange(0, span_sizes[component], 2, dtype=jnp.float32) / span_sizes[component]
        )
        frequency = 1.0 / 10000.0**exponents
        angles.append(places[component].astype(jnp.float32)[:, None] * frequency[None, :])
    joined = jnp.concatenate(angles, axis=1)
    tiled_angles = jnp.tile(jnp.repeat(joined, 2, axis=1), (1, head_count))
    parity = jnp.where(jnp.arange(tiled_angles.shape[1]) % 2 == 0, -1.0, 1.0)
    return (jnp.cos(tiled_angles), jnp.sin(tiled_angles) * parity)


def rotate(tensor, cosine, signed_sine):
    even_lane = jnp.arange(tensor.shape[-1]) % 2 == 0
    swapped = jnp.where(even_lane, jnp.roll(tensor, -1, axis=-1), jnp.roll(tensor, 1, axis=-1))
    return tensor * cosine + swapped * signed_sine


def split_heads(tensor):
    return tensor.reshape(tensor.shape[0], tensor.shape[1], tensor.shape[2] // HEAD, HEAD)


def attend(queries, key_rows, value_rows):
    scores = jnp.einsum(
        "bqhd,bkhd->bhqk",
        split_heads(queries),
        split_heads(key_rows),
        preferred_element_type=jnp.float32,
    ) * HEAD ** (-0.5)
    row_max = jnp.max(scores, axis=-1, keepdims=True)
    exponentials = jnp.exp(scores - row_max)
    row_total = jnp.sum(exponentials, axis=-1, keepdims=True)
    probabilities = (exponentials / row_total).astype(jnp.bfloat16)
    result = jnp.einsum(
        "bhqk,bkhd->bqhd", probabilities, split_heads(value_rows), preferred_element_type=jnp.float32
    )
    return (result.reshape(queries.shape).astype(jnp.bfloat16), row_max + jnp.log(row_total))


def attend_back(queries, key_rows, value_rows, log_total, grad_rows):
    query_split = split_heads(queries)
    key_split = split_heads(key_rows)
    grad_split = split_heads(grad_rows)
    scale_factor = HEAD ** (-0.5)
    scores = (
        jnp.einsum("bqhd,bkhd->bhqk", query_split, key_split, preferred_element_type=jnp.float32)
        * scale_factor
    )
    probs_full = jnp.exp(scores - log_total)
    probs_low = probs_full.astype(jnp.bfloat16)
    grad_values = jnp.einsum(
        "bhqk,bqhd->bkhd", probs_low, grad_split, preferred_element_type=jnp.float32
    )
    grad_probs = jnp.einsum(
        "bqhd,bkhd->bhqk", grad_split, split_heads(value_rows), preferred_element_type=jnp.float32
    )
    grad_scores = (
        probs_full * (grad_probs - jnp.sum(grad_probs * probs_full, axis=-1, keepdims=True))
    ).astype(jnp.bfloat16)
    grad_queries = (
        jnp.einsum("bhqk,bkhd->bqhd", grad_scores, key_split, preferred_element_type=jnp.float32)
        * scale_factor
    )
    grad_keys = (
        jnp.einsum("bhqk,bqhd->bkhd", grad_scores, query_split, preferred_element_type=jnp.float32)
        * scale_factor
    )
    return (
        grad_queries.reshape(queries.shape),
        grad_keys.reshape(key_rows.shape),
        grad_values.reshape(value_rows.shape),
    )


def swap_core(tensor):
    return lax.ppermute(tensor, "core", SWAP)


def join(mine, other, core):
    width = mine.shape[-1]
    both = jnp.concatenate([other, mine, other], axis=-1)
    return lax.dynamic_slice_in_dim(both, (1 - core) * width, 2 * width, axis=-1)


def halves(tensor, core):
    width = tensor.shape[-1] // 2
    return (
        lax.dynamic_slice_in_dim(tensor, core * width, width, axis=-1),
        lax.dynamic_slice_in_dim(tensor, (1 - core) * width, width, axis=-1),
    )


def swap_y(tensor):
    return lax.ppermute(tensor, "y", SWAP)


class Split:
    def __init__(self, parts, spot):
        self.parts, self.spot = parts, spot

    def apply(self, rows):
        y, core = self.spot
        outs = [matmul(rows, part) for part in self.parts]
        if len(outs) == 2:
            return join(outs[0], outs[1], core)
        return join(join(outs[0], outs[1], y), join(outs[2], outs[3], y), core)

    def quarters(self, grad):
        y, core = self.spot
        grad_mine, grad_other = halves(grad, core)
        return halves(grad_mine, y) + halves(grad_other, y)

    def back(self, grad):
        if len(self.parts) == 2:
            grad_mine, grad_other = halves(grad, self.spot[1])
            return outer_cols(grad_mine, self.parts[0]) + outer_cols(grad_other, self.parts[1])
        pieces = [outer_cols(g, part) for g, part in zip(self.quarters(grad), self.parts)]
        return (pieces[0] + pieces[1]) + (pieces[2] + pieces[3])

    def grad(self, rows, grad, quarters=True):
        pieces = self.quarters(grad) if quarters else halves(grad, self.spot[1])
        return tuple(inner_rows(rows, g) for g in pieces)


def fetch_split(local, gather_axis, spot, quarters=True):
    y, core = spot
    if not quarters:
        width = local.shape[-1] // 2
        part = lax.dynamic_slice_in_dim(local, core * width, width, axis=-1)
        mine = lax.all_gather(part, "fsdp", axis=gather_axis, tiled=True)
        return (mine, swap_core(mine))
    width = local.shape[-1] // 4
    part = lax.dynamic_slice_in_dim(local, (2 * core + y) * width, width, axis=-1)
    own = lax.all_gather(part, "fsdp", axis=gather_axis, tiled=True)
    y_part = swap_y(own)
    return (own, y_part, swap_core(own), swap_core(y_part))


def reduce_split(parts, scatter_axis, spot):
    y, core = spot
    own, y_part, core_part, cross_part = parts
    from_core = swap_core(core_part.astype(jnp.bfloat16)).astype(jnp.float32)
    from_cross = swap_core(cross_part.astype(jnp.bfloat16)).astype(jnp.float32)
    chip_own = own + from_core
    chip_y = (y_part + from_cross).astype(jnp.bfloat16)
    total = (chip_own + swap_y(chip_y).astype(jnp.float32)).astype(jnp.bfloat16)
    owned = lax.psum_scatter(total, "fsdp", scatter_dimension=scatter_axis, tiled=True)
    owned_y = swap_y(owned)
    mine = join(owned, owned_y, y)
    return join(mine, swap_core(mine), core).astype(jnp.float32)


def reduce_half(parts, scatter_axis, spot):
    y, core = spot
    mine, other = parts
    received = swap_core(other.astype(jnp.bfloat16)).astype(jnp.float32)
    chip = (mine + received).astype(jnp.bfloat16)
    owned = lax.psum_scatter(chip, "fsdp", scatter_dimension=scatter_axis, tiled=True)
    summed = owned.astype(jnp.float32) + swap_y(owned).astype(jnp.float32)
    return join(summed, swap_core(summed), core)


def fetch_small(modulation, gains, biases, ffn_bias):
    width = modulation.shape[1]
    length = ffn_bias.shape[0]
    rows = -(-length // width)
    padded = jnp.pad(ffn_bias, (0, rows * width - length)).reshape(rows, width)
    packed = jnp.concatenate([modulation, gains, biases, padded], axis=0)
    full = lax.all_gather(packed, "fsdp", axis=1, tiled=True)
    shards = full.shape[1] // width
    bias_rows = full[21:].reshape(rows, shards, width).transpose(1, 0, 2)
    bias_full = bias_rows.reshape(shards, rows * width)[:, :length].reshape(shards * length)
    return full[:6], full[6:11], full[11:21], bias_full


def reduce_small(grad_mod, grad_gains, grad_biases, grad_ffn_bias, grad_time, width, length):
    rows = -(-length // width)
    shards = grad_mod.shape[1] // width
    bias_rows = jnp.pad(grad_ffn_bias.reshape(shards, length), ((0, 0), (0, rows * width - length)))
    bias_rows = bias_rows.reshape(shards, rows, width).transpose(1, 0, 2).reshape(rows, shards * width)
    packed = jnp.concatenate([grad_mod, grad_gains, grad_biases, bias_rows], axis=0)
    place = lax.axis_index("fsdp")
    slots = jnp.zeros((shards, grad_time.size), jnp.float32)
    slots = lax.dynamic_update_slice_in_dim(slots, grad_time.reshape(1, -1), place, axis=0)
    flat = jnp.concatenate([packed.reshape(-1), slots.reshape(-1)])
    summed = lax.psum(flat, ("y", "core", "fsdp"))
    owned = lax.dynamic_slice_in_dim(summed[: packed.size].reshape(packed.shape), place * width, width, axis=1)
    grad_time = lax.dynamic_slice_in_dim(summed[packed.size :].reshape(shards, -1), place, 1, axis=0)
    grad_time = grad_time.reshape(grad_time.size // (6 * packed.shape[1]), 6, packed.shape[1])
    bias_owned = owned[21:].reshape(-1)[:length]
    return owned[:6], owned[6:11], owned[11:21], bias_owned, grad_time


def micro_step(weights, hidden, key_all, value_all, time_emb, places, cotangent):
    modulation, self_q, self_k, self_v, self_o, cross_q, cross_k, cross_v, cross_o, ffn_in, ffn_out, gains, biases, ffn_bias = (
        weights
    )
    gain_rows = gains.astype(jnp.float32)
    bias_rows = biases.astype(jnp.float32)
    modulated = modulation.astype(jnp.float32)[None] + time_emb.astype(jnp.float32)
    mod = [modulated[:, row, None, :] for row in range(6)]
    cosine, signed_sine = jax.vmap(lambda clip_places: rotary_tables(clip_places, HEAD, HEADS))(places)
    residual_in = hidden.astype(jnp.float32)
    normed_full, pull_first = jax.vjp(modulate_norm, residual_in, mod[0], mod[1])
    normed = normed_full.astype(jnp.bfloat16)
    query_pre = self_q.apply(normed) + bias_rows[0]
    key_pre = self_k.apply(normed) + bias_rows[1]
    value_low = (self_v.apply(normed) + bias_rows[2]).astype(jnp.bfloat16)

    def turn_both(query_input, key_input, gain_query, gain_key):
        return (
            rotate(rms_norm(query_input, gain_query), cosine, signed_sine),
            rotate(rms_norm(key_input, gain_key), cosine, signed_sine),
        )

    turned, pull_turn = jax.vjp(turn_both, query_pre, key_pre, gain_rows[0], gain_rows[1])
    query_heads, key_heads, value_heads = (
        lax.all_to_all(turned[0].astype(jnp.bfloat16), SEQ, split_axis=2, concat_axis=1, tiled=True),
        lax.all_to_all(turned[1].astype(jnp.bfloat16), SEQ, split_axis=2, concat_axis=1, tiled=True),
        lax.all_to_all(value_low, SEQ, split_axis=2, concat_axis=1, tiled=True),
    )
    attn_heads, log_total = attend(query_heads, key_heads, value_heads)
    attended = lax.all_to_all(attn_heads, SEQ, split_axis=1, concat_axis=2, tiled=True)
    branch = self_o.apply(attended) + bias_rows[3]
    after_attn = residual_in + branch * mod[2]
    crossed_full, pull_cross = jax.vjp(affine_norm, after_attn, gain_rows[4], bias_rows[8])
    crossed = crossed_full.astype(jnp.bfloat16)
    cross_query_pre = cross_q.apply(crossed) + bias_rows[4]
    cross_query_full, pull_cross_query = jax.vjp(rms_norm, cross_query_pre, gain_rows[2])
    cross_query = cross_query_full.astype(jnp.bfloat16)
    cross_rows, cross_total = attend(cross_query, key_all, value_all)
    second = after_attn + cross_o.apply(cross_rows) + bias_rows[7]
    ffn_normed_full, pull_second = jax.vjp(modulate_norm, second, mod[3], mod[4])
    ffn_normed = ffn_normed_full.astype(jnp.bfloat16)
    pre_act = ffn_in.apply(ffn_normed) + ffn_bias.astype(jnp.float32)
    activation_full, pull_gelu = jax.vjp(gelu_tanh, pre_act)
    activation = activation_full.astype(jnp.bfloat16)
    ffn_branch = ffn_out.apply(activation) + bias_rows[9]
    mixed = (second + ffn_branch * mod[5]).astype(jnp.bfloat16)
    grad_output = cotangent.astype(jnp.float32)
    gate_ffn = jnp.sum(grad_output * ffn_branch, axis=1)
    grad_ffn_branch = (grad_output * mod[5]).astype(jnp.bfloat16)
    grad_pre_full = pull_gelu(ffn_out.back(grad_ffn_branch))[0]
    grad_pre = grad_pre_full.astype(jnp.bfloat16)
    grad_second_part, shift_ffn, scale_ffn = pull_second(ffn_in.back(grad_pre))
    grad_second = grad_output + grad_second_part
    grad_cross_branch = grad_second.astype(jnp.bfloat16)
    grad_cross_rows = cross_o.back(grad_cross_branch).astype(jnp.bfloat16)
    grad_cross_query, grad_key_all, grad_value_all = attend_back(
        cross_query, key_all, value_all, cross_total, grad_cross_rows
    )
    grad_cross_query_full, gain_cross_query = pull_cross_query(grad_cross_query)
    grad_cross_query_pre = grad_cross_query_full.astype(jnp.bfloat16)
    grad_after_part, gain_norm, bias_norm = pull_cross(cross_q.back(grad_cross_query_pre))
    grad_after = grad_second + grad_after_part
    gate_attn = jnp.sum(grad_after * branch, axis=1)
    grad_branch = (grad_after * mod[2]).astype(jnp.bfloat16)
    grad_attended = self_o.back(grad_branch).astype(jnp.bfloat16)
    grad_attn_heads = lax.all_to_all(grad_attended, SEQ, split_axis=2, concat_axis=1, tiled=True)
    grad_query_heads, grad_key_heads, grad_value_heads = attend_back(
        query_heads, key_heads, value_heads, log_total, grad_attn_heads
    )
    grad_query_turned, grad_key_turned, grad_value = (
        lax.all_to_all(
            grad_query_heads.astype(jnp.bfloat16), SEQ, split_axis=1, concat_axis=2, tiled=True
        ),
        lax.all_to_all(
            grad_key_heads.astype(jnp.bfloat16), SEQ, split_axis=1, concat_axis=2, tiled=True
        ),
        lax.all_to_all(
            grad_value_heads.astype(jnp.bfloat16), SEQ, split_axis=1, concat_axis=2, tiled=True
        ),
    )
    grad_query_full, grad_key_full, gain_query, gain_key = pull_turn(
        (grad_query_turned.astype(jnp.float32), grad_key_turned.astype(jnp.float32))
    )
    grad_query_pre = grad_query_full.astype(jnp.bfloat16)
    grad_key_pre = grad_key_full.astype(jnp.bfloat16)
    grad_normed = self_q.back(grad_query_pre) + self_k.back(grad_key_pre) + self_v.back(grad_value)
    grad_start, shift_attn, scale_attn = pull_first(grad_normed)
    grad_hidden = grad_after + grad_start
    grad_modulated = jnp.stack(
        (shift_attn[:, 0], scale_attn[:, 0], gate_attn, shift_ffn[:, 0], scale_ffn[:, 0], gate_ffn), axis=1
    )
    grad_gains = jnp.stack((gain_query, gain_key, gain_cross_query, jnp.zeros_like(gain_query), gain_norm))
    grad_biases = jnp.stack(
        (
            column_sums(grad_query_pre),
            column_sums(grad_key_pre),
            column_sums(grad_value),
            column_sums(grad_branch),
            column_sums(grad_cross_query_pre),
            jnp.zeros_like(bias_norm),
            jnp.zeros_like(bias_norm),
            column_sums(grad_cross_branch),
            bias_norm,
            column_sums(grad_ffn_branch),
        )
    )
    small = (jnp.sum(grad_modulated, axis=0), grad_gains, grad_biases, column_sums(grad_pre))
    split = (
        (normed, grad_query_pre),
        (normed, grad_key_pre),
        (normed, grad_value),
        (attended, grad_branch),
        (crossed, grad_cross_query_pre),
        (cross_rows, grad_cross_branch),
        (ffn_normed, grad_pre),
        (activation, grad_ffn_branch),
    )
    return (mixed, grad_hidden, (grad_key_all, grad_value_all), grad_modulated, small, split)


def body(
    hidden,
    text,
    time_emb,
    modulation,
    self_in,
    self_out,
    cross_in,
    cross_out,
    ffn_in,
    ffn_out,
    gains,
    biases,
    ffn_bias,
    positions,
    cotangent,
):
    spot = (lax.axis_index("y"), lax.axis_index("core"))
    width = modulation.shape[1]
    length = ffn_bias.shape[0]
    heads_in = self_in.shape[0]
    attn_in_parts = fetch_split(jnp.concatenate([self_in, cross_in], axis=0), 1, spot)
    attn_out_parts = fetch_split(jnp.stack([self_out, cross_out]), 1, spot)
    ffn_in_parts = fetch_split(ffn_in, 0, spot, quarters=False)
    ffn_out_parts = fetch_split(ffn_out, 0, spot, quarters=False)
    modulation_full, gains_full, biases_full, ffn_bias_full = fetch_small(modulation, gains, biases, ffn_bias)
    in_split = [Split(tuple(part[i] for part in attn_in_parts), spot) for i in range(2 * heads_in)]
    out_split = [Split(tuple(part[i] for part in attn_out_parts), spot) for i in range(2)]
    weights = (
        modulation_full,
        in_split[0],
        in_split[1],
        in_split[2],
        out_split[0],
        in_split[3],
        in_split[4],
        in_split[5],
        out_split[1],
        Split(ffn_in_parts, spot),
        Split(ffn_out_parts, spot),
        gains_full,
        biases_full,
        ffn_bias_full,
    )
    cross_k, cross_v = in_split[4], in_split[5]
    gain_rows = gains_full.astype(jnp.float32)
    bias_rows = biases_full.astype(jnp.float32)
    clips, words, model = text.shape
    text_flat = text.reshape(clips * words, model)
    text_key_pre = cross_k.apply(text_flat) + bias_rows[5]
    text_key_full, pull_text_key = jax.vjp(rms_norm, text_key_pre, gain_rows[3])
    text_value = (cross_v.apply(text_flat) + bias_rows[6]).astype(jnp.bfloat16)
    text_key_low = text_key_full.astype(jnp.bfloat16)
    local_kv = jnp.concatenate(
        [part[i * words : (i + 1) * words] for part in (text_key_low, text_value) for i in range(clips)], axis=1
    )
    all_kv = lax.all_gather(local_kv, SEQ, axis=0, tiled=True)
    key_all = jnp.stack([all_kv[:, i * model : (i + 1) * model] for i in range(clips)])
    value_all = jnp.stack([all_kv[:, (clips + i) * model : (clips + i + 1) * model] for i in range(clips)])
    mixed, grad_hidden, text_grads, grad_time, small_totals, split = micro_step(
        weights, hidden, key_all, value_all, time_emb, positions, cotangent
    )
    key_grads = [text_grads[0][i] for i in range(clips)]
    value_grads = [text_grads[1][i] for i in range(clips)]
    pairs = [(rows.reshape(-1, rows.shape[-1]), grad.reshape(-1, grad.shape[-1])) for rows, grad in split]
    split_grads = [
        split_weight.grad(rows, grad, quarters=index != 6)
        for index, (split_weight, (rows, grad)) in enumerate(
            zip(
                (in_split[0], in_split[1], in_split[2], out_split[0], in_split[3], out_split[1], weights[9], weights[10]),
                pairs,
            )
        )
    ]
    grad_kv = jnp.concatenate(key_grads + value_grads, axis=1).astype(jnp.bfloat16)
    owned_kv = lax.psum_scatter(grad_kv, SEQ, scatter_dimension=0, tiled=True).astype(jnp.float32)
    owned_parts = [owned_kv[:, i * model : (i + 1) * model] for i in range(2 * clips)]
    grad_text_key = jnp.concatenate(owned_parts[:clips], axis=0)
    grad_text_value = jnp.concatenate(owned_parts[clips:], axis=0).astype(jnp.bfloat16)
    grad_text_key_full, gain_cross_key = pull_text_key(grad_text_key)
    grad_text_key_pre = grad_text_key_full.astype(jnp.bfloat16)
    weight_cross_key = cross_k.grad(text_flat, grad_text_key_pre)
    weight_cross_value = cross_v.grad(text_flat, grad_text_value)
    grad_words = cross_k.back(grad_text_key_pre) + cross_v.back(grad_text_value)
    grad_mod, grad_gains, grad_biases, grad_ffn_bias_local = small_totals
    grad_gains = grad_gains.at[3].add(gain_cross_key)
    grad_biases = grad_biases.at[5].add(column_sums(grad_text_key_pre))
    grad_biases = grad_biases.at[6].add(column_sums(grad_text_value))
    attn_in_grads = tuple(
        jnp.stack(
            [split_grads[0][q], split_grads[1][q], split_grads[2][q], split_grads[4][q], weight_cross_key[q], weight_cross_value[q]]
        )
        for q in range(4)
    )
    attn_out_grads = tuple(jnp.stack([split_grads[3][q], split_grads[5][q]]) for q in range(4))
    attn_final = reduce_split(
        tuple(jnp.concatenate([a, b]) for a, b in zip(attn_in_grads, attn_out_grads)), 1, spot
    )
    attn_in_final = attn_final[: 2 * heads_in]
    attn_out_final = attn_final[2 * heads_in :]
    ffn_in_final = reduce_half(split_grads[6], 0, spot)
    ffn_out_final = reduce_split(split_grads[7], 0, spot)
    grad_mod, grad_gains, grad_biases, grad_ffn_bias, grad_time = reduce_small(
        grad_mod, grad_gains, grad_biases, grad_ffn_bias_local, grad_time, width, length
    )
    return (
        mixed,
        grad_hidden,
        grad_words.reshape(clips, words, model),
        grad_time,
        grad_mod,
        attn_in_final[:heads_in],
        attn_out_final[0],
        attn_in_final[heads_in:],
        attn_out_final[1],
        ffn_in_final,
        ffn_out_final,
        grad_gains,
        grad_biases,
        grad_ffn_bias,
    )


def solution(mesh):
    devices = mesh.devices
    split_mesh = Mesh(
        devices.reshape(devices.shape[0] // 2, 2, devices.shape[1]), ("y", "core", "fsdp")
    )
    return jax.shard_map(
        body,
        mesh=split_mesh,
        in_specs=(
            P("fsdp", SEQ, None),
            P("fsdp", SEQ, None),
            P("fsdp", None, None),
            P(None, "fsdp"),
            P(None, "fsdp", None),
            P("fsdp", None),
            P(None, "fsdp", None),
            P("fsdp", None),
            P("fsdp", None),
            P("fsdp", None),
            P(None, "fsdp"),
            P(None, "fsdp"),
            P("fsdp"),
            P("fsdp", None, SEQ),
            P("fsdp", SEQ, None),
        ),
        out_specs=(
            P("fsdp", SEQ, None),
            P("fsdp", SEQ, None),
            P("fsdp", SEQ, None),
            P("fsdp", None, None),
            P(None, "fsdp"),
            P(None, "fsdp", None),
            P("fsdp", None),
            P(None, "fsdp", None),
            P("fsdp", None),
            P("fsdp", None),
            P("fsdp", None),
            P(None, "fsdp"),
            P(None, "fsdp"),
            P("fsdp"),
        ),
        check_vma=False,
    )
```

```python
import jax
import jax.numpy as jnp
from jax import lax
from jax.sharding import Mesh, PartitionSpec as P

HEADS = 12
HEAD = 128


EPSILON = 1e-06
SEQ = ("y", "core")
SWAP = [(0, 1), (1, 0)]


def matmul(operand, factor):
    return jnp.dot(operand, factor, preferred_element_type=jnp.float32)


def inner_rows(operand, factor):
    return lax.dot_general(
        operand, factor, (((0,), (0,)), ((), ())), preferred_element_type=jnp.float32
    )


def outer_cols(operand, factor):
    return lax.dot_general(
        operand, factor, (((operand.ndim - 1,), (1,)), ((), ())), preferred_element_type=jnp.float32
    )


def column_sums(tensor):
    return jnp.sum(tensor.astype(jnp.float32), axis=tuple(range(tensor.ndim - 1)))


def layer_norm(tensor):
    centered = tensor - jnp.mean(tensor, axis=-1, keepdims=True)
    return centered * lax.rsqrt(jnp.mean(centered * centered, axis=-1, keepdims=True) + EPSILON)


def rms_norm(tensor, weight):
    return tensor * lax.rsqrt(jnp.mean(tensor * tensor, axis=-1, keepdims=True) + EPSILON) * weight


def modulate_norm(tensor, shift, scale):
    return layer_norm(tensor) * (1.0 + scale) + shift


def affine_norm(tensor, weight, offset):
    return layer_norm(tensor) * weight + offset


def gelu_tanh(tensor):
    return jax.nn.gelu(tensor, approximate=True)


def rotary_tables(places, head_size, head_count):
    one_sixth = head_size // 6
    span_sizes = (head_size - 4 * one_sixth, 2 * one_sixth, 2 * one_sixth)
    angles = []
    for component in range(3):
        exponents = (
            jnp.arange(0, span_sizes[component], 2, dtype=jnp.float32) / span_sizes[component]
        )
        frequency = 1.0 / 10000.0**exponents
        angles.append(places[component].astype(jnp.float32)[:, None] * frequency[None, :])
    joined = jnp.concatenate(angles, axis=1)
    tiled_angles = jnp.tile(jnp.repeat(joined, 2, axis=1), (1, head_count))
    parity = jnp.where(jnp.arange(tiled_angles.shape[1]) % 2 == 0, -1.0, 1.0)
    return (jnp.cos(tiled_angles), jnp.sin(tiled_angles) * parity)


def rotate(tensor, cosine, signed_sine):
    even_lane = jnp.arange(tensor.shape[-1]) % 2 == 0
    swapped = jnp.where(even_lane, jnp.roll(tensor, -1, axis=-1), jnp.roll(tensor, 1, axis=-1))
    return tensor * cosine + swapped * signed_sine


def split_heads(tensor):
    return tensor.reshape(tensor.shape[0], tensor.shape[1], tensor.shape[2] // HEAD, HEAD)


def attend(queries, key_rows, value_rows):
    scores = jnp.einsum(
        "bqhd,bkhd->bhqk",
        split_heads(queries),
        split_heads(key_rows),
        preferred_element_type=jnp.float32,
    ) * HEAD ** (-0.5)
    row_max = jnp.max(scores, axis=-1, keepdims=True)
    exponentials = jnp.exp(scores - row_max)
    row_total = jnp.sum(exponentials, axis=-1, keepdims=True)
    probabilities = (exponentials / row_total).astype(jnp.bfloat16)
    result = jnp.einsum(
        "bhqk,bkhd->bqhd", probabilities, split_heads(value_rows), preferred_element_type=jnp.float32
    )
    return (result.reshape(queries.shape).astype(jnp.bfloat16), row_max + jnp.log(row_total))


def attend_back(queries, key_rows, value_rows, log_total, grad_rows):
    query_split = split_heads(queries)
    key_split = split_heads(key_rows)
    grad_split = split_heads(grad_rows)
    scale_factor = HEAD ** (-0.5)
    scores = (
        jnp.einsum("bqhd,bkhd->bhqk", query_split, key_split, preferred_element_type=jnp.float32)
        * scale_factor
    )
    probs_full = jnp.exp(scores - log_total)
    probs_low = probs_full.astype(jnp.bfloat16)
    grad_values = jnp.einsum(
        "bhqk,bqhd->bkhd", probs_low, grad_split, preferred_element_type=jnp.float32
    )
    grad_probs = jnp.einsum(
        "bqhd,bkhd->bhqk", grad_split, split_heads(value_rows), preferred_element_type=jnp.float32
    )
    grad_scores = (
        probs_full * (grad_probs - jnp.sum(grad_probs * probs_full, axis=-1, keepdims=True))
    ).astype(jnp.bfloat16)
    grad_queries = (
        jnp.einsum("bhqk,bkhd->bqhd", grad_scores, key_split, preferred_element_type=jnp.float32)
        * scale_factor
    )
    grad_keys = (
        jnp.einsum("bhqk,bqhd->bkhd", grad_scores, query_split, preferred_element_type=jnp.float32)
        * scale_factor
    )
    return (
        grad_queries.reshape(queries.shape),
        grad_keys.reshape(key_rows.shape),
        grad_values.reshape(value_rows.shape),
    )


def swap_core(tensor):
    return lax.ppermute(tensor, "core", SWAP)


def join(mine, other, core):
    width = mine.shape[-1]
    both = jnp.concatenate([other, mine, other], axis=-1)
    return lax.dynamic_slice_in_dim(both, (1 - core) * width, 2 * width, axis=-1)


def halves(tensor, core):
    width = tensor.shape[-1] // 2
    return (
        lax.dynamic_slice_in_dim(tensor, core * width, width, axis=-1),
        lax.dynamic_slice_in_dim(tensor, (1 - core) * width, width, axis=-1),
    )


def swap_y(tensor):
    return lax.ppermute(tensor, "y", SWAP)


class Split:
    def __init__(self, parts, spot):
        self.parts, self.spot = parts, spot

    def apply(self, rows):
        y, core = self.spot
        outs = [matmul(rows, part) for part in self.parts]
        if len(outs) == 2:
            return join(outs[0], outs[1], core)
        return join(join(outs[0], outs[1], y), join(outs[2], outs[3], y), core)

    def quarters(self, grad):
        y, core = self.spot
        grad_mine, grad_other = halves(grad, core)
        return halves(grad_mine, y) + halves(grad_other, y)

    def back(self, grad):
        if len(self.parts) == 2:
            grad_mine, grad_other = halves(grad, self.spot[1])
            return outer_cols(grad_mine, self.parts[0]) + outer_cols(grad_other, self.parts[1])
        pieces = [outer_cols(g, part) for g, part in zip(self.quarters(grad), self.parts)]
        return (pieces[0] + pieces[1]) + (pieces[2] + pieces[3])

    def grad(self, rows, grad, quarters=True):
        pieces = self.quarters(grad) if quarters else halves(grad, self.spot[1])
        return tuple(inner_rows(rows, g) for g in pieces)


def fetch_split(local, gather_axis, spot, quarters=True):
    y, core = spot
    if not quarters:
        width = local.shape[-1] // 2
        part = lax.dynamic_slice_in_dim(local, core * width, width, axis=-1)
        mine = lax.all_gather(part, "fsdp", axis=gather_axis, tiled=True)
        return (mine, swap_core(mine))
    width = local.shape[-1] // 4
    part = lax.dynamic_slice_in_dim(local, (2 * core + y) * width, width, axis=-1)
    own = lax.all_gather(part, "fsdp", axis=gather_axis, tiled=True)
    y_part = swap_y(own)
    return (own, y_part, swap_core(own), swap_core(y_part))


def reduce_split(parts, scatter_axis, spot):
    y, core = spot
    own, y_part, core_part, cross_part = parts
    from_core = swap_core(core_part.astype(jnp.bfloat16)).astype(jnp.float32)
    from_cross = swap_core(cross_part.astype(jnp.bfloat16)).astype(jnp.float32)
    chip_own = own + from_core
    chip_y = (y_part + from_cross).astype(jnp.bfloat16)
    total = (chip_own + swap_y(chip_y).astype(jnp.float32)).astype(jnp.bfloat16)
    owned = lax.psum_scatter(total, "fsdp", scatter_dimension=scatter_axis, tiled=True)
    owned_y = swap_y(owned)
    mine = join(owned, owned_y, y)
    return join(mine, swap_core(mine), core).astype(jnp.float32)


def reduce_half(parts, scatter_axis, spot):
    y, core = spot
    mine, other = parts
    received = swap_core(other.astype(jnp.bfloat16)).astype(jnp.float32)
    chip = (mine + received).astype(jnp.bfloat16)
    owned = lax.psum_scatter(chip, "fsdp", scatter_dimension=scatter_axis, tiled=True)
    summed = owned.astype(jnp.float32) + swap_y(owned).astype(jnp.float32)
    return join(summed, swap_core(summed), core)


def fetch_small(modulation, gains, biases, ffn_bias):
    width = modulation.shape[1]
    length = ffn_bias.shape[0]
    rows = -(-length // width)
    padded = jnp.pad(ffn_bias, (0, rows * width - length)).reshape(rows, width)
    packed = jnp.concatenate([modulation, gains, biases, padded], axis=0)
    full = lax.all_gather(packed, "fsdp", axis=1, tiled=True)
    shards = full.shape[1] // width
    bias_rows = full[21:].reshape(rows, shards, width).transpose(1, 0, 2)
    bias_full = bias_rows.reshape(shards, rows * width)[:, :length].reshape(shards * length)
    return full[:6], full[6:11], full[11:21], bias_full


def reduce_small(grad_mod, grad_gains, grad_biases, grad_ffn_bias, grad_time, width, length):
    rows = -(-length // width)
    shards = grad_mod.shape[1] // width
    bias_rows = jnp.pad(grad_ffn_bias.reshape(shards, length), ((0, 0), (0, rows * width - length)))
    bias_rows = bias_rows.reshape(shards, rows, width).transpose(1, 0, 2).reshape(rows, shards * width)
    packed = jnp.concatenate([grad_mod, grad_gains, grad_biases, bias_rows], axis=0)
    owned = lax.psum_scatter(packed, "fsdp", scatter_dimension=1, tiled=True)
    flat = jnp.concatenate([owned.reshape(-1), grad_time.reshape(-1)])
    summed = lax.psum(flat, SEQ)
    owned = summed[: owned.size].reshape(owned.shape)
    grad_time = summed[owned.size :].reshape(grad_time.shape)
    bias_owned = owned[21:].reshape(-1)[:length]
    return owned[:6], owned[6:11], owned[11:21], bias_owned, grad_time


def micro_step(weights, hidden, key_all, value_all, time_emb, places, cotangent):
    modulation, self_q, self_k, self_v, self_o, cross_q, cross_k, cross_v, cross_o, ffn_in, ffn_out, gains, biases, ffn_bias = (
        weights
    )
    gain_rows = gains.astype(jnp.float32)
    bias_rows = biases.astype(jnp.float32)
    modulated = modulation.astype(jnp.float32)[None] + time_emb.astype(jnp.float32)
    mod = [modulated[:, row, None, :] for row in range(6)]
    cosine, signed_sine = jax.vmap(lambda clip_places: rotary_tables(clip_places, HEAD, HEADS))(places)
    residual_in = hidden.astype(jnp.float32)
    normed_full, pull_first = jax.vjp(modulate_norm, residual_in, mod[0], mod[1])
    normed = normed_full.astype(jnp.bfloat16)
    query_pre = self_q.apply(normed) + bias_rows[0]
    key_pre = self_k.apply(normed) + bias_rows[1]
    value_low = (self_v.apply(normed) + bias_rows[2]).astype(jnp.bfloat16)

    def turn_both(query_input, key_input, gain_query, gain_key):
        return (
            rotate(rms_norm(query_input, gain_query), cosine, signed_sine),
            rotate(rms_norm(key_input, gain_key), cosine, signed_sine),
        )

    turned, pull_turn = jax.vjp(turn_both, query_pre, key_pre, gain_rows[0], gain_rows[1])
    query_heads, key_heads, value_heads = (
        lax.all_to_all(turned[0].astype(jnp.bfloat16), SEQ, split_axis=2, concat_axis=1, tiled=True),
        lax.all_to_all(turned[1].astype(jnp.bfloat16), SEQ, split_axis=2, concat_axis=1, tiled=True),
        lax.all_to_all(value_low, SEQ, split_axis=2, concat_axis=1, tiled=True),
    )
    attn_heads, log_total = attend(query_heads, key_heads, value_heads)
    attended = lax.all_to_all(attn_heads, SEQ, split_axis=1, concat_axis=2, tiled=True)
    branch = self_o.apply(attended) + bias_rows[3]
    after_attn = residual_in + branch * mod[2]
    crossed_full, pull_cross = jax.vjp(affine_norm, after_attn, gain_rows[4], bias_rows[8])
    crossed = crossed_full.astype(jnp.bfloat16)
    cross_query_pre = cross_q.apply(crossed) + bias_rows[4]
    cross_query_full, pull_cross_query = jax.vjp(rms_norm, cross_query_pre, gain_rows[2])
    cross_query = cross_query_full.astype(jnp.bfloat16)
    cross_rows, cross_total = attend(cross_query, key_all, value_all)
    second = after_attn + cross_o.apply(cross_rows) + bias_rows[7]
    ffn_normed_full, pull_second = jax.vjp(modulate_norm, second, mod[3], mod[4])
    ffn_normed = ffn_normed_full.astype(jnp.bfloat16)
    pre_act = ffn_in.apply(ffn_normed) + ffn_bias.astype(jnp.float32)
    activation_full, pull_gelu = jax.vjp(gelu_tanh, pre_act)
    activation = activation_full.astype(jnp.bfloat16)
    ffn_branch = ffn_out.apply(activation) + bias_rows[9]
    mixed = (second + ffn_branch * mod[5]).astype(jnp.bfloat16)
    grad_output = cotangent.astype(jnp.float32)
    gate_ffn = jnp.sum(grad_output * ffn_branch, axis=1)
    grad_ffn_branch = (grad_output * mod[5]).astype(jnp.bfloat16)
    grad_pre_full = pull_gelu(ffn_out.back(grad_ffn_branch))[0]
    grad_pre = grad_pre_full.astype(jnp.bfloat16)
    grad_second_part, shift_ffn, scale_ffn = pull_second(ffn_in.back(grad_pre))
    grad_second = grad_output + grad_second_part
    grad_cross_branch = grad_second.astype(jnp.bfloat16)
    grad_cross_rows = cross_o.back(grad_cross_branch).astype(jnp.bfloat16)
    grad_cross_query, grad_key_all, grad_value_all = attend_back(
        cross_query, key_all, value_all, cross_total, grad_cross_rows
    )
    grad_cross_query_full, gain_cross_query = pull_cross_query(grad_cross_query)
    grad_cross_query_pre = grad_cross_query_full.astype(jnp.bfloat16)
    grad_after_part, gain_norm, bias_norm = pull_cross(cross_q.back(grad_cross_query_pre))
    grad_after = grad_second + grad_after_part
    gate_attn = jnp.sum(grad_after * branch, axis=1)
    grad_branch = (grad_after * mod[2]).astype(jnp.bfloat16)
    grad_attended = self_o.back(grad_branch).astype(jnp.bfloat16)
    grad_attn_heads = lax.all_to_all(grad_attended, SEQ, split_axis=2, concat_axis=1, tiled=True)
    grad_query_heads, grad_key_heads, grad_value_heads = attend_back(
        query_heads, key_heads, value_heads, log_total, grad_attn_heads
    )
    grad_query_turned, grad_key_turned, grad_value = (
        lax.all_to_all(
            grad_query_heads.astype(jnp.bfloat16), SEQ, split_axis=1, concat_axis=2, tiled=True
        ),
        lax.all_to_all(
            grad_key_heads.astype(jnp.bfloat16), SEQ, split_axis=1, concat_axis=2, tiled=True
        ),
        lax.all_to_all(
            grad_value_heads.astype(jnp.bfloat16), SEQ, split_axis=1, concat_axis=2, tiled=True
        ),
    )
    grad_query_full, grad_key_full, gain_query, gain_key = pull_turn(
        (grad_query_turned.astype(jnp.float32), grad_key_turned.astype(jnp.float32))
    )
    grad_query_pre = grad_query_full.astype(jnp.bfloat16)
    grad_key_pre = grad_key_full.astype(jnp.bfloat16)
    grad_normed = self_q.back(grad_query_pre) + self_k.back(grad_key_pre) + self_v.back(grad_value)
    grad_start, shift_attn, scale_attn = pull_first(grad_normed)
    grad_hidden = grad_after + grad_start
    grad_modulated = jnp.stack(
        (shift_attn[:, 0], scale_attn[:, 0], gate_attn, shift_ffn[:, 0], scale_ffn[:, 0], gate_ffn), axis=1
    )
    grad_gains = jnp.stack((gain_query, gain_key, gain_cross_query, jnp.zeros_like(gain_query), gain_norm))
    grad_biases = jnp.stack(
        (
            column_sums(grad_query_pre),
            column_sums(grad_key_pre),
            column_sums(grad_value),
            column_sums(grad_branch),
            column_sums(grad_cross_query_pre),
            jnp.zeros_like(bias_norm),
            jnp.zeros_like(bias_norm),
            column_sums(grad_cross_branch),
            bias_norm,
            column_sums(grad_ffn_branch),
        )
    )
    small = (jnp.sum(grad_modulated, axis=0), grad_gains, grad_biases, column_sums(grad_pre))
    split = (
        (normed, grad_query_pre),
        (normed, grad_key_pre),
        (normed, grad_value),
        (attended, grad_branch),
        (crossed, grad_cross_query_pre),
        (cross_rows, grad_cross_branch),
        (ffn_normed, grad_pre),
        (activation, grad_ffn_branch),
    )
    return (mixed, grad_hidden, (grad_key_all, grad_value_all), grad_modulated, small, split)


def body(
    hidden,
    text,
    time_emb,
    modulation,
    self_in,
    self_out,
    cross_in,
    cross_out,
    ffn_in,
    ffn_out,
    gains,
    biases,
    ffn_bias,
    positions,
    cotangent,
):
    spot = (lax.axis_index("y"), lax.axis_index("core"))
    width = modulation.shape[1]
    length = ffn_bias.shape[0]
    heads_in = self_in.shape[0]
    attn_in_parts = fetch_split(jnp.concatenate([self_in, cross_in], axis=0), 1, spot)
    attn_out_parts = fetch_split(jnp.stack([self_out, cross_out]), 1, spot)
    ffn_in_parts = fetch_split(ffn_in, 0, spot, quarters=False)
    ffn_out_parts = fetch_split(ffn_out, 0, spot, quarters=False)
    modulation_full, gains_full, biases_full, ffn_bias_full = fetch_small(modulation, gains, biases, ffn_bias)
    in_split = [Split(tuple(part[i] for part in attn_in_parts), spot) for i in range(2 * heads_in)]
    out_split = [Split(tuple(part[i] for part in attn_out_parts), spot) for i in range(2)]
    weights = (
        modulation_full,
        in_split[0],
        in_split[1],
        in_split[2],
        out_split[0],
        in_split[3],
        in_split[4],
        in_split[5],
        out_split[1],
        Split(ffn_in_parts, spot),
        Split(ffn_out_parts, spot),
        gains_full,
        biases_full,
        ffn_bias_full,
    )
    cross_k, cross_v = in_split[4], in_split[5]
    gain_rows = gains_full.astype(jnp.float32)
    bias_rows = biases_full.astype(jnp.float32)
    clips, words, model = text.shape
    text_flat = text.reshape(clips * words, model)
    text_key_pre = cross_k.apply(text_flat) + bias_rows[5]
    text_key_full, pull_text_key = jax.vjp(rms_norm, text_key_pre, gain_rows[3])
    text_value = (cross_v.apply(text_flat) + bias_rows[6]).astype(jnp.bfloat16)
    text_key_low = text_key_full.astype(jnp.bfloat16)
    local_kv = jnp.concatenate(
        [part[i * words : (i + 1) * words] for part in (text_key_low, text_value) for i in range(clips)], axis=1
    )
    all_kv = lax.all_gather(local_kv, SEQ, axis=0, tiled=True)
    key_all = jnp.stack([all_kv[:, i * model : (i + 1) * model] for i in range(clips)])
    value_all = jnp.stack([all_kv[:, (clips + i) * model : (clips + i + 1) * model] for i in range(clips)])
    mixed, grad_hidden, text_grads, grad_time, small_totals, split = micro_step(
        weights, hidden, key_all, value_all, time_emb, positions, cotangent
    )
    key_grads = [text_grads[0][i] for i in range(clips)]
    value_grads = [text_grads[1][i] for i in range(clips)]
    pairs = [(rows.reshape(-1, rows.shape[-1]), grad.reshape(-1, grad.shape[-1])) for rows, grad in split]
    split_grads = [
        split_weight.grad(rows, grad, quarters=index == 7)
        for index, (split_weight, (rows, grad)) in enumerate(
            zip(
                (in_split[0], in_split[1], in_split[2], out_split[0], in_split[3], out_split[1], weights[9], weights[10]),
                pairs,
            )
        )
    ]
    grad_kv = jnp.concatenate(key_grads + value_grads, axis=1).astype(jnp.bfloat16)
    owned_kv = lax.psum_scatter(grad_kv, SEQ, scatter_dimension=0, tiled=True).astype(jnp.float32)
    owned_parts = [owned_kv[:, i * model : (i + 1) * model] for i in range(2 * clips)]
    grad_text_key = jnp.concatenate(owned_parts[:clips], axis=0)
    grad_text_value = jnp.concatenate(owned_parts[clips:], axis=0).astype(jnp.bfloat16)
    grad_text_key_full, gain_cross_key = pull_text_key(grad_text_key)
    grad_text_key_pre = grad_text_key_full.astype(jnp.bfloat16)
    weight_cross_key = cross_k.grad(text_flat, grad_text_key_pre, quarters=False)
    weight_cross_value = cross_v.grad(text_flat, grad_text_value, quarters=False)
    grad_words = cross_k.back(grad_text_key_pre) + cross_v.back(grad_text_value)
    grad_mod, grad_gains, grad_biases, grad_ffn_bias_local = small_totals
    grad_gains = grad_gains.at[3].add(gain_cross_key)
    grad_biases = grad_biases.at[5].add(column_sums(grad_text_key_pre))
    grad_biases = grad_biases.at[6].add(column_sums(grad_text_value))
    attn_grads = tuple(
        jnp.stack(
            [
                split_grads[0][h],
                split_grads[1][h],
                split_grads[2][h],
                split_grads[4][h],
                weight_cross_key[h],
                weight_cross_value[h],
                split_grads[3][h],
                split_grads[5][h],
            ]
        )
        for h in range(2)
    )
    attn_final = reduce_half(attn_grads, 1, spot)
    attn_in_final = attn_final[: 2 * heads_in]
    attn_out_final = attn_final[2 * heads_in :]
    ffn_in_final = reduce_half(split_grads[6], 0, spot)
    ffn_out_final = reduce_split(split_grads[7], 0, spot)
    grad_mod, grad_gains, grad_biases, grad_ffn_bias, grad_time = reduce_small(
        grad_mod, grad_gains, grad_biases, grad_ffn_bias_local, grad_time, width, length
    )
    return (
        mixed,
        grad_hidden,
        grad_words.reshape(clips, words, model),
        grad_time,
        grad_mod,
        attn_in_final[:heads_in],
        attn_out_final[0],
        attn_in_final[heads_in:],
        attn_out_final[1],
        ffn_in_final,
        ffn_out_final,
        grad_gains,
        grad_biases,
        grad_ffn_bias,
    )


def solution(mesh):
    devices = mesh.devices
    split_mesh = Mesh(
        devices.reshape(devices.shape[0] // 2, 2, devices.shape[1]), ("y", "core", "fsdp")
    )
    return jax.shard_map(
        body,
        mesh=split_mesh,
        in_specs=(
            P("fsdp", SEQ, None),
            P("fsdp", SEQ, None),
            P("fsdp", None, None),
            P(None, "fsdp"),
            P(None, "fsdp", None),
            P("fsdp", None),
            P(None, "fsdp", None),
            P("fsdp", None),
            P("fsdp", None),
            P("fsdp", None),
            P(None, "fsdp"),
            P(None, "fsdp"),
            P("fsdp"),
            P("fsdp", None, SEQ),
            P("fsdp", SEQ, None),
        ),
        out_specs=(
            P("fsdp", SEQ, None),
            P("fsdp", SEQ, None),
            P("fsdp", SEQ, None),
            P("fsdp", None, None),
            P(None, "fsdp"),
            P(None, "fsdp", None),
            P("fsdp", None),
            P(None, "fsdp", None),
            P("fsdp", None),
            P("fsdp", None),
            P("fsdp", None),
            P(None, "fsdp"),
            P(None, "fsdp"),
            P("fsdp"),
        ),
        check_vma=False,
    )
```

```python
import jax
import jax.numpy as jnp
from jax import lax
from jax.sharding import Mesh, PartitionSpec as P

HEADS = 12
HEAD = 128


EPSILON = 1e-06
SEQ = ("y", "core")
SWAP = [(0, 1), (1, 0)]


def matmul(operand, factor):
    return jnp.dot(operand, factor, preferred_element_type=jnp.float32)


def inner_rows(operand, factor):
    return lax.dot_general(
        operand, factor, (((0,), (0,)), ((), ())), preferred_element_type=jnp.float32
    )


def outer_cols(operand, factor):
    return lax.dot_general(
        operand, factor, (((operand.ndim - 1,), (1,)), ((), ())), preferred_element_type=jnp.float32
    )


def column_sums(tensor):
    return jnp.sum(tensor.astype(jnp.float32), axis=tuple(range(tensor.ndim - 1)))


def layer_norm(tensor):
    centered = tensor - jnp.mean(tensor, axis=-1, keepdims=True)
    return centered * lax.rsqrt(jnp.mean(centered * centered, axis=-1, keepdims=True) + EPSILON)


def rms_norm(tensor, weight):
    return tensor * lax.rsqrt(jnp.mean(tensor * tensor, axis=-1, keepdims=True) + EPSILON) * weight


def modulate_norm(tensor, shift, scale):
    return layer_norm(tensor) * (1.0 + scale) + shift


def affine_norm(tensor, weight, offset):
    return layer_norm(tensor) * weight + offset


def gelu_tanh(tensor):
    return jax.nn.gelu(tensor, approximate=True)


def rotary_tables(places, head_size, head_count):
    one_sixth = head_size // 6
    span_sizes = (head_size - 4 * one_sixth, 2 * one_sixth, 2 * one_sixth)
    angles = []
    for component in range(3):
        exponents = (
            jnp.arange(0, span_sizes[component], 2, dtype=jnp.float32) / span_sizes[component]
        )
        frequency = 1.0 / 10000.0**exponents
        angles.append(places[component].astype(jnp.float32)[:, None] * frequency[None, :])
    joined = jnp.concatenate(angles, axis=1)
    tiled_angles = jnp.tile(jnp.repeat(joined, 2, axis=1), (1, head_count))
    parity = jnp.where(jnp.arange(tiled_angles.shape[1]) % 2 == 0, -1.0, 1.0)
    return (jnp.cos(tiled_angles), jnp.sin(tiled_angles) * parity)


def rotate(tensor, cosine, signed_sine):
    even_lane = jnp.arange(tensor.shape[-1]) % 2 == 0
    swapped = jnp.where(even_lane, jnp.roll(tensor, -1, axis=-1), jnp.roll(tensor, 1, axis=-1))
    return tensor * cosine + swapped * signed_sine


def split_heads(tensor):
    return tensor.reshape(tensor.shape[0], tensor.shape[1], tensor.shape[2] // HEAD, HEAD)


def attend(queries, key_rows, value_rows):
    scores = jnp.einsum(
        "bqhd,bkhd->bhqk",
        split_heads(queries),
        split_heads(key_rows),
        preferred_element_type=jnp.float32,
    ) * HEAD ** (-0.5)
    row_max = jnp.max(scores, axis=-1, keepdims=True)
    exponentials = jnp.exp(scores - row_max)
    row_total = jnp.sum(exponentials, axis=-1, keepdims=True)
    probabilities = (exponentials / row_total).astype(jnp.bfloat16)
    result = jnp.einsum(
        "bhqk,bkhd->bqhd", probabilities, split_heads(value_rows), preferred_element_type=jnp.float32
    )
    return (result.reshape(queries.shape).astype(jnp.bfloat16), row_max + jnp.log(row_total))


def attend_back(queries, key_rows, value_rows, log_total, grad_rows):
    query_split = split_heads(queries)
    key_split = split_heads(key_rows)
    grad_split = split_heads(grad_rows)
    scale_factor = HEAD ** (-0.5)
    scores = (
        jnp.einsum("bqhd,bkhd->bhqk", query_split, key_split, preferred_element_type=jnp.float32)
        * scale_factor
    )
    probs_full = jnp.exp(scores - log_total)
    probs_low = probs_full.astype(jnp.bfloat16)
    grad_values = jnp.einsum(
        "bhqk,bqhd->bkhd", probs_low, grad_split, preferred_element_type=jnp.float32
    )
    grad_probs = jnp.einsum(
        "bqhd,bkhd->bhqk", grad_split, split_heads(value_rows), preferred_element_type=jnp.float32
    )
    grad_scores = (
        probs_full * (grad_probs - jnp.sum(grad_probs * probs_full, axis=-1, keepdims=True))
    ).astype(jnp.bfloat16)
    grad_queries = (
        jnp.einsum("bhqk,bkhd->bqhd", grad_scores, key_split, preferred_element_type=jnp.float32)
        * scale_factor
    )
    grad_keys = (
        jnp.einsum("bhqk,bqhd->bkhd", grad_scores, query_split, preferred_element_type=jnp.float32)
        * scale_factor
    )
    return (
        grad_queries.reshape(queries.shape),
        grad_keys.reshape(key_rows.shape),
        grad_values.reshape(value_rows.shape),
    )


def swap_core(tensor):
    return lax.ppermute(tensor, "core", SWAP)


def join(mine, other, core):
    width = mine.shape[-1]
    both = jnp.concatenate([other, mine, other], axis=-1)
    return lax.dynamic_slice_in_dim(both, (1 - core) * width, 2 * width, axis=-1)


def halves(tensor, core):
    width = tensor.shape[-1] // 2
    return (
        lax.dynamic_slice_in_dim(tensor, core * width, width, axis=-1),
        lax.dynamic_slice_in_dim(tensor, (1 - core) * width, width, axis=-1),
    )


def swap_y(tensor):
    return lax.ppermute(tensor, "y", SWAP)


class Split:
    def __init__(self, parts, spot):
        self.parts, self.spot = parts, spot

    def apply(self, rows):
        y, core = self.spot
        outs = [matmul(rows, part) for part in self.parts]
        if len(outs) == 2:
            return join(outs[0], outs[1], core)
        return join(join(outs[0], outs[1], y), join(outs[2], outs[3], y), core)

    def quarters(self, grad):
        y, core = self.spot
        grad_mine, grad_other = halves(grad, core)
        return halves(grad_mine, y) + halves(grad_other, y)

    def back(self, grad):
        if len(self.parts) == 2:
            grad_mine, grad_other = halves(grad, self.spot[1])
            return outer_cols(grad_mine, self.parts[0]) + outer_cols(grad_other, self.parts[1])
        pieces = [outer_cols(g, part) for g, part in zip(self.quarters(grad), self.parts)]
        return (pieces[0] + pieces[1]) + (pieces[2] + pieces[3])

    def grad(self, rows, grad, quarters=True):
        pieces = self.quarters(grad) if quarters else halves(grad, self.spot[1])
        return tuple(inner_rows(rows, g) for g in pieces)


def fetch_split(local, gather_axis, spot, quarters=True):
    y, core = spot
    if not quarters:
        width = local.shape[-1] // 2
        part = lax.dynamic_slice_in_dim(local, core * width, width, axis=-1)
        mine = lax.all_gather(part, "fsdp", axis=gather_axis, tiled=True)
        return (mine, swap_core(mine))
    width = local.shape[-1] // 4
    part = lax.dynamic_slice_in_dim(local, (2 * core + y) * width, width, axis=-1)
    own = lax.all_gather(part, "fsdp", axis=gather_axis, tiled=True)
    y_part = swap_y(own)
    return (own, y_part, swap_core(own), swap_core(y_part))


def reduce_split(parts, scatter_axis, spot, after=None):
    y, core = spot
    own, y_part, core_part, cross_part = parts
    from_core = swap_core(core_part.astype(jnp.bfloat16)).astype(jnp.float32)
    from_cross = swap_core(cross_part.astype(jnp.bfloat16)).astype(jnp.float32)
    chip_own = own + from_core
    chip_y = (y_part + from_cross).astype(jnp.bfloat16)
    from_y = swap_y(chip_y)
    if after is not None:
        from_y, _ = lax.optimization_barrier((from_y, after))
    total = (chip_own + from_y.astype(jnp.float32)).astype(jnp.bfloat16)
    owned = lax.psum_scatter(total, "fsdp", scatter_dimension=scatter_axis, tiled=True)
    owned_y = swap_y(owned)
    mine = join(owned, owned_y, y)
    return join(mine, swap_core(mine), core).astype(jnp.float32)


def reduce_half(parts, scatter_axis, spot):
    y, core = spot
    mine, other = parts
    received = swap_core(other.astype(jnp.bfloat16)).astype(jnp.float32)
    chip = (mine + received).astype(jnp.bfloat16)
    owned = lax.psum_scatter(chip, "fsdp", scatter_dimension=scatter_axis, tiled=True)
    summed = owned.astype(jnp.float32) + swap_y(owned).astype(jnp.float32)
    return join(summed, swap_core(summed), core)


def fetch_small(modulation, gains, biases, ffn_bias):
    width = modulation.shape[1]
    length = ffn_bias.shape[0]
    rows = -(-length // width)
    padded = jnp.pad(ffn_bias, (0, rows * width - length)).reshape(rows, width)
    packed = jnp.concatenate([modulation, gains, biases, padded], axis=0)
    full = lax.all_gather(packed, "fsdp", axis=1, tiled=True)
    shards = full.shape[1] // width
    bias_rows = full[21:].reshape(rows, shards, width).transpose(1, 0, 2)
    bias_full = bias_rows.reshape(shards, rows * width)[:, :length].reshape(shards * length)
    return full[:6], full[6:11], full[11:21], bias_full


def reduce_small(grad_mod, grad_gains, grad_biases, grad_ffn_bias, grad_time, width, length):
    rows = -(-length // width)
    shards = grad_mod.shape[1] // width
    bias_rows = jnp.pad(grad_ffn_bias.reshape(shards, length), ((0, 0), (0, rows * width - length)))
    bias_rows = bias_rows.reshape(shards, rows, width).transpose(1, 0, 2).reshape(rows, shards * width)
    packed = jnp.concatenate([grad_mod, grad_gains, grad_biases, bias_rows], axis=0)
    owned = lax.psum_scatter(packed, "fsdp", scatter_dimension=1, tiled=True)
    flat = jnp.concatenate([owned.reshape(-1), grad_time.reshape(-1)])
    summed = lax.psum(flat, SEQ)
    owned = summed[: owned.size].reshape(owned.shape)
    grad_time = summed[owned.size :].reshape(grad_time.shape)
    bias_owned = owned[21:].reshape(-1)[:length]
    return owned[:6], owned[6:11], owned[11:21], bias_owned, grad_time


def micro_step(weights, hidden, key_all, value_all, time_emb, places, cotangent):
    modulation, self_q, self_k, self_v, self_o, cross_q, cross_k, cross_v, cross_o, ffn_in, ffn_out, gains, biases, ffn_bias = (
        weights
    )
    gain_rows = gains.astype(jnp.float32)
    bias_rows = biases.astype(jnp.float32)
    modulated = modulation.astype(jnp.float32)[None] + time_emb.astype(jnp.float32)
    mod = [modulated[:, row, None, :] for row in range(6)]
    cosine, signed_sine = jax.vmap(lambda clip_places: rotary_tables(clip_places, HEAD, HEADS))(places)
    residual_in = hidden.astype(jnp.float32)
    normed_full, pull_first = jax.vjp(modulate_norm, residual_in, mod[0], mod[1])
    normed = normed_full.astype(jnp.bfloat16)
    query_pre = self_q.apply(normed) + bias_rows[0]
    key_pre = self_k.apply(normed) + bias_rows[1]
    value_low = (self_v.apply(normed) + bias_rows[2]).astype(jnp.bfloat16)

    def turn_both(query_input, key_input, gain_query, gain_key):
        return (
            rotate(rms_norm(query_input, gain_query), cosine, signed_sine),
            rotate(rms_norm(key_input, gain_key), cosine, signed_sine),
        )

    turned, pull_turn = jax.vjp(turn_both, query_pre, key_pre, gain_rows[0], gain_rows[1])
    query_heads, key_heads, value_heads = (
        lax.all_to_all(turned[0].astype(jnp.bfloat16), SEQ, split_axis=2, concat_axis=1, tiled=True),
        lax.all_to_all(turned[1].astype(jnp.bfloat16), SEQ, split_axis=2, concat_axis=1, tiled=True),
        lax.all_to_all(value_low, SEQ, split_axis=2, concat_axis=1, tiled=True),
    )
    attn_heads, log_total = attend(query_heads, key_heads, value_heads)
    attended = lax.all_to_all(attn_heads, SEQ, split_axis=1, concat_axis=2, tiled=True)
    branch = self_o.apply(attended) + bias_rows[3]
    after_attn = residual_in + branch * mod[2]
    crossed_full, pull_cross = jax.vjp(affine_norm, after_attn, gain_rows[4], bias_rows[8])
    crossed = crossed_full.astype(jnp.bfloat16)
    cross_query_pre = cross_q.apply(crossed) + bias_rows[4]
    cross_query_full, pull_cross_query = jax.vjp(rms_norm, cross_query_pre, gain_rows[2])
    cross_query = cross_query_full.astype(jnp.bfloat16)
    cross_rows, cross_total = attend(cross_query, key_all, value_all)
    second = after_attn + cross_o.apply(cross_rows) + bias_rows[7]
    ffn_normed_full, pull_second = jax.vjp(modulate_norm, second, mod[3], mod[4])
    ffn_normed = ffn_normed_full.astype(jnp.bfloat16)
    pre_act = ffn_in.apply(ffn_normed) + ffn_bias.astype(jnp.float32)
    activation_full, pull_gelu = jax.vjp(gelu_tanh, pre_act)
    activation = activation_full.astype(jnp.bfloat16)
    ffn_branch = ffn_out.apply(activation) + bias_rows[9]
    mixed = (second + ffn_branch * mod[5]).astype(jnp.bfloat16)
    grad_output = cotangent.astype(jnp.float32)
    gate_ffn = jnp.sum(grad_output * ffn_branch, axis=1)
    grad_ffn_branch = (grad_output * mod[5]).astype(jnp.bfloat16)
    grad_pre_full = pull_gelu(ffn_out.back(grad_ffn_branch))[0]
    grad_pre = grad_pre_full.astype(jnp.bfloat16)
    grad_second_part, shift_ffn, scale_ffn = pull_second(ffn_in.back(grad_pre))
    grad_second = grad_output + grad_second_part
    grad_cross_branch = grad_second.astype(jnp.bfloat16)
    grad_cross_rows = cross_o.back(grad_cross_branch).astype(jnp.bfloat16)
    grad_cross_query, grad_key_all, grad_value_all = attend_back(
        cross_query, key_all, value_all, cross_total, grad_cross_rows
    )
    grad_cross_query_full, gain_cross_query = pull_cross_query(grad_cross_query)
    grad_cross_query_pre = grad_cross_query_full.astype(jnp.bfloat16)
    grad_after_part, gain_norm, bias_norm = pull_cross(cross_q.back(grad_cross_query_pre))
    grad_after = grad_second + grad_after_part
    gate_attn = jnp.sum(grad_after * branch, axis=1)
    grad_branch = (grad_after * mod[2]).astype(jnp.bfloat16)
    grad_attended = self_o.back(grad_branch).astype(jnp.bfloat16)
    grad_attn_heads = lax.all_to_all(grad_attended, SEQ, split_axis=2, concat_axis=1, tiled=True)
    grad_query_heads, grad_key_heads, grad_value_heads = attend_back(
        query_heads, key_heads, value_heads, log_total, grad_attn_heads
    )
    grad_query_turned, grad_key_turned, grad_value = (
        lax.all_to_all(
            grad_query_heads.astype(jnp.bfloat16), SEQ, split_axis=1, concat_axis=2, tiled=True
        ),
        lax.all_to_all(
            grad_key_heads.astype(jnp.bfloat16), SEQ, split_axis=1, concat_axis=2, tiled=True
        ),
        lax.all_to_all(
            grad_value_heads.astype(jnp.bfloat16), SEQ, split_axis=1, concat_axis=2, tiled=True
        ),
    )
    grad_query_full, grad_key_full, gain_query, gain_key = pull_turn(
        (grad_query_turned.astype(jnp.float32), grad_key_turned.astype(jnp.float32))
    )
    grad_query_pre = grad_query_full.astype(jnp.bfloat16)
    grad_key_pre = grad_key_full.astype(jnp.bfloat16)
    grad_normed = self_q.back(grad_query_pre) + self_k.back(grad_key_pre) + self_v.back(grad_value)
    grad_start, shift_attn, scale_attn = pull_first(grad_normed)
    grad_hidden = grad_after + grad_start
    grad_modulated = jnp.stack(
        (shift_attn[:, 0], scale_attn[:, 0], gate_attn, shift_ffn[:, 0], scale_ffn[:, 0], gate_ffn), axis=1
    )
    grad_gains = jnp.stack((gain_query, gain_key, gain_cross_query, jnp.zeros_like(gain_query), gain_norm))
    grad_biases = jnp.stack(
        (
            column_sums(grad_query_pre),
            column_sums(grad_key_pre),
            column_sums(grad_value),
            column_sums(grad_branch),
            column_sums(grad_cross_query_pre),
            jnp.zeros_like(bias_norm),
            jnp.zeros_like(bias_norm),
            column_sums(grad_cross_branch),
            bias_norm,
            column_sums(grad_ffn_branch),
        )
    )
    small = (jnp.sum(grad_modulated, axis=0), grad_gains, grad_biases, column_sums(grad_pre))
    split = (
        (normed, grad_query_pre),
        (normed, grad_key_pre),
        (normed, grad_value),
        (attended, grad_branch),
        (crossed, grad_cross_query_pre),
        (cross_rows, grad_cross_branch),
        (ffn_normed, grad_pre),
        (activation, grad_ffn_branch),
    )
    return (mixed, grad_hidden, (grad_key_all, grad_value_all), grad_modulated, small, split)


def body(
    hidden,
    text,
    time_emb,
    modulation,
    self_in,
    self_out,
    cross_in,
    cross_out,
    ffn_in,
    ffn_out,
    gains,
    biases,
    ffn_bias,
    positions,
    cotangent,
):
    spot = (lax.axis_index("y"), lax.axis_index("core"))
    width = modulation.shape[1]
    length = ffn_bias.shape[0]
    heads_in = self_in.shape[0]
    attn_in_parts = fetch_split(jnp.concatenate([self_in, cross_in], axis=0), 1, spot)
    attn_out_parts = fetch_split(jnp.stack([self_out, cross_out]), 1, spot)
    ffn_in_parts = fetch_split(ffn_in, 0, spot, quarters=False)
    ffn_out_parts = fetch_split(ffn_out, 0, spot, quarters=False)
    modulation_full, gains_full, biases_full, ffn_bias_full = fetch_small(modulation, gains, biases, ffn_bias)
    in_split = [Split(tuple(part[i] for part in attn_in_parts), spot) for i in range(2 * heads_in)]
    out_split = [Split(tuple(part[i] for part in attn_out_parts), spot) for i in range(2)]
    weights = (
        modulation_full,
        in_split[0],
        in_split[1],
        in_split[2],
        out_split[0],
        in_split[3],
        in_split[4],
        in_split[5],
        out_split[1],
        Split(ffn_in_parts, spot),
        Split(ffn_out_parts, spot),
        gains_full,
        biases_full,
        ffn_bias_full,
    )
    cross_k, cross_v = in_split[4], in_split[5]
    gain_rows = gains_full.astype(jnp.float32)
    bias_rows = biases_full.astype(jnp.float32)
    clips, words, model = text.shape
    text_flat = text.reshape(clips * words, model)
    text_key_pre = cross_k.apply(text_flat) + bias_rows[5]
    text_key_full, pull_text_key = jax.vjp(rms_norm, text_key_pre, gain_rows[3])
    text_value = (cross_v.apply(text_flat) + bias_rows[6]).astype(jnp.bfloat16)
    text_key_low = text_key_full.astype(jnp.bfloat16)
    local_kv = jnp.concatenate(
        [part[i * words : (i + 1) * words] for part in (text_key_low, text_value) for i in range(clips)], axis=1
    )
    all_kv = lax.all_gather(local_kv, SEQ, axis=0, tiled=True)
    key_all = jnp.stack([all_kv[:, i * model : (i + 1) * model] for i in range(clips)])
    value_all = jnp.stack([all_kv[:, (clips + i) * model : (clips + i + 1) * model] for i in range(clips)])
    mixed, grad_hidden, text_grads, grad_time, small_totals, split = micro_step(
        weights, hidden, key_all, value_all, time_emb, positions, cotangent
    )
    key_grads = [text_grads[0][i] for i in range(clips)]
    value_grads = [text_grads[1][i] for i in range(clips)]
    pairs = [(rows.reshape(-1, rows.shape[-1]), grad.reshape(-1, grad.shape[-1])) for rows, grad in split]
    split_grads = [
        split_weight.grad(rows, grad, quarters=index != 6)
        for index, (split_weight, (rows, grad)) in enumerate(
            zip(
                (in_split[0], in_split[1], in_split[2], out_split[0], in_split[3], out_split[1], weights[9], weights[10]),
                pairs,
            )
        )
    ]
    grad_kv = jnp.concatenate(key_grads + value_grads, axis=1).astype(jnp.bfloat16)
    owned_kv = lax.psum_scatter(grad_kv, SEQ, scatter_dimension=0, tiled=True).astype(jnp.float32)
    owned_parts = [owned_kv[:, i * model : (i + 1) * model] for i in range(2 * clips)]
    grad_text_key = jnp.concatenate(owned_parts[:clips], axis=0)
    grad_text_value = jnp.concatenate(owned_parts[clips:], axis=0).astype(jnp.bfloat16)
    grad_text_key_full, gain_cross_key = pull_text_key(grad_text_key)
    grad_text_key_pre = grad_text_key_full.astype(jnp.bfloat16)
    weight_cross_key = cross_k.grad(text_flat, grad_text_key_pre)
    weight_cross_value = cross_v.grad(text_flat, grad_text_value)
    grad_words = cross_k.back(grad_text_key_pre) + cross_v.back(grad_text_value)
    grad_mod, grad_gains, grad_biases, grad_ffn_bias_local = small_totals
    grad_gains = grad_gains.at[3].add(gain_cross_key)
    grad_biases = grad_biases.at[5].add(column_sums(grad_text_key_pre))
    grad_biases = grad_biases.at[6].add(column_sums(grad_text_value))
    attn_in_grads = tuple(
        jnp.stack(
            [split_grads[0][q], split_grads[1][q], split_grads[2][q], split_grads[4][q], weight_cross_key[q], weight_cross_value[q]]
        )
        for q in range(4)
    )
    attn_out_grads = tuple(jnp.stack([split_grads[3][q], split_grads[5][q]]) for q in range(4))
    attn_parts = tuple(jnp.concatenate([a, b]) for a, b in zip(attn_in_grads, attn_out_grads))
    grad_mod, grad_gains, grad_biases, grad_ffn_bias, grad_time = reduce_small(
        grad_mod, grad_gains, grad_biases, grad_ffn_bias_local, grad_time, width, length
    )
    attn_final = reduce_split(attn_parts, 1, spot, after=grad_gains)
    attn_in_final = attn_final[: 2 * heads_in]
    attn_out_final = attn_final[2 * heads_in :]
    ffn_in_final = reduce_half(split_grads[6], 0, spot)
    ffn_out_final = reduce_split(split_grads[7], 0, spot, after=attn_parts[0])
    return (
        mixed,
        grad_hidden,
        grad_words.reshape(clips, words, model),
        grad_time,
        grad_mod,
        attn_in_final[:heads_in],
        attn_out_final[0],
        attn_in_final[heads_in:],
        attn_out_final[1],
        ffn_in_final,
        ffn_out_final,
        grad_gains,
        grad_biases,
        grad_ffn_bias,
    )


def solution(mesh):
    devices = mesh.devices
    split_mesh = Mesh(
        devices.reshape(devices.shape[0] // 2, 2, devices.shape[1]), ("y", "core", "fsdp")
    )
    return jax.shard_map(
        body,
        mesh=split_mesh,
        in_specs=(
            P("fsdp", SEQ, None),
            P("fsdp", SEQ, None),
            P("fsdp", None, None),
            P(None, "fsdp"),
            P(None, "fsdp", None),
            P("fsdp", None),
            P(None, "fsdp", None),
            P("fsdp", None),
            P("fsdp", None),
            P("fsdp", None),
            P(None, "fsdp"),
            P(None, "fsdp"),
            P("fsdp"),
            P("fsdp", None, SEQ),
            P("fsdp", SEQ, None),
        ),
        out_specs=(
            P("fsdp", SEQ, None),
            P("fsdp", SEQ, None),
            P("fsdp", SEQ, None),
            P("fsdp", None, None),
            P(None, "fsdp"),
            P(None, "fsdp", None),
            P("fsdp", None),
            P(None, "fsdp", None),
            P("fsdp", None),
            P("fsdp", None),
            P("fsdp", None),
            P(None, "fsdp"),
            P(None, "fsdp"),
            P("fsdp"),
        ),
        check_vma=False,
    )
```

```python
import jax
import jax.numpy as jnp
from jax import lax
from jax.sharding import Mesh, PartitionSpec as P

HEADS = 12
HEAD = 128


EPSILON = 1e-06
SEQ = ("y", "core")
SWAP = [(0, 1), (1, 0)]


def matmul(operand, factor):
    return jnp.dot(operand, factor, preferred_element_type=jnp.float32)


def inner_rows(operand, factor):
    return lax.dot_general(
        operand, factor, (((0,), (0,)), ((), ())), preferred_element_type=jnp.float32
    )


def outer_cols(operand, factor):
    return lax.dot_general(
        operand, factor, (((operand.ndim - 1,), (1,)), ((), ())), preferred_element_type=jnp.float32
    )


def column_sums(tensor):
    return jnp.sum(tensor.astype(jnp.float32), axis=tuple(range(tensor.ndim - 1)))


def layer_norm(tensor):
    centered = tensor - jnp.mean(tensor, axis=-1, keepdims=True)
    return centered * lax.rsqrt(jnp.mean(centered * centered, axis=-1, keepdims=True) + EPSILON)


def rms_norm(tensor, weight):
    return tensor * lax.rsqrt(jnp.mean(tensor * tensor, axis=-1, keepdims=True) + EPSILON) * weight


def modulate_norm(tensor, shift, scale):
    return layer_norm(tensor) * (1.0 + scale) + shift


def affine_norm(tensor, weight, offset):
    return layer_norm(tensor) * weight + offset


def gelu_tanh(tensor):
    return jax.nn.gelu(tensor, approximate=True)


def rotary_tables(places, head_size, head_count):
    one_sixth = head_size // 6
    span_sizes = (head_size - 4 * one_sixth, 2 * one_sixth, 2 * one_sixth)
    angles = []
    for component in range(3):
        exponents = (
            jnp.arange(0, span_sizes[component], 2, dtype=jnp.float32) / span_sizes[component]
        )
        frequency = 1.0 / 10000.0**exponents
        angles.append(places[component].astype(jnp.float32)[:, None] * frequency[None, :])
    joined = jnp.concatenate(angles, axis=1)
    tiled_angles = jnp.tile(jnp.repeat(joined, 2, axis=1), (1, head_count))
    parity = jnp.where(jnp.arange(tiled_angles.shape[1]) % 2 == 0, -1.0, 1.0)
    return (jnp.cos(tiled_angles), jnp.sin(tiled_angles) * parity)


def rotate(tensor, cosine, signed_sine):
    even_lane = jnp.arange(tensor.shape[-1]) % 2 == 0
    swapped = jnp.where(even_lane, jnp.roll(tensor, -1, axis=-1), jnp.roll(tensor, 1, axis=-1))
    return tensor * cosine + swapped * signed_sine


def split_heads(tensor):
    return tensor.reshape(tensor.shape[0], tensor.shape[1], tensor.shape[2] // HEAD, HEAD)


def attend(queries, key_rows, value_rows):
    scores = jnp.einsum(
        "bqhd,bkhd->bhqk",
        split_heads(queries),
        split_heads(key_rows),
        preferred_element_type=jnp.float32,
    ) * HEAD ** (-0.5)
    row_max = jnp.max(scores, axis=-1, keepdims=True)
    exponentials = jnp.exp(scores - row_max)
    row_total = jnp.sum(exponentials, axis=-1, keepdims=True)
    probabilities = (exponentials / row_total).astype(jnp.bfloat16)
    result = jnp.einsum(
        "bhqk,bkhd->bqhd", probabilities, split_heads(value_rows), preferred_element_type=jnp.float32
    )
    return (result.reshape(queries.shape).astype(jnp.bfloat16), row_max + jnp.log(row_total))


def attend_back(queries, key_rows, value_rows, log_total, grad_rows):
    query_split = split_heads(queries)
    key_split = split_heads(key_rows)
    grad_split = split_heads(grad_rows)
    scale_factor = HEAD ** (-0.5)
    scores = (
        jnp.einsum("bqhd,bkhd->bhqk", query_split, key_split, preferred_element_type=jnp.float32)
        * scale_factor
    )
    probs_full = jnp.exp(scores - log_total)
    probs_low = probs_full.astype(jnp.bfloat16)
    grad_values = jnp.einsum(
        "bhqk,bqhd->bkhd", probs_low, grad_split, preferred_element_type=jnp.float32
    )
    grad_probs = jnp.einsum(
        "bqhd,bkhd->bhqk", grad_split, split_heads(value_rows), preferred_element_type=jnp.float32
    )
    grad_scores = (
        probs_full * (grad_probs - jnp.sum(grad_probs * probs_full, axis=-1, keepdims=True))
    ).astype(jnp.bfloat16)
    grad_queries = (
        jnp.einsum("bhqk,bkhd->bqhd", grad_scores, key_split, preferred_element_type=jnp.float32)
        * scale_factor
    )
    grad_keys = (
        jnp.einsum("bhqk,bqhd->bkhd", grad_scores, query_split, preferred_element_type=jnp.float32)
        * scale_factor
    )
    return (
        grad_queries.reshape(queries.shape),
        grad_keys.reshape(key_rows.shape),
        grad_values.reshape(value_rows.shape),
    )


def swap_core(tensor):
    return lax.ppermute(tensor, "core", SWAP)


def join(mine, other, core):
    width = mine.shape[-1]
    both = jnp.concatenate([other, mine, other], axis=-1)
    return lax.dynamic_slice_in_dim(both, (1 - core) * width, 2 * width, axis=-1)


def halves(tensor, core):
    width = tensor.shape[-1] // 2
    return (
        lax.dynamic_slice_in_dim(tensor, core * width, width, axis=-1),
        lax.dynamic_slice_in_dim(tensor, (1 - core) * width, width, axis=-1),
    )


def swap_y(tensor):
    return lax.ppermute(tensor, "y", SWAP)


class Split:
    def __init__(self, parts, spot):
        self.parts, self.spot = parts, spot

    def apply(self, rows):
        y, core = self.spot
        outs = [matmul(rows, part) for part in self.parts]
        if len(outs) == 2:
            return join(outs[0], outs[1], core)
        return join(join(outs[0], outs[1], y), join(outs[2], outs[3], y), core)

    def quarters(self, grad):
        y, core = self.spot
        grad_mine, grad_other = halves(grad, core)
        return halves(grad_mine, y) + halves(grad_other, y)

    def back(self, grad):
        if len(self.parts) == 2:
            grad_mine, grad_other = halves(grad, self.spot[1])
            return outer_cols(grad_mine, self.parts[0]) + outer_cols(grad_other, self.parts[1])
        pieces = [outer_cols(g, part) for g, part in zip(self.quarters(grad), self.parts)]
        return (pieces[0] + pieces[1]) + (pieces[2] + pieces[3])

    def grad(self, rows, grad, quarters=True):
        pieces = self.quarters(grad) if quarters else halves(grad, self.spot[1])
        return tuple(inner_rows(rows, g) for g in pieces)


def fetch_split(local, gather_axis, spot, quarters=True):
    y, core = spot
    if not quarters:
        width = local.shape[-1] // 2
        part = lax.dynamic_slice_in_dim(local, core * width, width, axis=-1)
        mine = lax.all_gather(part, "fsdp", axis=gather_axis, tiled=True)
        return (mine, swap_core(mine))
    width = local.shape[-1] // 4
    part = lax.dynamic_slice_in_dim(local, (2 * core + y) * width, width, axis=-1)
    own = lax.all_gather(part, "fsdp", axis=gather_axis, tiled=True)
    y_part = swap_y(own)
    return (own, y_part, swap_core(own), swap_core(y_part))


def reduce_split(parts, scatter_axis, spot):
    y, core = spot
    own, y_part, core_part, cross_part = parts
    from_core = swap_core(core_part.astype(jnp.bfloat16)).astype(jnp.float32)
    from_cross = swap_core(cross_part.astype(jnp.bfloat16)).astype(jnp.float32)
    chip_own = own + from_core
    chip_y = (y_part + from_cross).astype(jnp.bfloat16)
    total = (chip_own + swap_y(chip_y).astype(jnp.float32)).astype(jnp.bfloat16)
    owned = lax.psum_scatter(total, "fsdp", scatter_dimension=scatter_axis, tiled=True)
    owned_y = swap_y(owned)
    mine = join(owned, owned_y, y)
    return join(mine, swap_core(mine), core).astype(jnp.float32)


def reduce_half(parts, scatter_axis, spot):
    y, core = spot
    mine, other = parts
    received = swap_core(other.astype(jnp.bfloat16)).astype(jnp.float32)
    chip = (mine + received).astype(jnp.bfloat16)
    owned = lax.psum_scatter(chip, "fsdp", scatter_dimension=scatter_axis, tiled=True)
    summed = owned.astype(jnp.float32) + swap_y(owned).astype(jnp.float32)
    return join(summed, swap_core(summed), core)


def fetch_small(modulation, gains, biases, ffn_bias):
    width = modulation.shape[1]
    length = ffn_bias.shape[0]
    rows = -(-length // width)
    padded = jnp.pad(ffn_bias, (0, rows * width - length)).reshape(rows, width)
    packed = jnp.concatenate([modulation, gains, biases, padded], axis=0)
    full = lax.all_gather(packed, "fsdp", axis=1, tiled=True)
    shards = full.shape[1] // width
    bias_rows = full[21:].reshape(rows, shards, width).transpose(1, 0, 2)
    bias_full = bias_rows.reshape(shards, rows * width)[:, :length].reshape(shards * length)
    return full[:6], full[6:11], full[11:21], bias_full


def reduce_small(grad_mod, grad_gains, grad_biases, grad_ffn_bias, grad_time, width, length):
    rows = -(-length // width)
    shards = grad_mod.shape[1] // width
    bias_rows = jnp.pad(grad_ffn_bias.reshape(shards, length), ((0, 0), (0, rows * width - length)))
    bias_rows = bias_rows.reshape(shards, rows, width).transpose(1, 0, 2).reshape(rows, shards * width)
    packed = jnp.concatenate([grad_mod, grad_gains, grad_biases, bias_rows], axis=0)
    owned = lax.psum_scatter(packed, "fsdp", scatter_dimension=1, tiled=True)
    flat = jnp.concatenate([owned.reshape(-1), grad_time.reshape(-1)])
    summed = lax.psum(flat, SEQ)
    owned = summed[: owned.size].reshape(owned.shape)
    grad_time = summed[owned.size :].reshape(grad_time.shape)
    bias_owned = owned[21:].reshape(-1)[:length]
    return owned[:6], owned[6:11], owned[11:21], bias_owned, grad_time


def micro_step(weights, hidden, key_all, value_all, time_emb, places, cotangent):
    modulation, self_q, self_k, self_v, self_o, cross_q, cross_k, cross_v, cross_o, ffn_in, ffn_out, gains, biases, ffn_bias = (
        weights
    )
    gain_rows = gains.astype(jnp.float32)
    bias_rows = biases.astype(jnp.float32)
    modulated = modulation.astype(jnp.float32)[None] + time_emb.astype(jnp.float32)
    mod = [modulated[:, row, None, :] for row in range(6)]
    cosine, signed_sine = jax.vmap(lambda clip_places: rotary_tables(clip_places, HEAD, HEADS))(places)
    residual_in = hidden.astype(jnp.float32)
    normed_full, pull_first = jax.vjp(modulate_norm, residual_in, mod[0], mod[1])
    normed = normed_full.astype(jnp.bfloat16)
    query_pre = self_q.apply(normed) + bias_rows[0]
    key_pre = self_k.apply(normed) + bias_rows[1]
    value_low = (self_v.apply(normed) + bias_rows[2]).astype(jnp.bfloat16)

    def turn_both(query_input, key_input, gain_query, gain_key):
        return (
            rotate(rms_norm(query_input, gain_query), cosine, signed_sine),
            rotate(rms_norm(key_input, gain_key), cosine, signed_sine),
        )

    turned, pull_turn = jax.vjp(turn_both, query_pre, key_pre, gain_rows[0], gain_rows[1])
    query_heads, key_heads, value_heads = (
        lax.all_to_all(turned[0].astype(jnp.bfloat16), SEQ, split_axis=2, concat_axis=1, tiled=True),
        lax.all_to_all(turned[1].astype(jnp.bfloat16), SEQ, split_axis=2, concat_axis=1, tiled=True),
        lax.all_to_all(value_low, SEQ, split_axis=2, concat_axis=1, tiled=True),
    )
    attn_heads, log_total = attend(query_heads, key_heads, value_heads)
    attended = lax.all_to_all(attn_heads, SEQ, split_axis=1, concat_axis=2, tiled=True)
    branch = self_o.apply(attended) + bias_rows[3]
    after_attn = residual_in + branch * mod[2]
    crossed_full, pull_cross = jax.vjp(affine_norm, after_attn, gain_rows[4], bias_rows[8])
    crossed = crossed_full.astype(jnp.bfloat16)
    cross_query_pre = cross_q.apply(crossed) + bias_rows[4]
    cross_query_full, pull_cross_query = jax.vjp(rms_norm, cross_query_pre, gain_rows[2])
    cross_query = cross_query_full.astype(jnp.bfloat16)
    cross_rows, cross_total = attend(cross_query, key_all, value_all)
    second = after_attn + cross_o.apply(cross_rows) + bias_rows[7]
    ffn_normed_full, pull_second = jax.vjp(modulate_norm, second, mod[3], mod[4])
    ffn_normed = ffn_normed_full.astype(jnp.bfloat16)
    pre_act = ffn_in.apply(ffn_normed) + ffn_bias.astype(jnp.float32)
    activation_full, pull_gelu = jax.vjp(gelu_tanh, pre_act)
    activation = activation_full.astype(jnp.bfloat16)
    ffn_branch = ffn_out.apply(activation) + bias_rows[9]
    mixed = (second + ffn_branch * mod[5]).astype(jnp.bfloat16)
    grad_output = cotangent.astype(jnp.float32)
    gate_ffn = jnp.sum(grad_output * ffn_branch, axis=1)
    grad_ffn_branch = (grad_output * mod[5]).astype(jnp.bfloat16)
    grad_pre_full = pull_gelu(ffn_out.back(grad_ffn_branch))[0]
    grad_pre = grad_pre_full.astype(jnp.bfloat16)
    grad_second_part, shift_ffn, scale_ffn = pull_second(ffn_in.back(grad_pre))
    grad_second = grad_output + grad_second_part
    grad_cross_branch = grad_second.astype(jnp.bfloat16)
    grad_cross_rows = cross_o.back(grad_cross_branch).astype(jnp.bfloat16)
    grad_cross_query, grad_key_all, grad_value_all = attend_back(
        cross_query, key_all, value_all, cross_total, grad_cross_rows
    )
    grad_cross_query_full, gain_cross_query = pull_cross_query(grad_cross_query)
    grad_cross_query_pre = grad_cross_query_full.astype(jnp.bfloat16)
    grad_after_part, gain_norm, bias_norm = pull_cross(cross_q.back(grad_cross_query_pre))
    grad_after = grad_second + grad_after_part
    gate_attn = jnp.sum(grad_after * branch, axis=1)
    grad_branch = (grad_after * mod[2]).astype(jnp.bfloat16)
    grad_attended = self_o.back(grad_branch).astype(jnp.bfloat16)
    grad_attn_heads = lax.all_to_all(grad_attended, SEQ, split_axis=2, concat_axis=1, tiled=True)
    grad_query_heads, grad_key_heads, grad_value_heads = attend_back(
        query_heads, key_heads, value_heads, log_total, grad_attn_heads
    )
    grad_query_turned, grad_key_turned, grad_value = (
        lax.all_to_all(
            grad_query_heads.astype(jnp.bfloat16), SEQ, split_axis=1, concat_axis=2, tiled=True
        ),
        lax.all_to_all(
            grad_key_heads.astype(jnp.bfloat16), SEQ, split_axis=1, concat_axis=2, tiled=True
        ),
        lax.all_to_all(
            grad_value_heads.astype(jnp.bfloat16), SEQ, split_axis=1, concat_axis=2, tiled=True
        ),
    )
    grad_query_full, grad_key_full, gain_query, gain_key = pull_turn(
        (grad_query_turned.astype(jnp.float32), grad_key_turned.astype(jnp.float32))
    )
    grad_query_pre = grad_query_full.astype(jnp.bfloat16)
    grad_key_pre = grad_key_full.astype(jnp.bfloat16)
    grad_normed = self_q.back(grad_query_pre) + self_k.back(grad_key_pre) + self_v.back(grad_value)
    grad_start, shift_attn, scale_attn = pull_first(grad_normed)
    grad_hidden = grad_after + grad_start
    grad_modulated = jnp.stack(
        (shift_attn[:, 0], scale_attn[:, 0], gate_attn, shift_ffn[:, 0], scale_ffn[:, 0], gate_ffn), axis=1
    )
    grad_gains = jnp.stack((gain_query, gain_key, gain_cross_query, jnp.zeros_like(gain_query), gain_norm))
    grad_biases = jnp.stack(
        (
            column_sums(grad_query_pre),
            column_sums(grad_key_pre),
            column_sums(grad_value),
            column_sums(grad_branch),
            column_sums(grad_cross_query_pre),
            jnp.zeros_like(bias_norm),
            jnp.zeros_like(bias_norm),
            column_sums(grad_cross_branch),
            bias_norm,
            column_sums(grad_ffn_branch),
        )
    )
    small = (jnp.sum(grad_modulated, axis=0), grad_gains, grad_biases, column_sums(grad_pre))
    split = (
        (normed, grad_query_pre),
        (normed, grad_key_pre),
        (normed, grad_value),
        (attended, grad_branch),
        (crossed, grad_cross_query_pre),
        (cross_rows, grad_cross_branch),
        (ffn_normed, grad_pre),
        (activation, grad_ffn_branch),
    )
    return (mixed, grad_hidden, (grad_key_all, grad_value_all), grad_modulated, small, split)


def body(
    hidden,
    text,
    time_emb,
    modulation,
    self_in,
    self_out,
    cross_in,
    cross_out,
    ffn_in,
    ffn_out,
    gains,
    biases,
    ffn_bias,
    positions,
    cotangent,
):
    spot = (lax.axis_index("y"), lax.axis_index("core"))
    width = modulation.shape[1]
    length = ffn_bias.shape[0]
    heads_in = self_in.shape[0]
    attn_in_parts = fetch_split(jnp.concatenate([self_in, cross_in], axis=0), 1, spot)
    attn_out_parts = fetch_split(jnp.stack([self_out, cross_out]), 1, spot)
    ffn_in_parts = fetch_split(ffn_in, 0, spot, quarters=False)
    ffn_out_parts = fetch_split(ffn_out, 0, spot, quarters=False)
    modulation_full, gains_full, biases_full, ffn_bias_full = fetch_small(modulation, gains, biases, ffn_bias)
    in_split = [Split(tuple(part[i] for part in attn_in_parts), spot) for i in range(2 * heads_in)]
    out_split = [Split(tuple(part[i] for part in attn_out_parts), spot) for i in range(2)]
    weights = (
        modulation_full,
        in_split[0],
        in_split[1],
        in_split[2],
        out_split[0],
        in_split[3],
        in_split[4],
        in_split[5],
        out_split[1],
        Split(ffn_in_parts, spot),
        Split(ffn_out_parts, spot),
        gains_full,
        biases_full,
        ffn_bias_full,
    )
    cross_k, cross_v = in_split[4], in_split[5]
    gain_rows = gains_full.astype(jnp.float32)
    bias_rows = biases_full.astype(jnp.float32)
    clips, words, model = text.shape
    text_flat = text.reshape(clips * words, model)
    text_key_pre = cross_k.apply(text_flat) + bias_rows[5]
    text_key_full, pull_text_key = jax.vjp(rms_norm, text_key_pre, gain_rows[3])
    text_value = (cross_v.apply(text_flat) + bias_rows[6]).astype(jnp.bfloat16)
    text_key_low = text_key_full.astype(jnp.bfloat16)
    local_kv = jnp.concatenate(
        [part[i * words : (i + 1) * words] for part in (text_key_low, text_value) for i in range(clips)], axis=1
    )
    all_kv = lax.all_gather(local_kv, SEQ, axis=0, tiled=True)
    key_all = jnp.stack([all_kv[:, i * model : (i + 1) * model] for i in range(clips)])
    value_all = jnp.stack([all_kv[:, (clips + i) * model : (clips + i + 1) * model] for i in range(clips)])
    mixed, grad_hidden, text_grads, grad_time, small_totals, split = micro_step(
        weights, hidden, key_all, value_all, time_emb, positions, cotangent
    )
    key_grads = [text_grads[0][i] for i in range(clips)]
    value_grads = [text_grads[1][i] for i in range(clips)]
    pairs = [(rows.reshape(-1, rows.shape[-1]), grad.reshape(-1, grad.shape[-1])) for rows, grad in split]
    split_grads = [
        split_weight.grad(rows, grad, quarters=index != 6)
        for index, (split_weight, (rows, grad)) in enumerate(
            zip(
                (in_split[0], in_split[1], in_split[2], out_split[0], in_split[3], out_split[1], weights[9], weights[10]),
                pairs,
            )
        )
    ]
    grad_kv = jnp.concatenate(key_grads + value_grads, axis=1).astype(jnp.bfloat16)
    owned_kv = lax.psum_scatter(grad_kv, SEQ, scatter_dimension=0, tiled=True).astype(jnp.float32)
    owned_parts = [owned_kv[:, i * model : (i + 1) * model] for i in range(2 * clips)]
    grad_text_key = jnp.concatenate(owned_parts[:clips], axis=0)
    grad_text_value = jnp.concatenate(owned_parts[clips:], axis=0).astype(jnp.bfloat16)
    grad_text_key_full, gain_cross_key = pull_text_key(grad_text_key)
    grad_text_key_pre = grad_text_key_full.astype(jnp.bfloat16)
    weight_cross_key = cross_k.grad(text_flat, grad_text_key_pre)
    weight_cross_value = cross_v.grad(text_flat, grad_text_value)
    grad_words = cross_k.back(grad_text_key_pre) + cross_v.back(grad_text_value)
    grad_mod, grad_gains, grad_biases, grad_ffn_bias_local = small_totals
    grad_gains = grad_gains.at[3].add(gain_cross_key)
    grad_biases = grad_biases.at[5].add(column_sums(grad_text_key_pre))
    grad_biases = grad_biases.at[6].add(column_sums(grad_text_value))
    attn_in_grads = tuple(
        jnp.stack(
            [split_grads[0][q], split_grads[1][q], split_grads[2][q], split_grads[4][q], weight_cross_key[q], weight_cross_value[q]]
        )
        for q in range(4)
    )
    attn_out_grads = tuple(jnp.stack([split_grads[3][q], split_grads[5][q]]) for q in range(4))
    attn_final = reduce_split(
        tuple(jnp.concatenate([a, b]) for a, b in zip(attn_in_grads, attn_out_grads)), 1, spot
    )
    attn_in_final = attn_final[: 2 * heads_in]
    attn_out_final = attn_final[2 * heads_in :]
    ffn_in_final = reduce_half(split_grads[6], 0, spot)
    ffn_out_final = reduce_split(split_grads[7], 0, spot)
    grad_mod, grad_gains, grad_biases, grad_ffn_bias, grad_time = reduce_small(
        grad_mod, grad_gains, grad_biases, grad_ffn_bias_local, grad_time, width, length
    )
    return (
        mixed,
        grad_hidden,
        grad_words.reshape(clips, words, model),
        grad_time,
        grad_mod,
        attn_in_final[:heads_in],
        attn_out_final[0],
        attn_in_final[heads_in:],
        attn_out_final[1],
        ffn_in_final,
        ffn_out_final,
        grad_gains,
        grad_biases,
        grad_ffn_bias,
    )


def solution(mesh):
    devices = mesh.devices
    split_mesh = Mesh(
        devices.reshape(devices.shape[0] // 2, 2, devices.shape[1]), ("y", "core", "fsdp")
    )
    return jax.shard_map(
        body,
        mesh=split_mesh,
        in_specs=(
            P("fsdp", SEQ, None),
            P("fsdp", SEQ, None),
            P("fsdp", None, None),
            P(None, "fsdp"),
            P(None, "fsdp", None),
            P("fsdp", None),
            P(None, "fsdp", None),
            P("fsdp", None),
            P("fsdp", None),
            P("fsdp", None),
            P(None, "fsdp"),
            P(None, "fsdp"),
            P("fsdp"),
            P("fsdp", None, SEQ),
            P("fsdp", SEQ, None),
        ),
        out_specs=(
            P("fsdp", SEQ, None),
            P("fsdp", SEQ, None),
            P("fsdp", SEQ, None),
            P("fsdp", None, None),
            P(None, "fsdp"),
            P(None, "fsdp", None),
            P("fsdp", None),
            P(None, "fsdp", None),
            P("fsdp", None),
            P("fsdp", None),
            P("fsdp", None),
            P(None, "fsdp"),
            P(None, "fsdp"),
            P("fsdp"),
        ),
        check_vma=False,
    )
```

```python
import jax
import jax.numpy as jnp
from jax import lax
from jax.sharding import Mesh, PartitionSpec as P

HEADS = 12
HEAD = 128


EPSILON = 1e-06
SEQ = ("y", "core")
SWAP = [(0, 1), (1, 0)]


def matmul(operand, factor):
    return jnp.dot(operand, factor, preferred_element_type=jnp.float32)


def inner_rows(operand, factor):
    return lax.dot_general(
        operand, factor, (((0,), (0,)), ((), ())), preferred_element_type=jnp.float32
    )


def outer_cols(operand, factor):
    return lax.dot_general(
        operand, factor, (((operand.ndim - 1,), (1,)), ((), ())), preferred_element_type=jnp.float32
    )


def column_sums(tensor):
    return jnp.sum(tensor.astype(jnp.float32), axis=tuple(range(tensor.ndim - 1)))


def layer_norm(tensor):
    centered = tensor - jnp.mean(tensor, axis=-1, keepdims=True)
    return centered * lax.rsqrt(jnp.mean(centered * centered, axis=-1, keepdims=True) + EPSILON)


def rms_norm(tensor, weight):
    return tensor * lax.rsqrt(jnp.mean(tensor * tensor, axis=-1, keepdims=True) + EPSILON) * weight


def modulate_norm(tensor, shift, scale):
    return layer_norm(tensor) * (1.0 + scale) + shift


def affine_norm(tensor, weight, offset):
    return layer_norm(tensor) * weight + offset


def gelu_tanh(tensor):
    return jax.nn.gelu(tensor, approximate=True)


def rotary_tables(places, head_size, head_count):
    one_sixth = head_size // 6
    span_sizes = (head_size - 4 * one_sixth, 2 * one_sixth, 2 * one_sixth)
    angles = []
    for component in range(3):
        exponents = (
            jnp.arange(0, span_sizes[component], 2, dtype=jnp.float32) / span_sizes[component]
        )
        frequency = 1.0 / 10000.0**exponents
        angles.append(places[component].astype(jnp.float32)[:, None] * frequency[None, :])
    joined = jnp.concatenate(angles, axis=1)
    tiled_angles = jnp.tile(jnp.repeat(joined, 2, axis=1), (1, head_count))
    parity = jnp.where(jnp.arange(tiled_angles.shape[1]) % 2 == 0, -1.0, 1.0)
    return (jnp.cos(tiled_angles), jnp.sin(tiled_angles) * parity)


def rotate(tensor, cosine, signed_sine):
    even_lane = jnp.arange(tensor.shape[-1]) % 2 == 0
    swapped = jnp.where(even_lane, jnp.roll(tensor, -1, axis=-1), jnp.roll(tensor, 1, axis=-1))
    return tensor * cosine + swapped * signed_sine


def split_heads(tensor):
    return tensor.reshape(tensor.shape[0], tensor.shape[1], tensor.shape[2] // HEAD, HEAD)


def attend(queries, key_rows, value_rows):
    scores = jnp.einsum(
        "bqhd,bkhd->bhqk",
        split_heads(queries),
        split_heads(key_rows),
        preferred_element_type=jnp.float32,
    ) * HEAD ** (-0.5)
    row_max = jnp.max(scores, axis=-1, keepdims=True)
    exponentials = jnp.exp(scores - row_max)
    row_total = jnp.sum(exponentials, axis=-1, keepdims=True)
    probabilities = (exponentials / row_total).astype(jnp.bfloat16)
    result = jnp.einsum(
        "bhqk,bkhd->bqhd", probabilities, split_heads(value_rows), preferred_element_type=jnp.float32
    )
    return (result.reshape(queries.shape).astype(jnp.bfloat16), row_max + jnp.log(row_total))


def attend_back(queries, key_rows, value_rows, log_total, grad_rows):
    query_split = split_heads(queries)
    key_split = split_heads(key_rows)
    grad_split = split_heads(grad_rows)
    scale_factor = HEAD ** (-0.5)
    scores = (
        jnp.einsum("bqhd,bkhd->bhqk", query_split, key_split, preferred_element_type=jnp.float32)
        * scale_factor
    )
    probs_full = jnp.exp(scores - log_total)
    probs_low = probs_full.astype(jnp.bfloat16)
    grad_values = jnp.einsum(
        "bhqk,bqhd->bkhd", probs_low, grad_split, preferred_element_type=jnp.float32
    )
    grad_probs = jnp.einsum(
        "bqhd,bkhd->bhqk", grad_split, split_heads(value_rows), preferred_element_type=jnp.float32
    )
    grad_scores = (
        probs_full * (grad_probs - jnp.sum(grad_probs * probs_full, axis=-1, keepdims=True))
    ).astype(jnp.bfloat16)
    grad_queries = (
        jnp.einsum("bhqk,bkhd->bqhd", grad_scores, key_split, preferred_element_type=jnp.float32)
        * scale_factor
    )
    grad_keys = (
        jnp.einsum("bhqk,bqhd->bkhd", grad_scores, query_split, preferred_element_type=jnp.float32)
        * scale_factor
    )
    return (
        grad_queries.reshape(queries.shape),
        grad_keys.reshape(key_rows.shape),
        grad_values.reshape(value_rows.shape),
    )


def swap_core(tensor):
    return lax.ppermute(tensor, "core", SWAP)


def join(mine, other, core):
    width = mine.shape[-1]
    both = jnp.concatenate([other, mine, other], axis=-1)
    return lax.dynamic_slice_in_dim(both, (1 - core) * width, 2 * width, axis=-1)


def halves(tensor, core):
    width = tensor.shape[-1] // 2
    return (
        lax.dynamic_slice_in_dim(tensor, core * width, width, axis=-1),
        lax.dynamic_slice_in_dim(tensor, (1 - core) * width, width, axis=-1),
    )


def swap_y(tensor):
    return lax.ppermute(tensor, "y", SWAP)


class Split:
    def __init__(self, parts, spot):
        self.parts, self.spot = parts, spot

    def apply(self, rows):
        y, core = self.spot
        outs = [matmul(rows, part) for part in self.parts]
        if len(outs) == 2:
            return join(outs[0], outs[1], core)
        return join(join(outs[0], outs[1], y), join(outs[2], outs[3], y), core)

    def quarters(self, grad):
        y, core = self.spot
        grad_mine, grad_other = halves(grad, core)
        return halves(grad_mine, y) + halves(grad_other, y)

    def back(self, grad):
        if len(self.parts) == 2:
            grad_mine, grad_other = halves(grad, self.spot[1])
            return outer_cols(grad_mine, self.parts[0]) + outer_cols(grad_other, self.parts[1])
        pieces = [outer_cols(g, part) for g, part in zip(self.quarters(grad), self.parts)]
        return (pieces[0] + pieces[1]) + (pieces[2] + pieces[3])

    def grad(self, rows, grad, quarters=True):
        pieces = self.quarters(grad) if quarters else halves(grad, self.spot[1])
        return tuple(inner_rows(rows, g) for g in pieces)


def fetch_split(local, gather_axis, spot, quarters=True):
    y, core = spot
    if not quarters:
        width = local.shape[-1] // 2
        part = lax.dynamic_slice_in_dim(local, core * width, width, axis=-1)
        mine = lax.all_gather(part, "fsdp", axis=gather_axis, tiled=True)
        return (mine, swap_core(mine))
    width = local.shape[-1] // 4
    part = lax.dynamic_slice_in_dim(local, (2 * core + y) * width, width, axis=-1)
    own = lax.all_gather(part, "fsdp", axis=gather_axis, tiled=True)
    y_part = swap_y(own)
    return (own, y_part, swap_core(own), swap_core(y_part))


def reduce_split(parts, scatter_axis, spot):
    y, core = spot
    own, y_part, core_part, cross_part = parts
    from_core = swap_core(core_part.astype(jnp.bfloat16)).astype(jnp.float32)
    from_cross = swap_core(cross_part.astype(jnp.bfloat16)).astype(jnp.float32)
    chip_own = own + from_core
    chip_y = (y_part + from_cross).astype(jnp.bfloat16)
    total = (chip_own + swap_y(chip_y).astype(jnp.float32)).astype(jnp.bfloat16)
    owned = lax.psum_scatter(total, "fsdp", scatter_dimension=scatter_axis, tiled=True)
    owned_y = swap_y(owned)
    mine = join(owned, owned_y, y)
    return join(mine, swap_core(mine), core).astype(jnp.float32)


def reduce_half(parts, scatter_axis, spot):
    y, core = spot
    mine, other = parts
    received = swap_core(other.astype(jnp.bfloat16)).astype(jnp.float32)
    chip = (mine + received).astype(jnp.bfloat16)
    owned = lax.psum_scatter(chip, "fsdp", scatter_dimension=scatter_axis, tiled=True)
    summed = owned.astype(jnp.float32) + swap_y(owned).astype(jnp.float32)
    return join(summed, swap_core(summed), core)


def fetch_small(modulation, gains, biases, ffn_bias):
    width = modulation.shape[1]
    length = ffn_bias.shape[0]
    rows = -(-length // width)
    padded = jnp.pad(ffn_bias, (0, rows * width - length)).reshape(rows, width)
    packed = jnp.concatenate([modulation, gains, biases, padded], axis=0)
    full = lax.all_gather(packed, "fsdp", axis=1, tiled=True)
    shards = full.shape[1] // width
    bias_rows = full[21:].reshape(rows, shards, width).transpose(1, 0, 2)
    bias_full = bias_rows.reshape(shards, rows * width)[:, :length].reshape(shards * length)
    return full[:6], full[6:11], full[11:21], bias_full


def reduce_small(grad_mod, grad_gains, grad_biases, grad_ffn_bias, grad_time, width, length):
    rows = -(-length // width)
    shards = grad_mod.shape[1] // width
    bias_rows = jnp.pad(grad_ffn_bias.reshape(shards, length), ((0, 0), (0, rows * width - length)))
    bias_rows = bias_rows.reshape(shards, rows, width).transpose(1, 0, 2).reshape(rows, shards * width)
    packed = jnp.concatenate([grad_mod, grad_gains, grad_biases, bias_rows], axis=0)
    owned = lax.psum_scatter(packed, "fsdp", scatter_dimension=1, tiled=True)
    flat = jnp.concatenate([owned.reshape(-1), grad_time.reshape(-1)])
    summed = lax.psum(flat, SEQ)
    owned = summed[: owned.size].reshape(owned.shape)
    grad_time = summed[owned.size :].reshape(grad_time.shape)
    bias_owned = owned[21:].reshape(-1)[:length]
    return owned[:6], owned[6:11], owned[11:21], bias_owned, grad_time


def micro_step(weights, hidden, key_all, value_all, time_emb, places, cotangent):
    modulation, self_q, self_k, self_v, self_o, cross_q, cross_k, cross_v, cross_o, ffn_in, ffn_out, gains, biases, ffn_bias = (
        weights
    )
    gain_rows = gains.astype(jnp.float32)
    bias_rows = biases.astype(jnp.float32)
    modulated = modulation.astype(jnp.float32)[None] + time_emb.astype(jnp.float32)
    mod = [modulated[:, row, None, :] for row in range(6)]
    cosine, signed_sine = jax.vmap(lambda clip_places: rotary_tables(clip_places, HEAD, HEADS))(places)
    residual_in = hidden.astype(jnp.float32)
    normed_full, pull_first = jax.vjp(modulate_norm, residual_in, mod[0], mod[1])
    normed = normed_full.astype(jnp.bfloat16)
    query_pre = self_q.apply(normed) + bias_rows[0]
    key_pre = self_k.apply(normed) + bias_rows[1]
    value_low = (self_v.apply(normed) + bias_rows[2]).astype(jnp.bfloat16)

    def turn_both(query_input, key_input, gain_query, gain_key):
        return (
            rotate(rms_norm(query_input, gain_query), cosine, signed_sine),
            rotate(rms_norm(key_input, gain_key), cosine, signed_sine),
        )

    turned, pull_turn = jax.vjp(turn_both, query_pre, key_pre, gain_rows[0], gain_rows[1])
    query_heads, key_heads, value_heads = (
        lax.all_to_all(turned[0].astype(jnp.bfloat16), SEQ, split_axis=2, concat_axis=1, tiled=True),
        lax.all_to_all(turned[1].astype(jnp.bfloat16), SEQ, split_axis=2, concat_axis=1, tiled=True),
        lax.all_to_all(value_low, SEQ, split_axis=2, concat_axis=1, tiled=True),
    )
    attn_heads, log_total = attend(query_heads, key_heads, value_heads)
    attended = lax.all_to_all(attn_heads, SEQ, split_axis=1, concat_axis=2, tiled=True)
    branch = self_o.apply(attended) + bias_rows[3]
    after_attn = residual_in + branch * mod[2]
    crossed_full, pull_cross = jax.vjp(affine_norm, after_attn, gain_rows[4], bias_rows[8])
    crossed = crossed_full.astype(jnp.bfloat16)
    cross_query_pre = cross_q.apply(crossed) + bias_rows[4]
    cross_query_full, pull_cross_query = jax.vjp(rms_norm, cross_query_pre, gain_rows[2])
    cross_query = cross_query_full.astype(jnp.bfloat16)
    cross_rows, cross_total = attend(cross_query, key_all, value_all)
    second = after_attn + cross_o.apply(cross_rows) + bias_rows[7]
    ffn_normed_full, pull_second = jax.vjp(modulate_norm, second, mod[3], mod[4])
    ffn_normed = ffn_normed_full.astype(jnp.bfloat16)
    pre_act = ffn_in.apply(ffn_normed) + ffn_bias.astype(jnp.float32)
    activation_full, pull_gelu = jax.vjp(gelu_tanh, pre_act)
    activation = activation_full.astype(jnp.bfloat16)
    ffn_branch = ffn_out.apply(activation) + bias_rows[9]
    mixed = (second + ffn_branch * mod[5]).astype(jnp.bfloat16)
    grad_output = cotangent.astype(jnp.float32)
    gate_ffn = jnp.sum(grad_output * ffn_branch, axis=1)
    grad_ffn_branch = (grad_output * mod[5]).astype(jnp.bfloat16)
    grad_pre_full = pull_gelu(ffn_out.back(grad_ffn_branch))[0]
    grad_pre = grad_pre_full.astype(jnp.bfloat16)
    grad_second_part, shift_ffn, scale_ffn = pull_second(ffn_in.back(grad_pre))
    grad_second = grad_output + grad_second_part
    grad_cross_branch = grad_second.astype(jnp.bfloat16)
    grad_cross_rows = cross_o.back(grad_cross_branch).astype(jnp.bfloat16)
    grad_cross_query, grad_key_all, grad_value_all = attend_back(
        cross_query, key_all, value_all, cross_total, grad_cross_rows
    )
    grad_cross_query_full, gain_cross_query = pull_cross_query(grad_cross_query)
    grad_cross_query_pre = grad_cross_query_full.astype(jnp.bfloat16)
    grad_after_part, gain_norm, bias_norm = pull_cross(cross_q.back(grad_cross_query_pre))
    grad_after = grad_second + grad_after_part
    gate_attn = jnp.sum(grad_after * branch, axis=1)
    grad_branch = (grad_after * mod[2]).astype(jnp.bfloat16)
    grad_attended = self_o.back(grad_branch).astype(jnp.bfloat16)
    grad_attn_heads = lax.all_to_all(grad_attended, SEQ, split_axis=2, concat_axis=1, tiled=True)
    grad_query_heads, grad_key_heads, grad_value_heads = attend_back(
        query_heads, key_heads, value_heads, log_total, grad_attn_heads
    )
    grad_query_turned, grad_key_turned, grad_value = (
        lax.all_to_all(
            grad_query_heads.astype(jnp.bfloat16), SEQ, split_axis=1, concat_axis=2, tiled=True
        ),
        lax.all_to_all(
            grad_key_heads.astype(jnp.bfloat16), SEQ, split_axis=1, concat_axis=2, tiled=True
        ),
        lax.all_to_all(
            grad_value_heads.astype(jnp.bfloat16), SEQ, split_axis=1, concat_axis=2, tiled=True
        ),
    )
    grad_query_full, grad_key_full, gain_query, gain_key = pull_turn(
        (grad_query_turned.astype(jnp.float32), grad_key_turned.astype(jnp.float32))
    )
    grad_query_pre = grad_query_full.astype(jnp.bfloat16)
    grad_key_pre = grad_key_full.astype(jnp.bfloat16)
    grad_normed = self_q.back(grad_query_pre) + self_k.back(grad_key_pre) + self_v.back(grad_value)
    grad_start, shift_attn, scale_attn = pull_first(grad_normed)
    grad_hidden = grad_after + grad_start
    grad_modulated = jnp.stack(
        (shift_attn[:, 0], scale_attn[:, 0], gate_attn, shift_ffn[:, 0], scale_ffn[:, 0], gate_ffn), axis=1
    )
    grad_gains = jnp.stack((gain_query, gain_key, gain_cross_query, jnp.zeros_like(gain_query), gain_norm))
    grad_biases = jnp.stack(
        (
            column_sums(grad_query_pre),
            column_sums(grad_key_pre),
            column_sums(grad_value),
            column_sums(grad_branch),
            column_sums(grad_cross_query_pre),
            jnp.zeros_like(bias_norm),
            jnp.zeros_like(bias_norm),
            column_sums(grad_cross_branch),
            bias_norm,
            column_sums(grad_ffn_branch),
        )
    )
    small = (jnp.sum(grad_modulated, axis=0), grad_gains, grad_biases, column_sums(grad_pre))
    split = (
        (normed, grad_query_pre),
        (normed, grad_key_pre),
        (normed, grad_value),
        (attended, grad_branch),
        (crossed, grad_cross_query_pre),
        (cross_rows, grad_cross_branch),
        (ffn_normed, grad_pre),
        (activation, grad_ffn_branch),
    )
    return (mixed, grad_hidden, (grad_key_all, grad_value_all), grad_modulated, small, split)


def body(
    hidden,
    text,
    time_emb,
    modulation,
    self_in,
    self_out,
    cross_in,
    cross_out,
    ffn_in,
    ffn_out,
    gains,
    biases,
    ffn_bias,
    positions,
    cotangent,
):
    spot = (lax.axis_index("y"), lax.axis_index("core"))
    width = modulation.shape[1]
    length = ffn_bias.shape[0]
    heads_in = self_in.shape[0]
    attn_in_parts = fetch_split(jnp.concatenate([self_in, cross_in], axis=0), 1, spot)
    attn_out_parts = fetch_split(jnp.stack([self_out, cross_out]), 1, spot)
    ffn_in_parts = fetch_split(ffn_in, 0, spot)
    ffn_out_parts = fetch_split(ffn_out, 0, spot, quarters=False)
    modulation_full, gains_full, biases_full, ffn_bias_full = fetch_small(modulation, gains, biases, ffn_bias)
    in_split = [Split(tuple(part[i] for part in attn_in_parts), spot) for i in range(2 * heads_in)]
    out_split = [Split(tuple(part[i] for part in attn_out_parts), spot) for i in range(2)]
    weights = (
        modulation_full,
        in_split[0],
        in_split[1],
        in_split[2],
        out_split[0],
        in_split[3],
        in_split[4],
        in_split[5],
        out_split[1],
        Split(ffn_in_parts, spot),
        Split(ffn_out_parts, spot),
        gains_full,
        biases_full,
        ffn_bias_full,
    )
    cross_k, cross_v = in_split[4], in_split[5]
    gain_rows = gains_full.astype(jnp.float32)
    bias_rows = biases_full.astype(jnp.float32)
    clips, words, model = text.shape
    text_flat = text.reshape(clips * words, model)
    text_key_pre = cross_k.apply(text_flat) + bias_rows[5]
    text_key_full, pull_text_key = jax.vjp(rms_norm, text_key_pre, gain_rows[3])
    text_value = (cross_v.apply(text_flat) + bias_rows[6]).astype(jnp.bfloat16)
    text_key_low = text_key_full.astype(jnp.bfloat16)
    local_kv = jnp.concatenate(
        [part[i * words : (i + 1) * words] for part in (text_key_low, text_value) for i in range(clips)], axis=1
    )
    all_kv = lax.all_gather(local_kv, SEQ, axis=0, tiled=True)
    key_all = jnp.stack([all_kv[:, i * model : (i + 1) * model] for i in range(clips)])
    value_all = jnp.stack([all_kv[:, (clips + i) * model : (clips + i + 1) * model] for i in range(clips)])
    mixed, grad_hidden, text_grads, grad_time, small_totals, split = micro_step(
        weights, hidden, key_all, value_all, time_emb, positions, cotangent
    )
    key_grads = [text_grads[0][i] for i in range(clips)]
    value_grads = [text_grads[1][i] for i in range(clips)]
    pairs = [(rows.reshape(-1, rows.shape[-1]), grad.reshape(-1, grad.shape[-1])) for rows, grad in split]
    split_grads = [
        split_weight.grad(rows, grad, quarters=index != 6)
        for index, (split_weight, (rows, grad)) in enumerate(
            zip(
                (in_split[0], in_split[1], in_split[2], out_split[0], in_split[3], out_split[1], weights[9], weights[10]),
                pairs,
            )
        )
    ]
    grad_kv = jnp.concatenate(key_grads + value_grads, axis=1).astype(jnp.bfloat16)
    owned_kv = lax.psum_scatter(grad_kv, SEQ, scatter_dimension=0, tiled=True).astype(jnp.float32)
    owned_parts = [owned_kv[:, i * model : (i + 1) * model] for i in range(2 * clips)]
    grad_text_key = jnp.concatenate(owned_parts[:clips], axis=0)
    grad_text_value = jnp.concatenate(owned_parts[clips:], axis=0).astype(jnp.bfloat16)
    grad_text_key_full, gain_cross_key = pull_text_key(grad_text_key)
    grad_text_key_pre = grad_text_key_full.astype(jnp.bfloat16)
    weight_cross_key = cross_k.grad(text_flat, grad_text_key_pre)
    weight_cross_value = cross_v.grad(text_flat, grad_text_value)
    grad_words = cross_k.back(grad_text_key_pre) + cross_v.back(grad_text_value)
    grad_mod, grad_gains, grad_biases, grad_ffn_bias_local = small_totals
    grad_gains = grad_gains.at[3].add(gain_cross_key)
    grad_biases = grad_biases.at[5].add(column_sums(grad_text_key_pre))
    grad_biases = grad_biases.at[6].add(column_sums(grad_text_value))
    attn_in_grads = tuple(
        jnp.stack(
            [split_grads[0][q], split_grads[1][q], split_grads[2][q], split_grads[4][q], weight_cross_key[q], weight_cross_value[q]]
        )
        for q in range(4)
    )
    attn_out_grads = tuple(jnp.stack([split_grads[3][q], split_grads[5][q]]) for q in range(4))
    attn_final = reduce_split(
        tuple(jnp.concatenate([a, b]) for a, b in zip(attn_in_grads, attn_out_grads)), 1, spot
    )
    attn_in_final = attn_final[: 2 * heads_in]
    attn_out_final = attn_final[2 * heads_in :]
    ffn_in_final = reduce_half(split_grads[6], 0, spot)
    ffn_out_final = reduce_split(split_grads[7], 0, spot)
    grad_mod, grad_gains, grad_biases, grad_ffn_bias, grad_time = reduce_small(
        grad_mod, grad_gains, grad_biases, grad_ffn_bias_local, grad_time, width, length
    )
    return (
        mixed,
        grad_hidden,
        grad_words.reshape(clips, words, model),
        grad_time,
        grad_mod,
        attn_in_final[:heads_in],
        attn_out_final[0],
        attn_in_final[heads_in:],
        attn_out_final[1],
        ffn_in_final,
        ffn_out_final,
        grad_gains,
        grad_biases,
        grad_ffn_bias,
    )


def solution(mesh):
    devices = mesh.devices
    split_mesh = Mesh(
        devices.reshape(devices.shape[0] // 2, 2, devices.shape[1]), ("y", "core", "fsdp")
    )
    return jax.shard_map(
        body,
        mesh=split_mesh,
        in_specs=(
            P("fsdp", SEQ, None),
            P("fsdp", SEQ, None),
            P("fsdp", None, None),
            P(None, "fsdp"),
            P(None, "fsdp", None),
            P("fsdp", None),
            P(None, "fsdp", None),
            P("fsdp", None),
            P("fsdp", None),
            P("fsdp", None),
            P(None, "fsdp"),
            P(None, "fsdp"),
            P("fsdp"),
            P("fsdp", None, SEQ),
            P("fsdp", SEQ, None),
        ),
        out_specs=(
            P("fsdp", SEQ, None),
            P("fsdp", SEQ, None),
            P("fsdp", SEQ, None),
            P("fsdp", None, None),
            P(None, "fsdp"),
            P(None, "fsdp", None),
            P("fsdp", None),
            P(None, "fsdp", None),
            P("fsdp", None),
            P("fsdp", None),
            P("fsdp", None),
            P(None, "fsdp"),
            P(None, "fsdp"),
            P("fsdp"),
        ),
        check_vma=False,
    )
```
